16 devices in a mesh: col: 2 (over z), row: 8 (over y, x, core).
Axes of the slice: x: 2, y: 2, z: 2, core: 2. Of those that a mesh axis runs over, the one named last changes fastest.
Arguments:
- mask: int32 [8192, 32768], P('row', 'col')
- user_emb: bfloat16 [8192, 128], P(('row', 'col'))
- item_emb: bfloat16 [32768, 128], P(('col', 'row'))
- queries: int32 [1024], replicated
Outputs:
- output 1: bfloat16 [8192, 128], P(('row', 'col'))
- output 2: bfloat16 [32768, 128], P(('col', 'row'))
- output 3: float32 [1024, 32768], P(None, ('col', 'row'))
All inputs are finite; a program needn't handle non-finite values.
Results may differ from the reference program's by a relative error of at most 0.00652722.
Values are sent between devices in bfloat16 or wider.
A program may use at most 1 GiB of HBM per device.

```python
import jax
import jax.numpy as jnp
from jax import lax

USERS = 8192
ITEMS = 32768
EMB = 128
LAYERS = 3
QUERIES = 1024


def draw_mask(key):
    k_noise, k_rows, k_cols = jax.random.split(key, 3)
    row_level = jax.random.randint(k_rows, (USERS,), 4, 33)
    col_level = jax.random.randint(k_cols, (ITEMS,), 4, 33)
    noise = jax.random.randint(k_noise, (USERS, ITEMS), 0, 1024)
    return (noise < row_level[:, None] * col_level[None, :]).astype(jnp.int32)


def setup_inputs(seed: int = 0) -> dict:
    key = jax.random.key(seed)
    k_mask, k_user, k_item, k_umean, k_imean, k_query = jax.random.split(key, 6)
    scale = EMB ** -0.25
    user_mean = jax.random.normal(k_umean, (EMB,), jnp.float32)
    item_mean = jax.random.normal(k_imean, (EMB,), jnp.float32)
    user_emb = ((jax.random.normal(k_user, (USERS, EMB), jnp.float32) + user_mean[None, :]) * scale).astype(jnp.bfloat16)
    item_emb = ((jax.random.normal(k_item, (ITEMS, EMB), jnp.float32) + item_mean[None, :]) * scale).astype(jnp.bfloat16)
    queries = jax.random.randint(k_query, (QUERIES,), 0, USERS).astype(jnp.int32)
    return {'mask': draw_mask(k_mask), 'user_emb': user_emb, 'item_emb': item_emb, 'queries': queries}


def norm_adjacency(mask):
    deg_user = jnp.maximum(jnp.sum(mask, axis=1), 1)
    deg_item = jnp.maximum(jnp.sum(mask, axis=0), 1)
    inv_user = lax.rsqrt(deg_user.astype(jnp.float32))
    inv_item = lax.rsqrt(deg_item.astype(jnp.float32))
    return (inv_user[:, None] * mask.astype(jnp.float32) * inv_item[None, :]).astype(jnp.bfloat16)


def reference(mask, user_emb, item_emb, queries):
    norm_adj = norm_adjacency(mask)

    def one_layer(carried, unused):
        user_cur, item_cur, user_sum, item_sum = carried
        user_next = jnp.dot(norm_adj, item_cur, preferred_element_type=jnp.float32).astype(jnp.bfloat16)
        item_next = lax.dot_general(norm_adj, user_cur, (((0,), (0,)), ((), ())), preferred_element_type=jnp.float32).astype(jnp.bfloat16)
        return (user_next, item_next, user_sum + user_next.astype(jnp.float32), item_sum + item_next.astype(jnp.float32)), None

    start_state = (user_emb, item_emb, user_emb.astype(jnp.float32), item_emb.astype(jnp.float32))
    end_state, unused_out = lax.scan(one_layer, start_state, None, length=LAYERS)
    final_user = (end_state[2] / (LAYERS + 1)).astype(jnp.bfloat16)
    final_item = (end_state[3] / (LAYERS + 1)).astype(jnp.bfloat16)
    picked = jnp.take(final_user, queries, axis=0)
    scores = lax.dot_general(picked, final_item, (((1,), (1,)), ((), ())), preferred_element_type=jnp.float32)
    return final_user, final_item, scores
```

```python
import functools

import jax
import jax.numpy as jnp
from jax import lax
from jax.experimental import pallas as pl
from jax.experimental.pallas import tpu as pltpu
from jax.sharding import PartitionSpec as P

LAYERS = 3
BF = jnp.bfloat16
F32 = jnp.float32
EMB = 128
ROWS = 1024
STRIPE = 2048
CHIPS = 4
COLS = STRIPE * CHIPS
UROWS = 512
HALF = STRIPE // 2
NCH = 4
CH = HALF // NCH
LROWS = 128
NLOAD = 6
NSTAGE = 3
QUERIES = 1024


def al(v, m):
    return pl.multiple_of(v, m)


def dot(a, b, ca, cb):
    return lax.dot_general(a, b, (((ca,), (cb,)), ((), ())), preferred_element_type=F32)


def kernel(mask_ref, ue_ref, ie_ref, q_ref, fu_ref, fi_ref, pk_ref,
           a, part, r1, r2, panel, eut, upart, ursib, urz, invi, mbuf, stage,
           cs, csr, dus, dur, dis, dir_, usum, pkc, pks, pkz, pkx, pka,
           lsem, xs, xr, s1s, s1r, s2s, s2r, ags, agr, fws, fwr,
           usibs, usibr, uzs, uzr, uas, uar, eis, eir, dgs, dgr, pqs, pqr):
    row = lax.axis_index('row')
    z = lax.axis_index('col')
    c = lax.rem(row, 2)
    x = lax.rem(lax.div(row, 2), 2)
    y = lax.div(row, 4)
    me = y * 2 + x

    def dev(xx, yy, cc, zz):
        return {'row': (yy * 2 + xx) * 2 + cc, 'col': zz}

    ox, oy, oc, oz = 1 - x, 1 - y, 1 - c, 1 - z
    xn, yn, dg = dev(ox, y, c, z), dev(x, oy, c, z), dev(ox, oy, c, z)
    zn, sib, zsib = dev(x, y, c, oz), dev(x, y, oc, z), dev(x, y, oc, oz)

    def rcopy(src, dst, ss, rs, to):
        return pltpu.make_async_remote_copy(src_ref=src, dst_ref=dst, send_sem=ss, recv_sem=rs,
                                            device_id=to, device_id_type=pl.DeviceIdType.MESH)

    barrier = pltpu.get_barrier_semaphore()
    for peer in (xn, yn, dg, zn, sib, zsib):
        pl.semaphore_signal(barrier, inc=1, device_id=peer, device_id_type=pl.DeviceIdType.MESH)

    def load(n):
        rg = lax.div(n, 8)
        p = lax.div(lax.rem(n, 8), 2)
        par = lax.rem(n, 2)
        s = 2 * p + par * c + (1 - par) * oc
        slot = lax.rem(n, NLOAD)
        return pltpu.make_async_copy(
            mask_ref.at[pl.ds(al(rg * LROWS, LROWS), LROWS), pl.ds(al(s * STRIPE, STRIPE), STRIPE)],
            mbuf.at[slot], lsem.at[slot])

    n_load = (ROWS // LROWS) * 8
    for n in range(NLOAD):
        load(n).start()

    ucol = al(c * ROWS + z * UROWS, UROWS)
    usum[...] = ue_ref[...].astype(F32)
    eut[0, :, pl.ds(ucol, UROWS)] = ue_ref[...].astype(F32).T.astype(BF)
    panel[0, pl.ds(al(me * STRIPE, STRIPE), STRIPE), :] = ie_ref[...]
    cs[...] = jnp.zeros_like(cs)
    upart[pl.ds(0, ROWS), :] = jnp.zeros((ROWS, EMB), F32)
    pl.semaphore_wait(barrier, 6)

    own_rows = pl.ds(al(me * STRIPE, STRIPE), STRIPE)

    def ei0(i):
        return rcopy(ie_ref, panel.at[0, own_rows], eis.at[i], eir.at[i], (xn, yn, dg)[i])

    def ua(j, i):
        blk = eut.at[j, :, pl.ds(ucol, UROWS)]
        return rcopy(blk, blk, uas.at[j, i], uar.at[j, i], (zn, sib, zsib)[i])

    for i in range(3):
        ei0(i).start()
    for i in range(3):
        ua(0, i).start()

    def xcopy(m):
        rg = lax.div(m, CHIPS)
        p = lax.rem(m, CHIPS)
        slot = lax.rem(m, NSTAGE)
        return rcopy(stage.at[slot],
                     a.at[pl.ds(al(c * ROWS + rg * LROWS, LROWS), LROWS), pl.ds(al(p * STRIPE, STRIPE), STRIPE)],
                     xs.at[slot], xr, sib)

    def count(m, par):
        n = 2 * m + par
        rg = lax.div(m, CHIPS)
        p = lax.rem(m, CHIPS)
        slot = lax.rem(n, NLOAD)
        sslot = lax.rem(m, NSTAGE)
        load(n).wait()
        cols = pl.ds(al(p * STRIPE, STRIPE), STRIPE)
        acc = jnp.zeros((8, STRIPE), F32)
        for g in range(LROWS // 16):
            v = mbuf[slot, g * 16:(g + 1) * 16, :].astype(F32)
            b = v.astype(BF)
            if par == 0:
                stage[sslot, g * 16:(g + 1) * 16, :] = b
            else:
                a[pl.ds(al(c * ROWS + rg * LROWS + g * 16, 16), 16), cols] = b
            acc = acc + v[0:8] + v[8:16]
            parts = [v[:, i * 128:(i + 1) * 128] for i in range(STRIPE // 128)]
            while len(parts) > 1:
                parts = [parts[i] + parts[i + 1] for i in range(0, len(parts), 2)]
            rsl = pl.ds(al(rg * LROWS + g * 16, 16), 16)
            upart[rsl, :] = upart[rsl, :] + parts[0]
        cs[par, :, cols] = cs[par, :, cols] + acc

        @pl.when(n + NLOAD < n_load)
        def _():
            load(n + NLOAD).start()

    def mask_step(m, _):
        @pl.when(m >= NSTAGE)
        def _():
            xcopy(m - NSTAGE).wait_send()
        count(m, 0)
        xcopy(m).start()
        count(m, 1)
        return 0

    n_pairs = n_load // 2
    lax.fori_loop(0, n_pairs, mask_step, 0)

    def csend():
        return rcopy(cs.at[0], csr, dgs.at[6], dgr.at[6], sib)

    def dusend(i):
        return rcopy(dus, dur.at[i], dgs.at[i], dgr.at[i], (zn, sib, zsib)[i])

    def disend(i):
        return rcopy(dis, dir_.at[i], dgs.at[3 + i], dgr.at[3 + i], (xn, yn, dg)[i])

    csend().start()
    for b in range(ROWS // 128):
        t = upart[b * 128:(b + 1) * 128, :].T
        v = jnp.sum(t, axis=0, keepdims=True)
        dus[:, b * 128:(b + 1) * 128] = jnp.broadcast_to(v, (8, 128))
    for i in range(3):
        dusend(i).start()
    csend().wait_recv()
    tot = jnp.sum(cs[1] + csr[...], axis=0, keepdims=True)
    for g in range(8):
        dis[g:g + 1, :] = tot[:, g * 1024:(g + 1) * 1024]
    for i in range(3):
        disend(i).start()
    for m in range(n_pairs - NSTAGE, n_pairs):
        xcopy(m).wait_send()
    for i in range(3):
        dusend(i).wait_recv()
    for blk, v in ((c, dus[...] + dur[0]), (oc, dur[1] + dur[2])):
        v = lax.rsqrt(jnp.maximum(v, 1.0))
        for b in range(ROWS // 128):
            w = jnp.broadcast_to(v[0:1, b * 128:(b + 1) * 128], (128, 128))
            upart[pl.ds(al(blk * ROWS + b * 128, 128), 128), :] = w.T
    for i in range(3):
        disend(i).wait_recv()
    v = lax.rsqrt(jnp.maximum((dis[...] + dir_[0]) + (dir_[1] + dir_[2]), 1.0))
    for g in range(8):
        invi[0:1, g * 1024:(g + 1) * 1024] = v[g:g + 1, :]
    half_a = a.at[pl.ds(al(oc * ROWS, ROWS), ROWS), :]
    rcopy(half_a, half_a, xs.at[0], xr, sib).wait_recv()
    for i in range(3):
        dusend(i).wait_send()
        disend(i).wait_send()
    csend().wait_send()

    def s1(st, t, k):
        h = lax.rem(t, 2)
        to = dev(x + (1 - h) * (1 - 2 * x), y + h * (1 - 2 * y), c, z)
        return rcopy(part.at[t, k], r1.at[st, t, k], s1s.at[st, t, k], s1r.at[st, t, k], to)

    def s2(st, h, k):
        return rcopy(part.at[6 + h, k], r2.at[st, h, k], s2s.at[st, h, k], s2r.at[st, h, k], (yn, xn)[h])

    def chunk_rows(q, h, k):
        return pl.ds(al(q * STRIPE + h * HALF + k * CH, CH), CH)

    def ag(st, d, h, k):
        blk = panel.at[1 - st, chunk_rows(me, h, k)]
        return rcopy(blk, blk, ags.at[st, d, h, k], agr.at[st, d, h, k], (xn, yn)[d])

    def fw(st, h, k):
        q = (y * 2 + ox, oy * 2 + x)[h]
        blk = panel.at[1 - st, chunk_rows(q, h, k)]
        return rcopy(blk, blk, fws.at[st, h, k], fwr.at[st, h, k], (yn, xn)[h])

    def usib(st):
        return rcopy(upart.at[pl.ds(al(oc * ROWS, ROWS), ROWS)], ursib.at[st], usibs.at[st], usibr.at[st], sib)

    def uz(st):
        return rcopy(upart.at[pl.ds(al(c * ROWS + oz * UROWS, UROWS), UROWS)], urz.at[st],
                     uzs.at[st], uzr.at[st], zn)

    qh, qq = QUERIES // 2, QUERIES // 4
    quarter = pl.ds(al(c * qh + z * qq, qq), qq)

    def pq_sib():
        return rcopy(pkc.at[pl.ds(al(oc * qh, qh), qh)], pks, pqs.at[0], pqr.at[0], sib)

    def pq_z():
        return rcopy(pkc.at[pl.ds(al(c * qh + oz * qq, qq), qq)], pkz, pqs.at[1], pqr.at[1], zn)

    def pq_x(i):
        return rcopy(pkc.at[quarter], pkx.at[i], pqs.at[2 + i], pqr.at[2 + i], (xn, yn, dg)[i])

    def pq_a(i):
        return rcopy(pka.at[quarter], pka.at[quarter], pqs.at[5 + i], pqr.at[5 + i], (zn, sib, zsib)[i])

    def badd(u, v):
        return (u.astype(F32) + v.astype(F32)).astype(BF)

    def round_body(j, _):
        st = lax.rem(j, 2)
        last = j == LAYERS - 1
        more = j < LAYERS - 1
        for i in range(3):
            ua(j, i).wait_recv()

        def item_tile(t, _):
            h = lax.rem(t, 2)
            u = lax.div(t, 2)
            f1, f2 = 1 - lax.div(u, 2), lax.rem(u, 2)
            fx = (1 - h) * f1 + h * f2
            fy = (1 - h) * f2 + h * f1
            q = (y + fy - 2 * y * fy) * 2 + (x + fx - 2 * x * fx)
            base = al(q * STRIPE + h * HALF, HALF)

            @pl.when(j == 0)
            def _():
                def norm(g, _):
                    rsl = pl.ds(al(g * 128, 128), 128)
                    iu = upart[rsl, :]
                    for b in range(HALF // 128):
                        cc = pl.ds(al(base + b * 128, 128), 128)
                        a[rsl, cc] = a[rsl, cc] * (iu * invi[0:1, cc]).astype(BF)
                    return 0
                lax.fori_loop(0, 2 * ROWS // 128, norm, 0)

            res = dot(eut[j], a[:, pl.ds(base, HALF)], 1, 0)
            for k in range(NCH):
                part[t, k] = res[:, k * CH:(k + 1) * CH]

            @pl.when(t < 4)
            def _():
                for k in range(NCH):
                    s1(st, t, k).start()
            return 0

        lax.fori_loop(0, 8, item_tile, 0)

        @pl.when(j == 0)
        def _():
            for i in range(3):
                ei0(i).wait_recv()

        @pl.when(j > 0)
        def _():
            for k in range(NCH):
                ag(1 - st, 0, 1, k).wait_recv()
                ag(1 - st, 1, 0, k).wait_recv()
                fw(1 - st, 0, k).wait_recv()
                fw(1 - st, 1, k).wait_recv()

        def user_tile(i, _):
            b = lax.div(i, 2)
            rsl = pl.ds(al((b * c + (1 - b) * oc) * ROWS + lax.rem(i, 2) * UROWS, UROWS), UROWS)
            upart[rsl, :] = dot(a[rsl, :], panel[st], 1, 0)

            @pl.when(i == 1)
            def _():
                usib(st).start()
            return 0

        lax.fori_loop(0, 4, user_tile, 0)
        usib(st).wait_recv()
        mine = pl.ds(al(c * ROWS, ROWS), ROWS)
        upart[mine, :] = upart[mine, :] + ursib[st]
        uz(st).start()

        def stage1(k, _):
            for h in range(2):
                s1(st, 2 + h, k).wait_recv()
                part[6 + h, k] = part[6 + h, k] + r1[st, 2 + h, k]
                s1(st, h, k).wait_recv()
                part[4 + h, k] = part[4 + h, k] + r1[st, h, k]
                s2(st, h, k).start()
            return 0

        lax.fori_loop(0, NCH - 1, stage1, 0)

        uz(st).wait_recv()
        e = (upart[pl.ds(ucol, UROWS), :] + urz[st]).astype(BF).astype(F32)
        usum[...] = usum[...] + e

        @pl.when(more)
        def _():
            eut[j + 1, :, pl.ds(ucol, UROWS)] = e.T.astype(BF)
            for i in range(3):
                ua(j + 1, i).start()

        @pl.when(last)
        def _():
            fu = (usum[...] * (1.0 / (LAYERS + 1))).astype(BF)
            fu_ref[...] = fu
            ids = lax.broadcasted_iota(jnp.int32, (UROWS, QUERIES), 0) + (row * 2 + z) * UROWS
            hot = jnp.where(ids == q_ref[...], 1.0, 0.0).astype(BF)
            pkc[...] = dot(hot, fu, 0, 0).astype(BF)
            pq_sib().start()

        stage1(NCH - 1, 0)

        @pl.when(last)
        def _():
            pq_sib().wait_recv()
            hrows = pl.ds(al(c * qh, qh), qh)
            pkc[hrows, :] = badd(pkc[hrows, :], pks[...])
            pq_z().start()

        def stage2(k, _):
            for h in range(2):
                s2(st, h, k).wait_recv()
                e = (part[4 + h, k] + r2[st, h, k]).T.astype(BF)
                rsl = chunk_rows(me, h, k)

                @pl.when(more)
                def _():
                    panel[1 - st, rsl, :] = e
                    ag(st, 0, h, k).start()
                    ag(st, 1, h, k).start()

                @pl.when(last)
                def _():
                    loc = pl.ds(al(h * HALF + k * CH, CH), CH)
                    tot = ie_ref[loc, :].astype(F32) + panel[1, rsl, :].astype(F32)
                    tot = tot + panel[0, rsl, :].astype(F32) + e.astype(F32)
                    fi_ref[loc, :] = (tot * (1.0 / (LAYERS + 1))).astype(BF)
            return 0

        stage2(0, 0)

        @pl.when(last)
        def _():
            pq_z().wait_recv()
            pkc[quarter, :] = badd(pkc[quarter, :], pkz[...])
            for i in range(3):
                pq_x(i).start()

        lax.fori_loop(1, NCH, stage2, 0)

        @pl.when(more)
        def _():
            def forward(k, _):
                ag(st, 0, 0, k).wait_recv()
                fw(st, 0, k).start()
                ag(st, 1, 1, k).wait_recv()
                fw(st, 1, k).start()
                return 0
            lax.fori_loop(0, NCH, forward, 0)

        usib(st).wait_send()
        uz(st).wait_send()
        for i in range(3):
            ua(j, i).wait_send()
        for k in range(NCH):
            for t in range(4):
                s1(st, t, k).wait_send()
            for h in range(2):
                s2(st, h, k).wait_send()

        @pl.when(j > 0)
        def _():
            for k in range(NCH):
                for h in range(2):
                    ag(1 - st, 0, h, k).wait_send()
                    ag(1 - st, 1, h, k).wait_send()
                    fw(1 - st, h, k).wait_send()
        return 0

    lax.fori_loop(0, LAYERS, round_body, 0)

    for i in range(3):
        ei0(i).wait_send()
        pq_x(i).wait_recv()
    tot = badd(badd(pkc[quarter, :], pkx[0]), badd(pkx[1], pkx[2]))
    pka[quarter, :] = tot
    for i in range(3):
        pq_a(i).start()
    pq_sib().wait_send()
    pq_z().wait_send()
    for i in range(3):
        pq_x(i).wait_send()
        pq_a(i).wait_recv()
    pk_ref[...] = pka[...]
    for i in range(3):
        pq_a(i).wait_send()


def propagate(mask_blk, user_shard, item_shard, queries):
    vm = pl.BlockSpec(memory_space=pltpu.VMEM)
    dma = pltpu.SemaphoreType.DMA
    qh, qq = QUERIES // 2, QUERIES // 4
    scratch = [
        pltpu.VMEM((2 * ROWS, COLS), BF),
        pltpu.VMEM((8, NCH, EMB, CH), F32),
        pltpu.VMEM((2, 4, NCH, EMB, CH), F32),
        pltpu.VMEM((2, 2, NCH, EMB, CH), F32),
        pltpu.VMEM((2, COLS, EMB), BF),
        pltpu.VMEM((LAYERS, EMB, 2 * ROWS), BF),
        pltpu.VMEM((2 * ROWS, EMB), F32),
        pltpu.VMEM((2, ROWS, EMB), F32),
        pltpu.VMEM((2, UROWS, EMB), F32),
        pltpu.VMEM((1, COLS), F32),
        pltpu.VMEM((NLOAD, LROWS, STRIPE), jnp.int32),
        pltpu.VMEM((NSTAGE, LROWS, STRIPE), BF),
        pltpu.VMEM((2, 8, COLS), F32),
        pltpu.VMEM((8, COLS), F32),
        pltpu.VMEM((8, ROWS), F32),
        pltpu.VMEM((3, 8, ROWS), F32),
        pltpu.VMEM((8, COLS // 8), F32),
        pltpu.VMEM((3, 8, COLS // 8), F32),
        pltpu.VMEM((UROWS, EMB), F32),
        pltpu.VMEM((QUERIES, EMB), BF),
        pltpu.VMEM((qh, EMB), BF),
        pltpu.VMEM((qq, EMB), BF),
        pltpu.VMEM((3, qq, EMB), BF),
        pltpu.VMEM((QUERIES, EMB), BF),
        dma((NLOAD,)), dma((NSTAGE,)), dma,
        dma((2, 4, NCH)), dma((2, 4, NCH)),
        dma((2, 2, NCH)), dma((2, 2, NCH)),
        dma((2, 2, 2, NCH)), dma((2, 2, 2, NCH)),
        dma((2, 2, NCH)), dma((2, 2, NCH)),
        dma((2,)), dma((2,)), dma((2,)), dma((2,)),
        dma((LAYERS, 3)), dma((LAYERS, 3)),
        dma((3,)), dma((3,)), dma((7,)), dma((7,)), dma((8,)), dma((8,)),
    ]
    return pl.pallas_call(
        kernel,
        out_shape=(jax.ShapeDtypeStruct((UROWS, EMB), BF),
                   jax.ShapeDtypeStruct((STRIPE, EMB), BF),
                   jax.ShapeDtypeStruct((QUERIES, EMB), BF)),
        in_specs=[pl.BlockSpec(memory_space=pl.ANY), vm, vm, vm],
        out_specs=(vm, vm, vm),
        scratch_shapes=scratch,
        compiler_params=pltpu.CompilerParams(collective_id=0, has_side_effects=True,
                                             vmem_limit_bytes=67043328),
        name='propagate',
    )(mask_blk, user_shard, item_shard, queries)


def solution(mesh):
    def device_step(mask_blk, user_shard, item_shard, queries):
        fu, fi, picked = propagate(mask_blk, user_shard, item_shard, queries.reshape(1, QUERIES))
        scores = lax.dot_general(picked, fi, (((1,), (1,)), ((), ())), preferred_element_type=F32)
        return fu, fi, scores

    return jax.shard_map(
        device_step, mesh=mesh,
        in_specs=(P('row', 'col'), P(('row', 'col'), None), P(('col', 'row'), None), P()),
        out_specs=(P(('row', 'col'), None), P(('col', 'row'), None), P(None, ('col', 'row'))),
        check_vma=False)
```

```python
import functools

import jax
import jax.numpy as jnp
from jax import lax
from jax.experimental import pallas as pl
from jax.experimental.pallas import tpu as pltpu
from jax.sharding import PartitionSpec as P

LAYERS = 3
BF = jnp.bfloat16
F32 = jnp.float32
EMB = 128
ROWS = 1024
STRIPE = 2048
CHIPS = 4
COLS = STRIPE * CHIPS
UROWS = 512
HALF = STRIPE // 2
NCH = 4
CH = HALF // NCH
LROWS = 128
NLOAD = 6
NSTAGE = 8
QUERIES = 1024


def al(v, m):
    return pl.multiple_of(v, m)


def dot(a, b, ca, cb):
    return lax.dot_general(a, b, (((ca,), (cb,)), ((), ())), preferred_element_type=F32)


def kernel(mask_ref, ue_ref, ie_ref, q_ref, fu_ref, fi_ref, pk_ref,
           a, part, r1, r2, panel, eut, upart, ursib, urz, invi, mbuf, stage,
           cs, dcs, dcr, dus, dur, usum, pkc, pks, pkz, pkx, pka,
           lsem, xs, xr, s1s, s1r, s2s, s2r, ags, agr, fws, fwr,
           usibs, usibr, uzs, uzr, uas, uar, eis, eir, dgs, dgr, dvs, dvr, pqs, pqr):
    row = lax.axis_index('row')
    z = lax.axis_index('col')
    c = lax.rem(row, 2)
    x = lax.rem(lax.div(row, 2), 2)
    y = lax.div(row, 4)
    me = y * 2 + x

    def dev(xx, yy, cc, zz):
        return {'row': (yy * 2 + xx) * 2 + cc, 'col': zz}

    ox, oy, oc, oz = 1 - x, 1 - y, 1 - c, 1 - z
    xn, yn, dg = dev(ox, y, c, z), dev(x, oy, c, z), dev(ox, oy, c, z)
    zn, sib, zsib = dev(x, y, c, oz), dev(x, y, oc, z), dev(x, y, oc, oz)
    xnc, ync, dgc = dev(ox, y, oc, z), dev(x, oy, oc, z), dev(ox, oy, oc, z)

    def rcopy(src, dst, ss, rs, to):
        return pltpu.make_async_remote_copy(src_ref=src, dst_ref=dst, send_sem=ss, recv_sem=rs,
                                            device_id=to, device_id_type=pl.DeviceIdType.MESH)

    barrier = pltpu.get_barrier_semaphore()
    peers = (xn, yn, dg, zn, sib, zsib, xnc, ync, dgc)
    for peer in peers:
        pl.semaphore_signal(barrier, inc=1, device_id=peer, device_id_type=pl.DeviceIdType.MESH)

    n_group = ROWS // LROWS
    n_load = n_group * 2 * CHIPS

    def stripe(i):
        fx = 1 - lax.rem(i, 2)
        fy = lax.rem(lax.div(i + 1, 2), 2)
        return (y + fy - 2 * y * fy) * 2 + (x + fx - 2 * x * fx)

    def load_at(i, rg, par, n):
        s = 2 * stripe(i) + par * c + (1 - par) * oc
        slot = lax.rem(n, NLOAD)
        return pltpu.make_async_copy(
            mask_ref.at[pl.ds(al(rg * LROWS, LROWS), LROWS), pl.ds(al(s * STRIPE, STRIPE), STRIPE)],
            mbuf.at[slot], lsem.at[slot])

    def load(n):
        first = 1 - lax.min(lax.div(n, 2 * n_group), 1)
        i = lax.div(n, 2 * n_group)
        w = lax.rem(n, 2 * n_group)
        rg = first * lax.rem(w, n_group) + (1 - first) * lax.div(w, 2)
        par = first * (1 - lax.div(w, n_group)) + (1 - first) * lax.rem(w, 2)
        return load_at(i, rg, par, n)

    for n in range(NLOAD):
        load(jnp.int32(n)).start()

    ucol = al(c * ROWS + z * UROWS, UROWS)
    usum[...] = ue_ref[...].astype(F32)
    eut[0, :, pl.ds(ucol, UROWS)] = ue_ref[...].astype(F32).T.astype(BF)
    own_rows = pl.ds(al(me * STRIPE, STRIPE), STRIPE)
    panel[0, own_rows, :] = ie_ref[...]
    cs[...] = jnp.zeros_like(cs)
    upart[pl.ds(0, ROWS), :] = jnp.zeros((ROWS, EMB), F32)

    def count(i, rg, par, n, sslot):
        p = stripe(i)
        slot = lax.rem(n, NLOAD)
        load_at(i, rg, par, n).wait()
        cols = pl.ds(al(p * STRIPE, STRIPE), STRIPE)
        acc = jnp.zeros((8, STRIPE), F32)
        for g in range(LROWS // 16):
            v = mbuf[slot, g * 16:(g + 1) * 16, :].astype(F32)
            b = v.astype(BF)
            if par == 0:
                stage[sslot, g * 16:(g + 1) * 16, :] = b
            else:
                a[pl.ds(al(c * ROWS + rg * LROWS + g * 16, 16), 16), cols] = b
            acc = acc + v[0:8] + v[8:16]
            parts = [v[:, q * 128:(q + 1) * 128] for q in range(STRIPE // 128)]
            while len(parts) > 1:
                parts = [parts[q] + parts[q + 1] for q in range(0, len(parts), 2)]
            rsl = pl.ds(al(rg * LROWS + g * 16, 16), 16)
            upart[rsl, :] = upart[rsl, :] + parts[0]
        cs[par] = cs[par] + acc

        @pl.when(n + NLOAD < n_load)
        def _():
            load(n + NLOAD).start()

    def xcopy(i, rg):
        slot = lax.rem(i * n_group + rg, NSTAGE)
        return rcopy(stage.at[slot],
                     a.at[pl.ds(al(c * ROWS + rg * LROWS, LROWS), LROWS), pl.ds(al(stripe(i) * STRIPE, STRIPE), STRIPE)],
                     xs.at[slot], xr.at[i], sib)

    def dgsend(p, i):
        return rcopy(dcs.at[(1, 1, 1, 0, 0, 0, 0)[i], p], dcr.at[i, p], dgs.at[i, p], dgr.at[i, p],
                     (xn, yn, dg, sib, xnc, ync, dgc)[i])

    def dusend(i):
        return rcopy(dus, dur.at[i], dvs.at[i], dvr.at[i], (zn, sib, zsib)[i])

    def stripe_degrees(i):
        p = stripe(i)
        for par in range(2):
            v = jnp.sum(cs[par], axis=0, keepdims=True)
            for g in range(8):
                dcs[par, p, g:g + 1, :] = v[:, g * 256:(g + 1) * 256]
        cs[...] = jnp.zeros_like(cs)
        for k in range(7):
            dgsend(p, k).start()

    def own_first(rg, _):
        count(0, rg, 1, rg, 0)
        return 0

    lax.fori_loop(0, n_group, own_first, 0)
    pl.semaphore_wait(barrier, len(peers))

    def ei0(i):
        return rcopy(ie_ref, panel.at[0, own_rows], eis.at[i], eir.at[i], (xn, yn, dg)[i])

    def ua(j, i):
        blk = eut.at[j, :, pl.ds(ucol, UROWS)]
        return rcopy(blk, blk, uas.at[j, i], uar.at[j, i], (zn, sib, zsib)[i])

    def sib_first(rg, _):
        count(0, rg, 0, n_group + rg, rg)
        xcopy(0, rg).start()
        return 0

    lax.fori_loop(0, n_group, sib_first, 0)
    for i in range(3):
        ei0(i).start()
    for i in range(3):
        ua(0, i).start()
    stripe_degrees(0)

    def mask_step(m, _):
        i = lax.div(m, n_group)
        rg = lax.rem(m, n_group)
        xcopy(i - 1, rg).wait_send()
        count(i, rg, 0, 2 * m, rg)
        xcopy(i, rg).start()
        count(i, rg, 1, 2 * m + 1, 0)

        @pl.when(i == CHIPS - 1)
        def _():
            rsl = pl.ds(al(rg * LROWS, LROWS), LROWS)
            v = jnp.sum(upart[rsl, :].T, axis=0, keepdims=True)
            dus[:, rsl] = jnp.broadcast_to(v, (8, LROWS))

        @pl.when(rg == n_group - 1)
        def _():
            stripe_degrees(i)
        return 0

    lax.fori_loop(n_group, CHIPS * n_group, mask_step, 0)

    for i in range(3):
        dusend(i).start()

    def stripe_inverse(i):
        p = stripe(i)
        for k in range(7):
            dgsend(p, k).wait_recv()
        v = dcs[1, p]
        for k in range(7):
            v = v + dcr[k, p]
        v = lax.rsqrt(jnp.maximum(v, 1.0))
        for g in range(8):
            invi[0:1, pl.ds(al(p * STRIPE + g * 256, 256), 256)] = v[g:g + 1, :]

    def swapped(i):
        region = a.at[pl.ds(al(oc * ROWS, ROWS), ROWS), pl.ds(al(stripe(i) * STRIPE, STRIPE), STRIPE)]
        rcopy(region, region, xs.at[0], xr.at[i], sib).wait_recv()

    for i in range(3):
        stripe_inverse(i)
    for i in range(3):
        dusend(i).wait_recv()
    for blk, v in ((c, dus[...] + dur[0]), (oc, dur[1] + dur[2])):
        v = lax.rsqrt(jnp.maximum(v, 1.0))
        for b in range(ROWS // 128):
            w = jnp.broadcast_to(v[0:1, b * 128:(b + 1) * 128], (128, 128))
            upart[pl.ds(al(blk * ROWS + b * 128, 128), 128), :] = w.T
    for i in range(3):
        swapped(i)

    def tile_q(t):
        h = lax.rem(t, 2)
        u = lax.div(t, 2)
        f1, f2 = 1 - lax.div(u, 2), lax.rem(lax.div(u + 1, 2), 2)
        fx = (1 - h) * f1 + h * f2
        fy = (1 - h) * f2 + h * f1
        return (y + fy - 2 * y * fy) * 2 + (x + fx - 2 * x * fx)

    def s1(st, t, k):
        h = lax.rem(t, 2)
        to = dev(x + (1 - h) * (1 - 2 * x), y + h * (1 - 2 * y), c, z)
        return rcopy(part.at[t, k], r1.at[t, k], s1s.at[st, t, k], s1r.at[st, t, k], to)

    def s2(st, h, k):
        return rcopy(part.at[4 + h, k], r2.at[h, k], s2s.at[st, h, k], s2r.at[st, h, k], (yn, xn)[h])

    def chunk_rows(q, h, k):
        return pl.ds(al(q * STRIPE + h * HALF + k * CH, CH), CH)

    def ag(st, d, h, k):
        blk = panel.at[1 - st, chunk_rows(me, h, k)]
        return rcopy(blk, blk, ags.at[st, d, h, k], agr.at[st, d, h, k], (xn, yn)[d])

    def fw(st, h, k):
        q = (y * 2 + ox, oy * 2 + x)[h]
        blk = panel.at[1 - st, chunk_rows(q, h, k)]
        return rcopy(blk, blk, fws.at[st, h, k], fwr.at[st, h, k], (yn, xn)[h])

    def usib(j):
        return rcopy(upart.at[pl.ds(al(oc * ROWS, ROWS), ROWS)], ursib, usibs.at[j], usibr.at[j], sib)

    def uz(j):
        return rcopy(upart.at[pl.ds(al(c * ROWS + oz * UROWS, UROWS), UROWS)], urz,
                     uzs.at[j], uzr.at[j], zn)

    qh, qq = QUERIES // 2, QUERIES // 4
    quarter = pl.ds(al(c * qh + z * qq, qq), qq)

    def pq_sib():
        return rcopy(pkc.at[pl.ds(al(oc * qh, qh), qh)], pks, pqs.at[0], pqr.at[0], sib)

    def pq_z():
        return rcopy(pkc.at[pl.ds(al(c * qh + oz * qq, qq), qq)], pkz, pqs.at[1], pqr.at[1], zn)

    def pq_x(i):
        return rcopy(pkc.at[quarter], pkx.at[i], pqs.at[2 + i], pqr.at[2 + i], (xn, yn, dg)[i])

    def pq_a(i):
        return rcopy(pka.at[quarter], pka.at[quarter], pqs.at[5 + i], pqr.at[5 + i], (zn, sib, zsib)[i])

    def badd(u, v):
        return (u.astype(F32) + v.astype(F32)).astype(BF)

    def normalise(base, width):
        def norm(g, _):
            rsl = pl.ds(al(g * 128, 128), 128)
            iu = upart[rsl, :]
            for b in range(width // 128):
                cc = pl.ds(al(base + b * 128, 128), 128)
                a[rsl, cc] = a[rsl, cc] * (iu * invi[0:1, cc]).astype(BF)
            return 0
        lax.fori_loop(0, 2 * ROWS // 128, norm, 0)

    for j in range(LAYERS):
        st = j % 2
        last = j == LAYERS - 1
        for i in range(3):
            ua(j, i).wait_recv()

        def item_tile(t, _):
            base = al(tile_q(t) * STRIPE + lax.rem(t, 2) * HALF, HALF)
            if j == 0:
                normalise(base, HALF)
            res = dot(eut[j], a[:, pl.ds(base, HALF)], 1, 0)
            for k in range(NCH):
                part[t, k] = res[:, k * CH:(k + 1) * CH]
            return 0

        def send_tile(t, _):
            item_tile(t, 0)
            for k in range(NCH):
                s1(st, t, k).start()
            return 0

        def first_chunk(n, _):
            t = lax.rem(n, 2)
            k = lax.div(n, 2)
            base = al(tile_q(t) * STRIPE + t * HALF + k * CH, CH)
            normalise(base, CH)
            part[t, k] = dot(eut[j], a[:, pl.ds(base, CH)], 1, 0)
            s1(st, t, k).start()
            return 0

        def stage1(k, _):
            for h in range(2):
                s1(st, 2 + h, k).wait_recv()
                part[4 + h, k] = part[4 + h, k] + r1[2 + h, k]
                s1(st, h, k).wait_recv()
                part[6 + h, k] = part[6 + h, k] + r1[h, k]
                s2(st, h, k).start()
            return 0

        def stage2(k, _):
            for h in range(2):
                s2(st, h, k).wait_recv()
                e = (part[6 + h, k] + r2[h, k]).T.astype(BF)
                rsl = chunk_rows(me, h, k)
                if last:
                    loc = pl.ds(al(h * HALF + k * CH, CH), CH)
                    tot = ie_ref[loc, :].astype(F32) + panel[1, rsl, :].astype(F32)
                    tot = tot + panel[0, rsl, :].astype(F32) + e.astype(F32)
                    fi_ref[loc, :] = (tot * (1.0 / (LAYERS + 1))).astype(BF)
                else:
                    panel[1 - st, rsl, :] = e
                    ag(st, 0, h, k).start()
                    ag(st, 1, h, k).start()
            return 0

        def forward(k, _):
            ag(st, 0, 0, k).wait_recv()
            fw(st, 0, k).start()
            ag(st, 1, 1, k).wait_recv()
            fw(st, 1, k).start()
            return 0

        def user_near(i, _):
            rsl = pl.ds(al(i * UROWS, UROWS), UROWS)
            tot = None
            for q in (me, y * 2 + ox, oy * 2 + x):
                ks = pl.ds(al(q * STRIPE, STRIPE), STRIPE)
                d = dot(a[rsl, ks], panel[st, ks, :], 1, 0)
                tot = d if tot is None else tot + d
            upart[rsl, :] = tot
            return 0

        def user_far(i, _):
            b = lax.div(i, 2)
            rsl = pl.ds(al((b * c + (1 - b) * oc) * ROWS + lax.rem(i, 2) * UROWS, UROWS), UROWS)
            ks = pl.ds(al((oy * 2 + ox) * STRIPE, STRIPE), STRIPE)
            upart[rsl, :] = upart[rsl, :] + dot(a[rsl, ks], panel[st, ks, :], 1, 0)

            @pl.when(i == 1)
            def _():
                usib(j).start()
            return 0

        def users():
            if j == 0:
                for i in range(3):
                    ei0(i).wait_recv()
            else:
                for k in range(NCH):
                    ag(1 - st, 0, 1, k).wait_recv()
                    ag(1 - st, 1, 0, k).wait_recv()
            lax.fori_loop(0, 4, user_near, 0)
            if j > 0:
                for k in range(NCH):
                    fw(1 - st, 0, k).wait_recv()
                    fw(1 - st, 1, k).wait_recv()
            lax.fori_loop(0, 4, user_far, 0)
            usib(j).wait_recv()
            mine = pl.ds(al(c * ROWS, ROWS), ROWS)
            upart[mine, :] = upart[mine, :] + ursib[...]
            uz(j).start()

        def user_final():
            uz(j).wait_recv()
            e = (upart[pl.ds(ucol, UROWS), :] + urz[...]).astype(BF).astype(F32)
            usum[...] = usum[...] + e
            if not last:
                eut[j + 1, :, pl.ds(ucol, UROWS)] = e.T.astype(BF)
                for i in range(3):
                    ua(j + 1, i).start()
                return
            fu = (usum[...] * (1.0 / (LAYERS + 1))).astype(BF)
            fu_ref[...] = fu
            ids = lax.broadcasted_iota(jnp.int32, (UROWS, QUERIES), 0) + (row * 2 + z) * UROWS
            hot = jnp.where(ids == q_ref[...], 1.0, 0.0).astype(BF)
            pkc[...] = dot(hot, fu, 0, 0).astype(BF)
            pq_sib().start()

        if j == 0:
            lax.fori_loop(0, 2 * NCH, first_chunk, 0)
            lax.fori_loop(2, 4, send_tile, 0)
            lax.fori_loop(4, 6, item_tile, 0)
            swapped(3)
            stripe_inverse(3)
            lax.fori_loop(6, 8, item_tile, 0)
            lax.fori_loop(0, NCH - 1, stage1, 0)
            users()
            stage1(NCH - 1, 0)
            lax.fori_loop(0, NCH, stage2, 0)
            user_final()
        else:
            lax.fori_loop(0, 4, send_tile, 0)
            users()
            lax.fori_loop(4, 8, item_tile, 0)
            lax.fori_loop(0, 2, stage1, 0)
            user_final()
            if last:
                pq_sib().wait_recv()
                hrows = pl.ds(al(c * qh, qh), qh)
                pkc[hrows, :] = badd(pkc[hrows, :], pks[...])
                pq_z().start()
                pq_z().wait_recv()
                pkc[quarter, :] = badd(pkc[quarter, :], pkz[...])
                for i in range(3):
                    pq_x(i).start()
            lax.fori_loop(2, NCH, stage1, 0)
            lax.fori_loop(0, NCH - 1, stage2, 0)
            if last:
                for i in range(3):
                    pq_x(i).wait_recv()
                pka[quarter, :] = badd(badd(pkc[quarter, :], pkx[0]), badd(pkx[1], pkx[2]))
                for i in range(3):
                    pq_a(i).start()
            stage2(NCH - 1, 0)
        if not last:
            lax.fori_loop(0, NCH, forward, 0)

        usib(j).wait_send()
        uz(j).wait_send()
        for i in range(3):
            ua(j, i).wait_send()
        for k in range(NCH):
            for t in range(4):
                s1(st, t, k).wait_send()
            for h in range(2):
                s2(st, h, k).wait_send()
        if j == 0:
            def drain_degrees(p, _):
                for k in range(7):
                    dgsend(p, k).wait_send()
                return 0
            lax.fori_loop(0, CHIPS, drain_degrees, 0)

            def drain_swap(rg, _):
                xcopy(CHIPS - 1, rg).wait_send()
                return 0
            lax.fori_loop(0, n_group, drain_swap, 0)
            for i in range(3):
                dusend(i).wait_send()
                ei0(i).wait_send()
        else:
            for k in range(NCH):
                for h in range(2):
                    ag(1 - st, 0, h, k).wait_send()
                    ag(1 - st, 1, h, k).wait_send()
                    fw(1 - st, h, k).wait_send()

    pq_sib().wait_send()
    pq_z().wait_send()
    for i in range(3):
        pq_x(i).wait_send()
        pq_a(i).wait_recv()
    pk_ref[...] = pka[...]
    for i in range(3):
        pq_a(i).wait_send()


def score_kernel(fu_ref, fi_ref, pk_ref, fu_out, fi_out, s_out):
    fu_out[...] = fu_ref[...]
    fi_out[...] = fi_ref[...]
    s_out[...] = dot(pk_ref[...], fi_ref[...], 1, 1)


def scores_of(fu, fi, picked):
    width = 256
    whole = lambda shape: pl.BlockSpec(shape, lambda i: (0, 0))
    return pl.pallas_call(
        score_kernel,
        grid=(STRIPE // width,),
        out_shape=(jax.ShapeDtypeStruct(fu.shape, BF), jax.ShapeDtypeStruct(fi.shape, BF),
                   jax.ShapeDtypeStruct((QUERIES, STRIPE), F32)),
        in_specs=[whole((UROWS, EMB)), pl.BlockSpec((width, EMB), lambda i: (i, 0)), whole((QUERIES, EMB))],
        out_specs=(whole((UROWS, EMB)), pl.BlockSpec((width, EMB), lambda i: (i, 0)),
                   pl.BlockSpec((QUERIES, width), lambda i: (0, i))),
        name='scores',
    )(fu, fi, picked)


def propagate(mask_blk, user_shard, item_shard, queries):
    vm = pl.BlockSpec(memory_space=pltpu.VMEM)
    dma = pltpu.SemaphoreType.DMA
    qh, qq = QUERIES // 2, QUERIES // 4
    scratch = [
        pltpu.VMEM((2 * ROWS, COLS), BF),
        pltpu.VMEM((8, NCH, EMB, CH), F32),
        pltpu.VMEM((4, NCH, EMB, CH), F32),
        pltpu.VMEM((2, NCH, EMB, CH), F32),
        pltpu.VMEM((2, COLS, EMB), BF),
        pltpu.VMEM((LAYERS, EMB, 2 * ROWS), BF),
        pltpu.VMEM((2 * ROWS, EMB), F32),
        pltpu.VMEM((ROWS, EMB), F32),
        pltpu.VMEM((UROWS, EMB), F32),
        pltpu.VMEM((1, COLS), F32),
        pltpu.VMEM((NLOAD, LROWS, STRIPE), jnp.int32),
        pltpu.VMEM((NSTAGE, LROWS, STRIPE), BF),
        pltpu.VMEM((2, 8, STRIPE), F32),
        pltpu.VMEM((2, CHIPS, 8, STRIPE // 8), F32),
        pltpu.VMEM((7, CHIPS, 8, STRIPE // 8), F32),
        pltpu.VMEM((8, ROWS), F32),
        pltpu.VMEM((3, 8, ROWS), F32),
        pltpu.VMEM((UROWS, EMB), F32),
        pltpu.VMEM((QUERIES, EMB), BF),
        pltpu.VMEM((qh, EMB), BF),
        pltpu.VMEM((qq, EMB), BF),
        pltpu.VMEM((3, qq, EMB), BF),
        pltpu.VMEM((QUERIES, EMB), BF),
        dma((NLOAD,)), dma((NSTAGE,)), dma((CHIPS,)),
        dma((2, 4, NCH)), dma((2, 4, NCH)),
        dma((2, 2, NCH)), dma((2, 2, NCH)),
        dma((2, 2, 2, NCH)), dma((2, 2, 2, NCH)),
        dma((2, 2, NCH)), dma((2, 2, NCH)),
        dma((LAYERS,)), dma((LAYERS,)), dma((LAYERS,)), dma((LAYERS,)),
        dma((LAYERS, 3)), dma((LAYERS, 3)),
        dma((3,)), dma((3,)), dma((7, CHIPS)), dma((7, CHIPS)), dma((3,)), dma((3,)), dma((8,)), dma((8,)),
    ]
    return pl.pallas_call(
        kernel,
        out_shape=(jax.ShapeDtypeStruct((UROWS, EMB), BF),
                   jax.ShapeDtypeStruct((STRIPE, EMB), BF),
                   jax.ShapeDtypeStruct((QUERIES, EMB), BF)),
        in_specs=[pl.BlockSpec(memory_space=pl.ANY), vm, vm, vm],
        out_specs=(vm, vm, vm),
        scratch_shapes=scratch,
        compiler_params=pltpu.CompilerParams(collective_id=0, has_side_effects=True,
                                             vmem_limit_bytes=67043328),
        name='propagate',
    )(mask_blk, user_shard, item_shard, queries)


def solution(mesh):
    def device_step(mask_blk, user_shard, item_shard, queries):
        fu, fi, picked = propagate(mask_blk, user_shard, item_shard, queries.reshape(1, QUERIES))
        return scores_of(fu, fi, picked)

    return jax.shard_map(
        device_step, mesh=mesh,
        in_specs=(P('row', 'col'), P(('row', 'col'), None), P(('col', 'row'), None), P()),
        out_specs=(P(('row', 'col'), None), P(('col', 'row'), None), P(None, ('col', 'row'))),
        check_vma=False)
```

```python
import functools

import jax
import jax.numpy as jnp
from jax import lax
from jax.experimental import pallas as pl
from jax.experimental.pallas import tpu as pltpu
from jax.sharding import PartitionSpec as P

LAYERS = 3
BF = jnp.bfloat16
F32 = jnp.float32
EMB = 128
ROWS = 1024
STRIPE = 2048
CHIPS = 4
COLS = STRIPE * CHIPS
UROWS = 512
HALF = STRIPE // 2
NCH = 4
CH = HALF // NCH
LROWS = 128
NLOAD = 6
NSTAGE = 11
N_HELD = 8
QUERIES = 1024
SROWS = 128


def al(v, m):
    return pl.multiple_of(v, m)


def dot(a, b, ca, cb):
    return lax.dot_general(a, b, (((ca,), (cb,)), ((), ())), preferred_element_type=F32)


def kernel(mask_ref, ue_hbm, ie_hbm, q_hbm, fu_hbm, fi_hbm, pk_hbm, ue_ref, ie_ref, q_ref, fu_ref, fi_ref, pkf,
           a, part, r1, r2, panel, eut, upart, ursib, urz, invi, mbuf, stage,
           cs, dcs, dcr, dus, dur, usum, pkc, pks, pkz, pkx, pka,
           lsem, xs, xr, s1s, s1r, s2s, s2r, ags, agr, fws, fwr,
           usibs, usibr, uzs, uzr, uas, uar, eis, eir, dgs, dgr, dvs, dvr, pqs, pqr, ins, outs, fis):
    row = lax.axis_index('row')
    z = lax.axis_index('col')
    c = lax.rem(row, 2)
    x = lax.rem(lax.div(row, 2), 2)
    y = lax.div(row, 4)
    me = y * 2 + x

    def dev(xx, yy, cc, zz):
        return {'row': (yy * 2 + xx) * 2 + cc, 'col': zz}

    ox, oy, oc, oz = 1 - x, 1 - y, 1 - c, 1 - z
    xn, yn, dg = dev(ox, y, c, z), dev(x, oy, c, z), dev(ox, oy, c, z)
    zn, sib, zsib = dev(x, y, c, oz), dev(x, y, oc, z), dev(x, y, oc, oz)
    xnc, ync, dgc = dev(ox, y, oc, z), dev(x, oy, oc, z), dev(ox, oy, oc, z)

    def rcopy(src, dst, ss, rs, to):
        return pltpu.make_async_remote_copy(src_ref=src, dst_ref=dst, send_sem=ss, recv_sem=rs,
                                            device_id=to, device_id_type=pl.DeviceIdType.MESH)

    barrier = pltpu.get_barrier_semaphore()
    peers = (xn, yn, dg, zn, sib, zsib, xnc, ync, dgc)
    for peer in peers:
        pl.semaphore_signal(barrier, inc=1, device_id=peer, device_id_type=pl.DeviceIdType.MESH)

    n_group = ROWS // LROWS
    n_load = n_group * 2 * CHIPS

    def stripe(i):
        fx = 1 - lax.rem(i, 2)
        fy = lax.rem(lax.div(i + 1, 2), 2)
        return (y + fy - 2 * y * fy) * 2 + (x + fx - 2 * x * fx)

    def load_at(i, rg, par, n):
        s = 2 * stripe(i) + par * c + (1 - par) * oc
        slot = lax.rem(n, NLOAD)
        return pltpu.make_async_copy(
            mask_ref.at[pl.ds(al(rg * LROWS, LROWS), LROWS), pl.ds(al(s * STRIPE, STRIPE), STRIPE)],
            mbuf.at[slot], lsem.at[slot])

    def load(n):
        first = 1 - lax.min(lax.div(n, 2 * n_group), 1)
        i = lax.div(n, 2 * n_group)
        w = lax.rem(n, 2 * n_group)
        rg = first * lax.rem(w, n_group) + (1 - first) * lax.div(w, 2)
        par = first * (1 - lax.div(w, n_group)) + (1 - first) * lax.rem(w, 2)
        return load_at(i, rg, par, n)

    inputs = [pltpu.make_async_copy(src, dst, ins.at[i])
              for i, (src, dst) in enumerate(((ie_hbm, ie_ref), (ue_hbm, ue_ref), (q_hbm, q_ref)))]
    for cp in inputs:
        cp.start()
    for n in range(NLOAD):
        load(jnp.int32(n)).start()
    cs[...] = jnp.zeros_like(cs)
    upart[pl.ds(0, ROWS), :] = jnp.zeros((ROWS, EMB), F32)
    ucol = al(c * ROWS + z * UROWS, UROWS)

    def count(i, rg, par, n, sslot):
        p = stripe(i)
        slot = lax.rem(n, NLOAD)
        load_at(i, rg, par, n).wait()
        cols = pl.ds(al(p * STRIPE, STRIPE), STRIPE)
        acc = jnp.zeros((8, STRIPE), F32)
        for g in range(LROWS // 16):
            v = mbuf[slot, g * 16:(g + 1) * 16, :].astype(F32)
            b = v.astype(BF)
            if par == 0:
                stage[sslot, g * 16:(g + 1) * 16, :] = b
            else:
                a[pl.ds(al(c * ROWS + rg * LROWS + g * 16, 16), 16), cols] = b
            acc = acc + v[0:8] + v[8:16]
            parts = [v[:, q * 128:(q + 1) * 128] for q in range(STRIPE // 128)]
            while len(parts) > 1:
                parts = [parts[q] + parts[q + 1] for q in range(0, len(parts), 2)]
            rsl = pl.ds(al(rg * LROWS + g * 16, 16), 16)
            upart[rsl, :] = upart[rsl, :] + parts[0]
        cs[par] = cs[par] + acc

        @pl.when(n + NLOAD < n_load)
        def _():
            load(n + NLOAD).start()

    def xcopy(m):
        i = lax.div(m, n_group)
        rg = lax.rem(m, n_group)
        slot = lax.rem(m, NSTAGE)
        return rcopy(stage.at[slot],
                     a.at[pl.ds(al(c * ROWS + rg * LROWS, LROWS), LROWS), pl.ds(al(stripe(i) * STRIPE, STRIPE), STRIPE)],
                     xs.at[slot], xr.at[i], sib)

    def dgsend(p, i):
        return rcopy(dcs.at[(1, 1, 1, 0, 0, 0, 0)[i], p], dcr.at[i, p], dgs, dgr,
                     (xn, yn, dg, sib, xnc, ync, dgc)[i])

    def dusend(i):
        return rcopy(dus, dur.at[i], dvs, dvr, (zn, sib, zsib)[i])

    def stripe_degrees(i):
        p = stripe(i)
        for par in range(2):
            v = jnp.sum(cs[par], axis=0, keepdims=True)
            for g in range(8):
                dcs[par, p, g:g + 1, :] = v[:, g * 256:(g + 1) * 256]
        cs[...] = jnp.zeros_like(cs)
        for k in range(7):
            dgsend(p, k).start()

    def own_first(rg, _):
        count(0, rg, 1, rg, 0)
        return 0

    lax.fori_loop(0, n_group, own_first, 0)
    for cp in inputs:
        cp.wait()
    usum[...] = ue_ref[...].astype(F32)
    eut[0, :, pl.ds(ucol, UROWS)] = ue_ref[...].astype(F32).T.astype(BF)
    own_rows = pl.ds(al(me * STRIPE, STRIPE), STRIPE)
    panel[0, own_rows, :] = ie_ref[...]
    pl.semaphore_wait(barrier, len(peers))

    def half_rows(q, h):
        return pl.ds(al(q * STRIPE + h * HALF, HALF), HALF)

    def ei0(i):
        q, h, to = ((me, 0, xn), (me, 1, yn), (me, 1, xn), (me, 0, yn), (y * 2 + ox, 0, yn), (oy * 2 + x, 1, xn))[i]
        blk = panel.at[0, half_rows(q, h)]
        src = ie_ref.at[pl.ds(h * HALF, HALF)] if i < 4 else blk
        return rcopy(src, blk, eis, eir.at[min(i, 2)], to)

    def ua(j, i):
        blk = eut.at[j, :, pl.ds(ucol, UROWS)]
        return rcopy(blk, blk, uas.at[j], uar.at[j], (zn, sib, zsib)[i])

    for i in range(4):
        ei0(i).start()
    for i in range(3):
        ua(0, i).start()

    def sib_first(rg, _):
        count(0, rg, 0, n_group + rg, rg)
        xcopy(rg).start()
        return 0

    lax.fori_loop(0, n_group, sib_first, 0)
    stripe_degrees(0)

    def mask_step(m, _):
        i = lax.div(m, n_group)
        rg = lax.rem(m, n_group)
        w = m - n_group

        @pl.when(m >= NSTAGE)
        def _():
            xcopy(m - NSTAGE).wait_send()
        count(i, rg, 0, 2 * m, lax.rem(m, NSTAGE))

        @pl.when(lax.rem(w, 3) != 0)
        def _():
            xcopy(n_group + lax.div(2 * w, 3)).start()

        @pl.when(m == 2 * n_group)
        def _():
            ei0(0).wait_recv()
            ei0(4).start()
            ei0(1).wait_recv()
            ei0(5).start()
        count(i, rg, 1, 2 * m + 1, 0)

        @pl.when(i == CHIPS - 1)
        def _():
            rsl = pl.ds(al(rg * LROWS, LROWS), LROWS)
            v = jnp.sum(upart[rsl, :].T, axis=0, keepdims=True)
            dus[:, rsl] = jnp.broadcast_to(v, (8, LROWS))

        @pl.when(rg == n_group - 1)
        def _():
            stripe_degrees(i)
        return 0

    lax.fori_loop(n_group, CHIPS * n_group, mask_step, 0)

    for i in range(3):
        dusend(i).start()
    for k in range(N_HELD):
        xcopy(jnp.int32(CHIPS * n_group - N_HELD + k)).start()

    def all_of(ref, ss, rs):
        return rcopy(ref, ref, ss, rs, sib)

    def swapped(i):
        region = a.at[pl.ds(al(oc * ROWS, ROWS), ROWS), pl.ds(al(stripe(i) * STRIPE, STRIPE), STRIPE)]
        rcopy(region, region, xs.at[0], xr.at[i], sib).wait_recv()

    all_of(dcr, dgs, dgr).wait_recv()
    for p in range(CHIPS):
        v = dcs[1, p]
        for k in range(7):
            v = v + dcr[k, p]
        v = lax.rsqrt(jnp.maximum(v, 1.0))
        for g in range(8):
            invi[0:1, p * STRIPE + g * 256:p * STRIPE + (g + 1) * 256] = v[g:g + 1, :]
    all_of(dur, dvs, dvr).wait_recv()
    for blk, v in ((c, dus[...] + dur[0]), (oc, dur[1] + dur[2])):
        v = lax.rsqrt(jnp.maximum(v, 1.0))
        for b in range(ROWS // 128):
            w = jnp.broadcast_to(v[0:1, b * 128:(b + 1) * 128], (128, 128))
            upart[pl.ds(al(blk * ROWS + b * 128, 128), 128), :] = w.T
    for i in range(3):
        swapped(i)

    def tile_q(t):
        h = lax.rem(t, 2)
        u = lax.div(t, 2)
        f1, f2 = 1 - lax.div(u, 2), lax.rem(lax.div(u + 1, 2), 2)
        fx = (1 - h) * f1 + h * f2
        fy = (1 - h) * f2 + h * f1
        return (y + fy - 2 * y * fy) * 2 + (x + fx - 2 * x * fx)

    def s1(st, t, k):
        h = lax.rem(t, 2)
        to = dev(x + (1 - h) * (1 - 2 * x), y + h * (1 - 2 * y), c, z)
        return rcopy(part.at[t, k], r1.at[t, k], s1s, s1r.at[st, k], to)

    def s2(st, h, k):
        return rcopy(part.at[4 + h, k], r2.at[h, k], s2s, s2r.at[st, k], (yn, xn)[h])

    def chunk_rows(q, h, k):
        return pl.ds(al(q * STRIPE + h * HALF + k * CH, CH), CH)

    def ag(st, d, h, k):
        blk = panel.at[1 - st, chunk_rows(me, h, k)]
        rs = agr.at[st, k] if d == h else agr.at[st, NCH]
        return rcopy(blk, blk, ags.at[st], rs, (xn, yn)[d])

    def fw(st, h, k):
        q = (y * 2 + ox, oy * 2 + x)[h]
        blk = panel.at[1 - st, chunk_rows(q, h, k)]
        return rcopy(blk, blk, fws.at[st], fwr.at[st], (yn, xn)[h])

    def usib(j):
        return rcopy(upart.at[pl.ds(al(oc * ROWS, ROWS), ROWS)], ursib, usibs.at[j], usibr.at[j], sib)

    def uz(j):
        return rcopy(upart.at[pl.ds(al(c * ROWS + oz * UROWS, UROWS), UROWS)], urz,
                     uzs.at[j], uzr.at[j], zn)

    qh, qq = QUERIES // 2, QUERIES // 4
    quarter = pl.ds(al(c * qh + z * qq, qq), qq)

    def pq_sib():
        return rcopy(pkc.at[pl.ds(al(oc * qh, qh), qh)], pks, pqs, pqr.at[0], sib)

    def pq_z():
        return rcopy(pkc.at[pl.ds(al(c * qh + oz * qq, qq), qq)], pkz, pqs, pqr.at[1], zn)

    def pq_x(i):
        h, to = ((0, xn), (1, yn), (0, yn), (1, xn))[i]
        src = (pkc if i < 2 else pka).at[pl.ds(al(c * qh + z * qq + h * (qq // 2), qq // 2), qq // 2)]
        return rcopy(src, pkx.at[i], pqs, pqr.at[2 + i // 2], to)

    def pq_a(i):
        return rcopy(pkf.at[quarter], pkf.at[quarter], pqs, pqr.at[4], (zn, sib, zsib)[i])

    def badd(u, v):
        return (u.astype(F32) + v.astype(F32)).astype(BF)

    def normalise(base, width):
        def norm(g, _):
            rsl = pl.ds(al(g * 128, 128), 128)
            iu = upart[rsl, :]
            for b in range(width // 128):
                cc = pl.ds(al(base + b * 128, 128), 128)
                a[rsl, cc] = a[rsl, cc] * (iu * invi[0:1, cc]).astype(BF)
            return 0
        lax.fori_loop(0, 2 * ROWS // 128, norm, 0)

    def fu_out():
        return pltpu.make_async_copy(fu_ref, fu_hbm, outs.at[0])

    def pk_out():
        return pltpu.make_async_copy(pkf, pk_hbm, outs.at[1])

    def fi_out(h, k):
        loc = pl.ds(al(h * HALF + k * CH, CH), CH)
        return pltpu.make_async_copy(fi_ref.at[loc], fi_hbm.at[loc], fis)

    for j in range(LAYERS):
        st = j % 2
        last = j == LAYERS - 1
        all_of(eut.at[j, :, pl.ds(0, 3 * UROWS)], uas.at[j], uar.at[j]).wait_recv()

        def item_tile(t, _):
            base = al(tile_q(t) * STRIPE + lax.rem(t, 2) * HALF, HALF)
            if j == 0:
                normalise(base, HALF)
            res = dot(eut[j], a[:, pl.ds(base, HALF)], 1, 0)
            for k in range(NCH):
                part[t, k] = res[:, k * CH:(k + 1) * CH]
            return 0

        def send_tile(t, _):
            item_tile(t, 0)
            for k in range(NCH):
                s1(st, t, k).start()
            return 0

        def first_chunk(n, _):
            t = lax.rem(n, 2)
            k = lax.div(n, 2)
            base = al(tile_q(t) * STRIPE + t * HALF + k * CH, CH)
            normalise(base, CH)
            part[t, k] = dot(eut[j], a[:, pl.ds(base, CH)], 1, 0)
            s1(st, t, k).start()
            return 0

        def stage1(k, _):
            all_of(r1.at[:, k], s1s, s1r.at[st, k]).wait_recv()
            for h in range(2):
                part[4 + h, k] = part[4 + h, k] + r1[2 + h, k]
                part[6 + h, k] = part[6 + h, k] + r1[h, k]
                s2(st, h, k).start()
            return 0

        def stage2(k, _):
            all_of(r2.at[:, k], s2s, s2r.at[st, k]).wait_recv()
            for h in range(2):
                e = (part[6 + h, k] + r2[h, k]).T.astype(BF)
                rsl = chunk_rows(me, h, k)
                if last:
                    loc = pl.ds(al(h * HALF + k * CH, CH), CH)
                    tot = ie_ref[loc, :].astype(F32) + panel[1, rsl, :].astype(F32)
                    tot = tot + panel[0, rsl, :].astype(F32) + e.astype(F32)
                    fi_ref[loc, :] = (tot * (1.0 / (LAYERS + 1))).astype(BF)
                    fi_out(h, k).start()
                else:
                    panel[1 - st, rsl, :] = e
                    ag(st, 0, h, k).start()
                    ag(st, 1, h, k).start()
            return 0

        def forward(k, _):
            all_of(panel.at[1 - st, pl.ds(0, 2 * CH)], ags.at[st], agr.at[st, k]).wait_recv()
            fw(st, 0, k).start()
            fw(st, 1, k).start()
            return 0

        def user_near(i, _):
            rsl = pl.ds(al(i * UROWS, UROWS), UROWS)
            tot = None
            for q in (me, y * 2 + ox, oy * 2 + x):
                ks = pl.ds(al(q * STRIPE, STRIPE), STRIPE)
                d = dot(a[rsl, ks], panel[st, ks, :], 1, 0)
                tot = d if tot is None else tot + d
            upart[rsl, :] = tot
            return 0

        def user_far(i, _):
            b = lax.div(i, 2)
            rsl = pl.ds(al((b * c + (1 - b) * oc) * ROWS + lax.rem(i, 2) * UROWS, UROWS), UROWS)
            ks = pl.ds(al((oy * 2 + ox) * STRIPE, STRIPE), STRIPE)
            upart[rsl, :] = upart[rsl, :] + dot(a[rsl, ks], panel[st, ks, :], 1, 0)

            @pl.when(i == 1)
            def _():
                usib(j).start()
            return 0

        def users():
            if j == 0:
                all_of(panel.at[0, pl.ds(0, 4 * HALF)], eis, eir.at[2]).wait_recv()
            else:
                all_of(panel.at[st, pl.ds(0, STRIPE)], ags.at[1 - st], agr.at[1 - st, NCH]).wait_recv()
            lax.fori_loop(0, 4, user_near, 0)
            if j > 0:
                all_of(panel.at[st, pl.ds(0, STRIPE)], fws.at[1 - st], fwr.at[1 - st]).wait_recv()
            lax.fori_loop(0, 4, user_far, 0)

        def users_out():
            usib(j).wait_recv()
            mine = pl.ds(al(c * ROWS, ROWS), ROWS)
            upart[mine, :] = upart[mine, :] + ursib[...]
            uz(j).start()

        def user_final():
            uz(j).wait_recv()
            e = (upart[pl.ds(ucol, UROWS), :] + urz[...]).astype(BF).astype(F32)
            usum[...] = usum[...] + e
            if not last:
                eut[j + 1, :, pl.ds(ucol, UROWS)] = e.T.astype(BF)
                for i in range(3):
                    ua(j + 1, i).start()
                return
            fu = (usum[...] * (1.0 / (LAYERS + 1))).astype(BF)
            fu_ref[...] = fu
            fu_out().start()
            ids = lax.broadcasted_iota(jnp.int32, (UROWS, QUERIES), 0) + (row * 2 + z) * UROWS
            hot = jnp.where(ids == q_ref[...], 1.0, 0.0).astype(BF)
            pkc[...] = dot(hot, fu, 0, 0).astype(BF)
            pq_sib().start()

        if j == 0:
            lax.fori_loop(0, 2 * NCH, first_chunk, 0)
            lax.fori_loop(2, 4, send_tile, 0)
            lax.fori_loop(4, 6, item_tile, 0)
            swapped(3)
            lax.fori_loop(6, 8, item_tile, 0)
            lax.fori_loop(0, NCH - 1, stage1, 0)
            users()
            users_out()
            stage1(NCH - 1, 0)
            lax.fori_loop(0, NCH, stage2, 0)
            user_final()
        else:
            lax.fori_loop(0, 2, send_tile, 0)
            users()
            users_out()
            lax.fori_loop(2, 4, send_tile, 0)
            lax.fori_loop(4, 8, item_tile, 0)
            if not last:
                lax.fori_loop(0, 2, stage1, 0)
            user_final()
            if last:
                pq_sib().wait_recv()
                hrows = pl.ds(al(c * qh, qh), qh)
                pkc[hrows, :] = badd(pkc[hrows, :], pks[...])
                pq_z().start()
                stage1(0, 0)
                pq_z().wait_recv()
                pkc[quarter, :] = badd(pkc[quarter, :], pkz[...])
                for i in range(2):
                    pq_x(i).start()
                stage1(1, 0)
                all_of(pkx.at[pl.ds(0, 2)], pqs, pqr.at[2]).wait_recv()
                for i in range(2):
                    rsl = pl.ds(al(c * qh + z * qq + i * (qq // 2), qq // 2), qq // 2)
                    pka[rsl, :] = badd(pkc[rsl, :], pkx[i])
                for i in range(2, 4):
                    pq_x(i).start()
            lax.fori_loop(2, NCH, stage1, 0)
            lax.fori_loop(0, 2, stage2, 0)
            if last:
                all_of(pkx.at[pl.ds(2, 2)], pqs, pqr.at[3]).wait_recv()
                for i in range(2, 4):
                    rsl = pl.ds(al(c * qh + z * qq + (i - 2) * (qq // 2), qq // 2), qq // 2)
                    pkf[rsl, :] = badd(pka[rsl, :], pkx[i])
                for i in range(3):
                    pq_a(i).start()
            lax.fori_loop(2, NCH, stage2, 0)
        if not last:
            lax.fori_loop(0, NCH, forward, 0)

        usib(j).wait_send()
        uz(j).wait_send()
        all_of(eut.at[j, :, pl.ds(0, 3 * UROWS)], uas.at[j], uar.at[j]).wait_send()
        all_of(part.at[pl.ds(0, 4)], s1s, s1r.at[st, 0]).wait_send()
        all_of(part.at[pl.ds(4, 2)], s2s, s2r.at[st, 0]).wait_send()
        if j == 0:
            all_of(dcr, dgs, dgr).wait_send()
            all_of(dur, dvs, dvr).wait_send()
            def drain_swap(m, _):
                xcopy(m).wait_send()
                return 0
            lax.fori_loop(CHIPS * n_group - NSTAGE, CHIPS * n_group, drain_swap, 0)
            all_of(panel.at[0, pl.ds(0, 6 * HALF)], eis, eir.at[2]).wait_send()
        else:
            all_of(panel.at[st, pl.ds(0, 2 * STRIPE)], ags.at[1 - st], agr.at[1 - st, NCH]).wait_send()
            all_of(panel.at[st, pl.ds(0, STRIPE)], fws.at[1 - st], fwr.at[1 - st]).wait_send()

    all_of(pkf.at[pl.ds(0, 3 * qq)], pqs, pqr.at[4]).wait_recv()
    pk_out().start()
    all_of(fi_ref, pqs, pqr.at[4]).wait_send()
    pltpu.make_async_copy(fi_ref, fi_hbm, fis).wait()
    fu_out().wait()
    pk_out().wait()


def score_kernel(fu_ref, fi_ref, pk_ref, fu_out, fi_out, s_out, buf, sem, out_sem):
    copies = [pltpu.make_async_copy(fu_ref, fu_out, out_sem.at[0]),
              pltpu.make_async_copy(fi_ref, fi_out, out_sem.at[1])]
    for i in range(QUERIES // SROWS):
        rsl = pl.ds(i * SROWS, SROWS)
        buf[i] = dot(pk_ref[rsl, :], fi_ref[...], 1, 1)
        copies.append(pltpu.make_async_copy(buf.at[i], s_out.at[rsl, :], sem.at[i]))
        if i == 0:
            for cp in copies:
                cp.start()
        else:
            copies[-1].start()
    for cp in copies:
        cp.wait()


def scores_of(fu, fi, picked):
    vm = pl.BlockSpec(memory_space=pltpu.VMEM)
    hbm = pl.BlockSpec(memory_space=pl.ANY)
    return pl.pallas_call(
        score_kernel,
        out_shape=(jax.ShapeDtypeStruct(fu.shape, BF), jax.ShapeDtypeStruct(fi.shape, BF),
                   jax.ShapeDtypeStruct((QUERIES, STRIPE), F32)),
        in_specs=[vm, vm, vm],
        out_specs=(hbm, hbm, hbm),
        scratch_shapes=[pltpu.VMEM((QUERIES // SROWS, SROWS, STRIPE), F32),
                        pltpu.SemaphoreType.DMA((QUERIES // SROWS,)), pltpu.SemaphoreType.DMA((2,))],
        name='scores',
    )(fu, fi, picked)


def propagate(mask_blk, user_shard, item_shard, queries):
    hbm = pl.BlockSpec(memory_space=pl.ANY)
    dma = pltpu.SemaphoreType.DMA
    qh, qq = QUERIES // 2, QUERIES // 4
    scratch = [
        pltpu.VMEM((UROWS, EMB), BF),
        pltpu.VMEM((STRIPE, EMB), BF),
        pltpu.VMEM((1, QUERIES), jnp.int32),
        pltpu.VMEM((UROWS, EMB), BF),
        pltpu.VMEM((STRIPE, EMB), BF),
        pltpu.VMEM((QUERIES, EMB), BF),
        pltpu.VMEM((2 * ROWS, COLS), BF),
        pltpu.VMEM((8, NCH, EMB, CH), F32),
        pltpu.VMEM((4, NCH, EMB, CH), F32),
        pltpu.VMEM((2, NCH, EMB, CH), F32),
        pltpu.VMEM((2, COLS, EMB), BF),
        pltpu.VMEM((LAYERS, EMB, 2 * ROWS), BF),
        pltpu.VMEM((2 * ROWS, EMB), F32),
        pltpu.VMEM((ROWS, EMB), F32),
        pltpu.VMEM((UROWS, EMB), F32),
        pltpu.VMEM((1, COLS), F32),
        pltpu.VMEM((NLOAD, LROWS, STRIPE), jnp.int32),
        pltpu.VMEM((NSTAGE, LROWS, STRIPE), BF),
        pltpu.VMEM((2, 8, STRIPE), F32),
        pltpu.VMEM((2, CHIPS, 8, STRIPE // 8), F32),
        pltpu.VMEM((7, CHIPS, 8, STRIPE // 8), F32),
        pltpu.VMEM((8, ROWS), F32),
        pltpu.VMEM((3, 8, ROWS), F32),
        pltpu.VMEM((UROWS, EMB), F32),
        pltpu.VMEM((QUERIES, EMB), BF),
        pltpu.VMEM((qh, EMB), BF),
        pltpu.VMEM((qq, EMB), BF),
        pltpu.VMEM((4, qq // 2, EMB), BF),
        pltpu.VMEM((QUERIES, EMB), BF),
        dma((NLOAD,)), dma((NSTAGE,)), dma((CHIPS,)),
        dma, dma((2, NCH)),
        dma, dma((2, NCH)),
        dma((2,)), dma((2, NCH + 1)),
        dma((2,)), dma((2,)),
        dma((LAYERS,)), dma((LAYERS,)), dma((LAYERS,)), dma((LAYERS,)),
        dma((LAYERS,)), dma((LAYERS,)),
        dma, dma((3,)), dma, dma, dma, dma,
        dma, dma((5,)),
        dma((3,)), dma((2,)), dma,
    ]
    return pl.pallas_call(
        kernel,
        out_shape=(jax.ShapeDtypeStruct((UROWS, EMB), BF),
                   jax.ShapeDtypeStruct((STRIPE, EMB), BF),
                   jax.ShapeDtypeStruct((QUERIES, EMB), BF)),
        in_specs=[hbm] * 4,
        out_specs=(hbm, hbm, hbm),
        scratch_shapes=scratch,
        compiler_params=pltpu.CompilerParams(collective_id=0, has_side_effects=True,
                                             vmem_limit_bytes=67043328),
        name='propagate',
    )(mask_blk, user_shard, item_shard, queries)


def solution(mesh):
    def device_step(mask_blk, user_shard, item_shard, queries):
        fu, fi, picked = propagate(mask_blk, user_shard, item_shard, queries.reshape(1, QUERIES))
        return scores_of(fu, fi, picked)

    return jax.shard_map(
        device_step, mesh=mesh,
        in_specs=(P('row', 'col'), P(('row', 'col'), None), P(('col', 'row'), None), P()),
        out_specs=(P(('row', 'col'), None), P(('col', 'row'), None), P(None, ('col', 'row'))),
        check_vma=False)
```

```python
import functools

import jax
import jax.numpy as jnp
from jax import lax
from jax.experimental import pallas as pl
from jax.experimental.pallas import tpu as pltpu
from jax.sharding import PartitionSpec as P

LAYERS = 3
BF = jnp.bfloat16
F32 = jnp.float32
EMB = 128
ROWS = 1024
STRIPE = 2048
CHIPS = 4
COLS = STRIPE * CHIPS
UROWS = 512
HALF = STRIPE // 2
NCH = 4
CH = HALF // NCH
LROWS = 128
NLOAD = 6
NSTAGE = 11
N_HELD = 8
QUERIES = 1024
SROWS = 128


def al(v, m):
    return pl.multiple_of(v, m)


def dot(a, b, ca, cb):
    return lax.dot_general(a, b, (((ca,), (cb,)), ((), ())), preferred_element_type=F32)


def kernel(mask_ref, ue_hbm, ie_hbm, q_hbm, fu_hbm, fi_hbm, pk_hbm, ue_ref, ie_ref, q_ref, fu_ref, fi_ref, pkf,
           a, part, r1, r2, panel, eut, upart, ursib, urz, invi, mbuf, stage,
           cs, dcs, dcr, dus, dur, usum, pkc, pks, pkz, pkx, pka,
           lsem, xs, xr, s1s, s1r, s2s, s2r, ags, agr, fws, fwr,
           usibs, usibr, uzs, uzr, uas, uar, eis, eir, dgs, dgr, dvs, dvr, pqs, pqr, ins, outs, fis):
    row = lax.axis_index('row')
    z = lax.axis_index('col')
    c = lax.rem(row, 2)
    x = lax.rem(lax.div(row, 2), 2)
    y = lax.div(row, 4)
    me = y * 2 + x

    def dev(xx, yy, cc, zz):
        return {'row': (yy * 2 + xx) * 2 + cc, 'col': zz}

    ox, oy, oc, oz = 1 - x, 1 - y, 1 - c, 1 - z
    xn, yn, dg = dev(ox, y, c, z), dev(x, oy, c, z), dev(ox, oy, c, z)
    zn, sib, zsib = dev(x, y, c, oz), dev(x, y, oc, z), dev(x, y, oc, oz)
    xnc, ync, dgc = dev(ox, y, oc, z), dev(x, oy, oc, z), dev(ox, oy, oc, z)

    def rcopy(src, dst, ss, rs, to):
        return pltpu.make_async_remote_copy(src_ref=src, dst_ref=dst, send_sem=ss, recv_sem=rs,
                                            device_id=to, device_id_type=pl.DeviceIdType.MESH)

    barrier = pltpu.get_barrier_semaphore()
    peers = (xn, yn, dg, zn, sib, zsib, xnc, ync, dgc)
    for peer in peers:
        pl.semaphore_signal(barrier, inc=1, device_id=peer, device_id_type=pl.DeviceIdType.MESH)

    n_group = ROWS // LROWS
    n_load = n_group * 2 * CHIPS

    def stripe(i):
        fx = 1 - lax.rem(i, 2)
        fy = lax.rem(lax.div(i + 1, 2), 2)
        return (y + fy - 2 * y * fy) * 2 + (x + fx - 2 * x * fx)

    def load_at(i, rg, par, n):
        s = 2 * stripe(i) + par * c + (1 - par) * oc
        slot = lax.rem(n, NLOAD)
        return pltpu.make_async_copy(
            mask_ref.at[pl.ds(al(rg * LROWS, LROWS), LROWS), pl.ds(al(s * STRIPE, STRIPE), STRIPE)],
            mbuf.at[slot], lsem.at[slot])

    def load(n):
        first = 1 - lax.min(lax.div(n, 2 * n_group), 1)
        i = lax.div(n, 2 * n_group)
        w = lax.rem(n, 2 * n_group)
        rg = first * lax.rem(w, n_group) + (1 - first) * lax.div(w, 2)
        par = first * (1 - lax.div(w, n_group)) + (1 - first) * lax.rem(w, 2)
        return load_at(i, rg, par, n)

    inputs = [pltpu.make_async_copy(src, dst, ins.at[i])
              for i, (src, dst) in enumerate(((ie_hbm, ie_ref), (ue_hbm, ue_ref), (q_hbm, q_ref)))]
    for cp in inputs:
        cp.start()
    for n in range(NLOAD):
        load(jnp.int32(n)).start()
    cs[...] = jnp.zeros_like(cs)
    upart[pl.ds(0, ROWS), :] = jnp.zeros((ROWS, EMB), F32)
    ucol = al(c * ROWS + z * UROWS, UROWS)

    def count(i, rg, par, n, sslot):
        p = stripe(i)
        slot = lax.rem(n, NLOAD)
        load_at(i, rg, par, n).wait()
        cols = pl.ds(al(p * STRIPE, STRIPE), STRIPE)
        acc = jnp.zeros((8, STRIPE), F32)
        for g in range(LROWS // 16):
            v = mbuf[slot, g * 16:(g + 1) * 16, :].astype(F32)
            b = v.astype(BF)
            if par == 0:
                stage[sslot, g * 16:(g + 1) * 16, :] = b
            else:
                a[pl.ds(al(c * ROWS + rg * LROWS + g * 16, 16), 16), cols] = b
            acc = acc + v[0:8] + v[8:16]
            parts = [v[:, q * 128:(q + 1) * 128] for q in range(STRIPE // 128)]
            while len(parts) > 1:
                parts = [parts[q] + parts[q + 1] for q in range(0, len(parts), 2)]
            rsl = pl.ds(al(rg * LROWS + g * 16, 16), 16)
            upart[rsl, :] = upart[rsl, :] + parts[0]
        cs[par] = cs[par] + acc

        @pl.when(n + NLOAD < n_load)
        def _():
            load(n + NLOAD).start()

    def xcopy(m):
        i = lax.div(m, n_group)
        rg = lax.rem(m, n_group)
        slot = lax.rem(m, NSTAGE)
        return rcopy(stage.at[slot],
                     a.at[pl.ds(al(c * ROWS + rg * LROWS, LROWS), LROWS), pl.ds(al(stripe(i) * STRIPE, STRIPE), STRIPE)],
                     xs.at[slot], xr.at[i], sib)

    def dgsend(p, i):
        return rcopy(dcs.at[(1, 1, 1, 0, 0, 0, 0)[i], p], dcr.at[i, p], dgs, dgr,
                     (xn, yn, dg, sib, xnc, ync, dgc)[i])

    def dusend(i):
        return rcopy(dus, dur.at[i], dvs, dvr, (zn, sib, zsib)[i])

    def stripe_degrees(i):
        p = stripe(i)
        for par in range(2):
            v = jnp.sum(cs[par], axis=0, keepdims=True)
            for g in range(8):
                dcs[par, p, g:g + 1, :] = v[:, g * 256:(g + 1) * 256]
        cs[...] = jnp.zeros_like(cs)
        for k in range(7):
            dgsend(p, k).start()

    def own_first(rg, _):
        count(0, rg, 1, rg, 0)
        return 0

    lax.fori_loop(0, n_group, own_first, 0)
    for cp in inputs:
        cp.wait()
    usum[...] = ue_ref[...].astype(F32)
    eut[0, :, pl.ds(ucol, UROWS)] = ue_ref[...].astype(F32).T.astype(BF)
    own_rows = pl.ds(al(me * STRIPE, STRIPE), STRIPE)
    panel[0, own_rows, :] = ie_ref[...]
    pl.semaphore_wait(barrier, len(peers))

    def half_rows(q, h):
        return pl.ds(al(q * STRIPE + h * HALF, HALF), HALF)

    def ei0(i):
        q, h, to = ((me, 0, xn), (me, 1, yn), (me, 1, xn), (me, 0, yn), (y * 2 + ox, 0, yn), (oy * 2 + x, 1, xn))[i]
        blk = panel.at[0, half_rows(q, h)]
        src = ie_ref.at[pl.ds(h * HALF, HALF)] if i < 4 else blk
        return rcopy(src, blk, eis, eir.at[min(i, 2)], to)

    def ua(j, i):
        blk = eut.at[j, :, pl.ds(ucol, UROWS)]
        return rcopy(blk, blk, uas, uar.at[j], (zn, sib, zsib)[i])

    for i in range(4):
        ei0(i).start()
    for i in range(3):
        ua(0, i).start()

    def sib_first(rg, _):
        count(0, rg, 0, n_group + rg, rg)
        xcopy(rg).start()
        return 0

    lax.fori_loop(0, n_group, sib_first, 0)
    stripe_degrees(0)

    def mask_step(m, _):
        i = lax.div(m, n_group)
        rg = lax.rem(m, n_group)
        w = m - n_group

        @pl.when(m >= NSTAGE)
        def _():
            xcopy(m - NSTAGE).wait_send()
        count(i, rg, 0, 2 * m, lax.rem(m, NSTAGE))

        @pl.when(lax.rem(w, 3) != 0)
        def _():
            xcopy(n_group + lax.div(2 * w, 3)).start()

        @pl.when(m == 2 * n_group)
        def _():
            ei0(0).wait_recv()
            ei0(4).start()
            ei0(1).wait_recv()
            ei0(5).start()
        count(i, rg, 1, 2 * m + 1, 0)

        @pl.when(i == CHIPS - 1)
        def _():
            rsl = pl.ds(al(rg * LROWS, LROWS), LROWS)
            v = jnp.sum(upart[rsl, :].T, axis=0, keepdims=True)
            dus[:, rsl] = jnp.broadcast_to(v, (8, LROWS))

        @pl.when(rg == n_group - 1)
        def _():
            stripe_degrees(i)
        return 0

    lax.fori_loop(n_group, CHIPS * n_group, mask_step, 0)

    for i in range(3):
        dusend(i).start()
    for k in range(N_HELD):
        xcopy(jnp.int32(CHIPS * n_group - N_HELD + k)).start()

    def all_of(ref, ss, rs):
        return rcopy(ref, ref, ss, rs, sib)

    def swapped(i):
        region = a.at[pl.ds(al(oc * ROWS, ROWS), ROWS), pl.ds(al(stripe(i) * STRIPE, STRIPE), STRIPE)]
        rcopy(region, region, xs.at[0], xr.at[i], sib).wait_recv()

    all_of(dur, dvs, dvr).wait_recv()
    for blk, v in ((c, dus[...] + dur[0]), (oc, dur[1] + dur[2])):
        v = lax.rsqrt(jnp.maximum(v, 1.0))
        for b in range(ROWS // 128):
            w = jnp.broadcast_to(v[0:1, b * 128:(b + 1) * 128], (128, 128))
            upart[pl.ds(al(blk * ROWS + b * 128, 128), 128), :] = w.T
    all_of(dcr, dgs, dgr).wait_recv()
    for p in range(CHIPS):
        v = dcs[1, p]
        for k in range(7):
            v = v + dcr[k, p]
        v = lax.rsqrt(jnp.maximum(v, 1.0))
        for g in range(8):
            invi[0:1, p * STRIPE + g * 256:p * STRIPE + (g + 1) * 256] = v[g:g + 1, :]
    for i in range(3):
        swapped(i)

    def tile_q(t):
        h = lax.rem(t, 2)
        u = lax.div(t, 2)
        f1, f2 = 1 - lax.div(u, 2), lax.rem(lax.div(u + 1, 2), 2)
        fx = (1 - h) * f1 + h * f2
        fy = (1 - h) * f2 + h * f1
        return (y + fy - 2 * y * fy) * 2 + (x + fx - 2 * x * fx)

    def s1(st, t, k, cols=pl.ds(0, CH)):
        h = lax.rem(t, 2)
        to = dev(x + (1 - h) * (1 - 2 * x), y + h * (1 - 2 * y), c, z)
        return rcopy(part.at[t, k, :, cols], r1.at[t, k, :, cols], s1s, s1r.at[k], to)

    def s2(st, h, k):
        return rcopy(part.at[4 + h, k], r2.at[h, k], s2s, s2r.at[k], (yn, xn)[h])

    def chunk_rows(q, h, k):
        return pl.ds(al(q * STRIPE + h * HALF + k * CH, CH), CH)

    def ag(st, d, h, k):
        blk = panel.at[1 - st, chunk_rows(me, h, k)]
        rs = agr.at[k] if d == h else agr.at[NCH]
        return rcopy(blk, blk, ags.at[st], rs, (xn, yn)[d])

    def fw(st, h, k):
        q = (y * 2 + ox, oy * 2 + x)[h]
        blk = panel.at[1 - st, chunk_rows(q, h, k)]
        return rcopy(blk, blk, fws.at[st], fwr, (yn, xn)[h])

    def usib(j):
        return rcopy(upart.at[pl.ds(al(oc * ROWS, ROWS), ROWS)], ursib, usibs, usibr, sib)

    def uz(j):
        return rcopy(upart.at[pl.ds(al(c * ROWS + oz * UROWS, UROWS), UROWS)], urz,
                     uzs, uzr, zn)

    qh, qq = QUERIES // 2, QUERIES // 4
    quarter = pl.ds(al(c * qh + z * qq, qq), qq)

    def pq_sib():
        return rcopy(pkc.at[pl.ds(al(oc * qh, qh), qh)], pks, pqs, pqr.at[0], sib)

    def pq_z():
        return rcopy(pkc.at[pl.ds(al(c * qh + oz * qq, qq), qq)], pkz, pqs, pqr.at[1], zn)

    def pq_x(i):
        h, to = ((0, xn), (1, yn), (0, yn), (1, xn))[i]
        src = (pkc if i < 2 else pka).at[pl.ds(al(c * qh + z * qq + h * (qq // 2), qq // 2), qq // 2)]
        return rcopy(src, pkx.at[i], pqs, pqr.at[2 + i // 2], to)

    def pq_a(i):
        return rcopy(pkf.at[quarter], pkf.at[quarter], pqs, pqr.at[4], (zn, sib, zsib)[i])

    def badd(u, v):
        return (u.astype(F32) + v.astype(F32)).astype(BF)

    def normalise(base, width):
        def norm(g, _):
            rsl = pl.ds(al(g * 128, 128), 128)
            iu = upart[rsl, :]
            for b in range(width // 128):
                cc = pl.ds(al(base + b * 128, 128), 128)
                a[rsl, cc] = a[rsl, cc] * (iu * invi[0:1, cc]).astype(BF)
            return 0
        lax.fori_loop(0, 2 * ROWS // 128, norm, 0)

    def fu_out():
        return pltpu.make_async_copy(fu_ref, fu_hbm, outs.at[0])

    def pk_out():
        return pltpu.make_async_copy(pkf, pk_hbm, outs.at[1])

    def fi_out(h, k):
        loc = pl.ds(al(h * HALF + k * CH, CH), CH)
        return pltpu.make_async_copy(fi_ref.at[loc], fi_hbm.at[loc], fis)

    for j in range(LAYERS):
        st = j % 2
        last = j == LAYERS - 1
        all_of(eut.at[j, :, pl.ds(0, 3 * UROWS)], uas, uar.at[j]).wait_recv()

        def item_tile(t, _):
            base = al(tile_q(t) * STRIPE + lax.rem(t, 2) * HALF, HALF)
            if j == 0:
                normalise(base, HALF)
            res = dot(eut[j], a[:, pl.ds(base, HALF)], 1, 0)
            for k in range(NCH):
                part[t, k] = res[:, k * CH:(k + 1) * CH]
            return 0

        def send_tile(t, _):
            item_tile(t, 0)
            for k in range(NCH):
                s1(st, t, k).start()
            return 0

        def first_chunk(n, _):
            t = lax.rem(n, 2)
            k = lax.div(n, 2)
            base = al(tile_q(t) * STRIPE + t * HALF + k * CH, CH)
            normalise(base, CH)
            part[t, k] = dot(eut[j], a[:, pl.ds(base, CH)], 1, 0)
            s1(st, t, k).start()
            return 0

        def first_half(n, _):
            t = lax.rem(n, 2)
            cols = pl.ds(al(lax.div(n, 2) * 128, 128), 128)
            base = al(tile_q(t) * STRIPE + t * HALF + lax.div(n, 2) * 128, 128)
            normalise(base, 128)
            part[t, 0, :, cols] = dot(eut[j], a[:, pl.ds(base, 128)], 1, 0)
            s1(st, t, 0, cols).start()
            return 0

        def stage1(k, _):
            all_of(r1.at[:, k], s1s, s1r.at[k]).wait_recv()
            for h in range(2):
                part[4 + h, k] = part[4 + h, k] + r1[2 + h, k]
                part[6 + h, k] = part[6 + h, k] + r1[h, k]
                s2(st, h, k).start()
            return 0

        def stage2(k, _):
            all_of(r2.at[:, k], s2s, s2r.at[k]).wait_recv()
            for h in range(2):
                e = (part[6 + h, k] + r2[h, k]).T.astype(BF)
                rsl = chunk_rows(me, h, k)
                if last:
                    loc = pl.ds(al(h * HALF + k * CH, CH), CH)
                    tot = ie_ref[loc, :].astype(F32) + panel[1, rsl, :].astype(F32)
                    tot = tot + panel[0, rsl, :].astype(F32) + e.astype(F32)
                    fi_ref[loc, :] = (tot * (1.0 / (LAYERS + 1))).astype(BF)
                    fi_out(h, k).start()
                else:
                    panel[1 - st, rsl, :] = e
                    ag(st, 0, h, k).start()
                    ag(st, 1, h, k).start()
            return 0

        def forward(k, _):
            all_of(panel.at[1 - st, pl.ds(0, 2 * CH)], ags.at[st], agr.at[k]).wait_recv()
            fw(st, 0, k).start()
            fw(st, 1, k).start()
            return 0

        def user_near(i, _):
            rsl = pl.ds(al(i * UROWS, UROWS), UROWS)
            tot = None
            for q in (me, y * 2 + ox, oy * 2 + x):
                ks = pl.ds(al(q * STRIPE, STRIPE), STRIPE)
                d = dot(a[rsl, ks], panel[st, ks, :], 1, 0)
                tot = d if tot is None else tot + d
            upart[rsl, :] = tot
            if j == 0:
                @pl.when(i == 2)
                def _():
                    stage1(2, 0)
            return 0

        def user_far(i, _):
            b = lax.div(i, 2)
            rsl = pl.ds(al((b * c + (1 - b) * oc) * ROWS + lax.rem(i, 2) * UROWS, UROWS), UROWS)
            ks = pl.ds(al((oy * 2 + ox) * STRIPE, STRIPE), STRIPE)
            upart[rsl, :] = upart[rsl, :] + dot(a[rsl, ks], panel[st, ks, :], 1, 0)

            @pl.when(i == 1)
            def _():
                usib(j).start()
            return 0

        def users():
            if j == 0:
                all_of(panel.at[0, pl.ds(0, 4 * HALF)], eis, eir.at[2]).wait_recv()
            else:
                all_of(panel.at[st, pl.ds(0, STRIPE)], ags.at[1 - st], agr.at[NCH]).wait_recv()
            lax.fori_loop(0, 4, user_near, 0)
            if j == 0:
                stage1(3, 0)
                stage2(0, 0)
            if j > 0:
                all_of(panel.at[st, pl.ds(0, STRIPE)], fws.at[1 - st], fwr).wait_recv()
            lax.fori_loop(0, 4, user_far, 0)

        def users_out():
            usib(j).wait_recv()
            mine = pl.ds(al(c * ROWS, ROWS), ROWS)
            upart[mine, :] = upart[mine, :] + ursib[...]
            uz(j).start()

        def user_final():
            uz(j).wait_recv()
            e = (upart[pl.ds(ucol, UROWS), :] + urz[...]).astype(BF).astype(F32)
            usum[...] = usum[...] + e
            if not last:
                eut[j + 1, :, pl.ds(ucol, UROWS)] = e.T.astype(BF)
                for i in range(3):
                    ua(j + 1, i).start()
                return
            fu = (usum[...] * (1.0 / (LAYERS + 1))).astype(BF)
            fu_ref[...] = fu
            fu_out().start()
            ids = lax.broadcasted_iota(jnp.int32, (UROWS, QUERIES), 0) + (row * 2 + z) * UROWS
            hot = jnp.where(ids == q_ref[...], 1.0, 0.0).astype(BF)
            pkc[...] = dot(hot, fu, 0, 0).astype(BF)
            pq_sib().start()

        if j == 0:
            lax.fori_loop(0, 4, first_half, 0)
            lax.fori_loop(2, 2 * NCH, first_chunk, 0)
            lax.fori_loop(2, 4, send_tile, 0)
            lax.fori_loop(4, 6, item_tile, 0)
            swapped(3)
            lax.fori_loop(6, 8, item_tile, 0)
            lax.fori_loop(0, 2, stage1, 0)
            users()
            users_out()
            lax.fori_loop(1, NCH, stage2, 0)
            user_final()
        else:
            lax.fori_loop(0, 2, send_tile, 0)
            users()
            users_out()
            lax.fori_loop(2, 4, send_tile, 0)
            lax.fori_loop(4, 8, item_tile, 0)
            if not last:
                lax.fori_loop(0, 2, stage1, 0)
            user_final()
            if last:
                pq_sib().wait_recv()
                hrows = pl.ds(al(c * qh, qh), qh)
                pkc[hrows, :] = badd(pkc[hrows, :], pks[...])
                pq_z().start()
                stage1(0, 0)
                pq_z().wait_recv()
                pkc[quarter, :] = badd(pkc[quarter, :], pkz[...])
                for i in range(2):
                    pq_x(i).start()
                stage1(1, 0)
                all_of(pkx.at[pl.ds(0, 2)], pqs, pqr.at[2]).wait_recv()
                for i in range(2):
                    rsl = pl.ds(al(c * qh + z * qq + i * (qq // 2), qq // 2), qq // 2)
                    pka[rsl, :] = badd(pkc[rsl, :], pkx[i])
                for i in range(2, 4):
                    pq_x(i).start()
            lax.fori_loop(2, NCH, stage1, 0)
            lax.fori_loop(0, 2, stage2, 0)
            if last:
                all_of(pkx.at[pl.ds(2, 2)], pqs, pqr.at[3]).wait_recv()
                for i in range(2, 4):
                    rsl = pl.ds(al(c * qh + z * qq + (i - 2) * (qq // 2), qq // 2), qq // 2)
                    pkf[rsl, :] = badd(pka[rsl, :], pkx[i])
                for i in range(3):
                    pq_a(i).start()
            lax.fori_loop(2, NCH, stage2, 0)
        if not last:
            lax.fori_loop(0, NCH, forward, 0)

        usib(j).wait_send()
        uz(j).wait_send()
        all_of(eut.at[j, :, pl.ds(0, 3 * UROWS)], uas, uar.at[j]).wait_send()
        all_of(part.at[pl.ds(0, 4)], s1s, s1r.at[0]).wait_send()
        all_of(part.at[pl.ds(4, 2)], s2s, s2r.at[0]).wait_send()
        if j == 0:
            all_of(dcr, dgs, dgr).wait_send()
            all_of(dur, dvs, dvr).wait_send()
            def drain_swap(m, _):
                xcopy(m).wait_send()
                return 0
            lax.fori_loop(CHIPS * n_group - NSTAGE, CHIPS * n_group, drain_swap, 0)
            all_of(panel.at[0, pl.ds(0, 6 * HALF)], eis, eir.at[2]).wait_send()
        else:
            all_of(panel.at[st, pl.ds(0, 2 * STRIPE)], ags.at[1 - st], agr.at[NCH]).wait_send()
            all_of(panel.at[st, pl.ds(0, STRIPE)], fws.at[1 - st], fwr).wait_send()

    all_of(pkf.at[pl.ds(0, 3 * qq)], pqs, pqr.at[4]).wait_recv()
    pk_out().start()
    all_of(fi_ref, pqs, pqr.at[4]).wait_send()
    pltpu.make_async_copy(fi_ref, fi_hbm, fis).wait()
    fu_out().wait()
    pk_out().wait()


def score_kernel(fu_ref, fi_ref, pk_ref, fu_out, fi_out, s_out, buf, sem, out_sem):
    copies = [pltpu.make_async_copy(fu_ref, fu_out, out_sem.at[0]),
              pltpu.make_async_copy(fi_ref, fi_out, out_sem.at[1])]
    for i in range(QUERIES // SROWS):
        rsl = pl.ds(i * SROWS, SROWS)
        buf[i] = dot(pk_ref[rsl, :], fi_ref[...], 1, 1)
        copies.append(pltpu.make_async_copy(buf.at[i], s_out.at[rsl, :], sem.at[i]))
        if i == 0:
            for cp in copies:
                cp.start()
        else:
            copies[-1].start()
    for cp in copies:
        cp.wait()


def scores_of(fu, fi, picked):
    vm = pl.BlockSpec(memory_space=pltpu.VMEM)
    hbm = pl.BlockSpec(memory_space=pl.ANY)
    return pl.pallas_call(
        score_kernel,
        out_shape=(jax.ShapeDtypeStruct(fu.shape, BF), jax.ShapeDtypeStruct(fi.shape, BF),
                   jax.ShapeDtypeStruct((QUERIES, STRIPE), F32)),
        in_specs=[vm, vm, vm],
        out_specs=(hbm, hbm, hbm),
        scratch_shapes=[pltpu.VMEM((QUERIES // SROWS, SROWS, STRIPE), F32),
                        pltpu.SemaphoreType.DMA((QUERIES // SROWS,)), pltpu.SemaphoreType.DMA((2,))],
        name='scores',
    )(fu, fi, picked)


def propagate(mask_blk, user_shard, item_shard, queries):
    hbm = pl.BlockSpec(memory_space=pl.ANY)
    dma = pltpu.SemaphoreType.DMA
    qh, qq = QUERIES // 2, QUERIES // 4
    scratch = [
        pltpu.VMEM((UROWS, EMB), BF),
        pltpu.VMEM((STRIPE, EMB), BF),
        pltpu.VMEM((1, QUERIES), jnp.int32),
        pltpu.VMEM((UROWS, EMB), BF),
        pltpu.VMEM((STRIPE, EMB), BF),
        pltpu.VMEM((QUERIES, EMB), BF),
        pltpu.VMEM((2 * ROWS, COLS), BF),
        pltpu.VMEM((8, NCH, EMB, CH), F32),
        pltpu.VMEM((4, NCH, EMB, CH), F32),
        pltpu.VMEM((2, NCH, EMB, CH), F32),
        pltpu.VMEM((2, COLS, EMB), BF),
        pltpu.VMEM((LAYERS, EMB, 2 * ROWS), BF),
        pltpu.VMEM((2 * ROWS, EMB), F32),
        pltpu.VMEM((ROWS, EMB), F32),
        pltpu.VMEM((UROWS, EMB), F32),
        pltpu.VMEM((1, COLS), F32),
        pltpu.VMEM((NLOAD, LROWS, STRIPE), jnp.int32),
        pltpu.VMEM((NSTAGE, LROWS, STRIPE), BF),
        pltpu.VMEM((2, 8, STRIPE), F32),
        pltpu.VMEM((2, CHIPS, 8, STRIPE // 8), F32),
        pltpu.VMEM((7, CHIPS, 8, STRIPE // 8), F32),
        pltpu.VMEM((8, ROWS), F32),
        pltpu.VMEM((3, 8, ROWS), F32),
        pltpu.VMEM((UROWS, EMB), F32),
        pltpu.VMEM((QUERIES, EMB), BF),
        pltpu.VMEM((qh, EMB), BF),
        pltpu.VMEM((qq, EMB), BF),
        pltpu.VMEM((4, qq // 2, EMB), BF),
        pltpu.VMEM((QUERIES, EMB), BF),
        dma((NLOAD,)), dma((NSTAGE,)), dma((CHIPS,)),
        dma, dma((NCH,)),
        dma, dma((NCH,)),
        dma((2,)), dma((NCH + 1,)),
        dma((2,)), dma,
        dma, dma, dma, dma,
        dma, dma((LAYERS,)),
        dma, dma((3,)), dma, dma, dma, dma,
        dma, dma((5,)),
        dma((3,)), dma((2,)), dma,
    ]
    return pl.pallas_call(
        kernel,
        out_shape=(jax.ShapeDtypeStruct((UROWS, EMB), BF),
                   jax.ShapeDtypeStruct((STRIPE, EMB), BF),
                   jax.ShapeDtypeStruct((QUERIES, EMB), BF)),
        in_specs=[hbm] * 4,
        out_specs=(hbm, hbm, hbm),
        scratch_shapes=scratch,
        compiler_params=pltpu.CompilerParams(collective_id=0, has_side_effects=True,
                                             vmem_limit_bytes=67043328),
        name='propagate',
    )(mask_blk, user_shard, item_shard, queries)


def solution(mesh):
    def device_step(mask_blk, user_shard, item_shard, queries):
        fu, fi, picked = propagate(mask_blk, user_shard, item_shard, queries.reshape(1, QUERIES))
        return scores_of(fu, fi, picked)

    return jax.shard_map(
        device_step, mesh=mesh,
        in_specs=(P('row', 'col'), P(('row', 'col'), None), P(('col', 'row'), None), P()),
        out_specs=(P(('row', 'col'), None), P(('col', 'row'), None), P(None, ('col', 'row'))),
        check_vma=False)
```

```python
import functools

import jax
import jax.numpy as jnp
from jax import lax
from jax.experimental import pallas as pl
from jax.experimental.pallas import tpu as pltpu
from jax.sharding import PartitionSpec as P

LAYERS = 3
BF = jnp.bfloat16
F32 = jnp.float32
EMB = 128
ROWS = 1024
STRIPE = 2048
CHIPS = 4
COLS = STRIPE * CHIPS
UROWS = 512
HALF = STRIPE // 2
NCH = 4
CH = HALF // NCH
LROWS = 128
NLOAD = 6
NSTAGE = 11
N_HELD = 8
QUERIES = 1024
SROWS = 128


def al(v, m):
    return pl.multiple_of(v, m)


def dot(a, b, ca, cb):
    return lax.dot_general(a, b, (((ca,), (cb,)), ((), ())), preferred_element_type=F32)


def kernel(mask_ref, ue_hbm, ie_hbm, q_hbm, fu_hbm, fi_hbm, pk_hbm, ue_ref, ie_ref, q_ref, fu_ref, fi_ref, pkf,
           a, part, r1, r2, panel, eut, upart, ursib, urz, invi, mbuf, stage,
           cs, dcs, dcr, dus, dur, usum, pkc, pks, pkz, pkx, pka,
           lsem, xs, xr, s1s, s1r, s2s, s2r, ags, agr, fws, fwr,
           usibs, usibr, uzs, uzr, uas, uar, eis, eir, dgs, dgr, dvs, dvr, pqs, pqr, ins, outs, fis):
    row = lax.axis_index('row')
    z = lax.axis_index('col')
    c = lax.rem(row, 2)
    x = lax.rem(lax.div(row, 2), 2)
    y = lax.div(row, 4)
    me = y * 2 + x

    def dev(xx, yy, cc, zz):
        return {'row': (yy * 2 + xx) * 2 + cc, 'col': zz}

    ox, oy, oc, oz = 1 - x, 1 - y, 1 - c, 1 - z
    xn, yn, dg = dev(ox, y, c, z), dev(x, oy, c, z), dev(ox, oy, c, z)
    zn, sib, zsib = dev(x, y, c, oz), dev(x, y, oc, z), dev(x, y, oc, oz)
    xnc, ync, dgc = dev(ox, y, oc, z), dev(x, oy, oc, z), dev(ox, oy, oc, z)

    def rcopy(src, dst, ss, rs, to):
        return pltpu.make_async_remote_copy(src_ref=src, dst_ref=dst, send_sem=ss, recv_sem=rs,
                                            device_id=to, device_id_type=pl.DeviceIdType.MESH)

    barrier = pltpu.get_barrier_semaphore()
    peers = (xn, yn, dg, zn, sib, zsib, xnc, ync, dgc)
    for peer in peers:
        pl.semaphore_signal(barrier, inc=1, device_id=peer, device_id_type=pl.DeviceIdType.MESH)

    n_group = ROWS // LROWS
    n_load = n_group * 2 * CHIPS

    def load_at(i, rg, par, n):
        s = 2 * i + par * c + (1 - par) * oc
        slot = lax.rem(n, NLOAD)
        return pltpu.make_async_copy(
            mask_ref.at[pl.ds(al(rg * LROWS, LROWS), LROWS), pl.ds(al(s * STRIPE, STRIPE), STRIPE)],
            mbuf.at[slot], lsem.at[slot])

    def load(n):
        first = 1 - lax.min(lax.div(n, 2 * n_group), 1)
        i = lax.div(n, 2 * n_group)
        w = lax.rem(n, 2 * n_group)
        rg = first * lax.rem(w, n_group) + (1 - first) * lax.div(w, 2)
        par = first * (1 - lax.div(w, n_group)) + (1 - first) * lax.rem(w, 2)
        return load_at(i, rg, par, n)

    inputs = [pltpu.make_async_copy(src, dst, ins.at[i])
              for i, (src, dst) in enumerate(((ie_hbm, ie_ref), (ue_hbm, ue_ref), (q_hbm, q_ref)))]
    for cp in inputs:
        cp.start()
    for n in range(NLOAD):
        load(jnp.int32(n)).start()
    cs[...] = jnp.zeros_like(cs)
    upart[pl.ds(0, ROWS), :] = jnp.zeros((ROWS, EMB), F32)
    ucol = al(c * ROWS + z * UROWS, UROWS)

    def count(i, rg, par, n, sslot):
        slot = lax.rem(n, NLOAD)
        load_at(i, rg, par, n).wait()
        cols = pl.ds(al(i * STRIPE, STRIPE), STRIPE)
        acc = jnp.zeros((8, STRIPE), F32)
        for g in range(LROWS // 16):
            v = mbuf[slot, g * 16:(g + 1) * 16, :].astype(F32)
            b = v.astype(BF)
            if par == 0:
                stage[sslot, g * 16:(g + 1) * 16, :] = b
            else:
                a[pl.ds(al(c * ROWS + rg * LROWS + g * 16, 16), 16), cols] = b
            acc = acc + v[0:8] + v[8:16]
            parts = [v[:, q * 128:(q + 1) * 128] for q in range(STRIPE // 128)]
            while len(parts) > 1:
                parts = [parts[q] + parts[q + 1] for q in range(0, len(parts), 2)]
            rsl = pl.ds(al(rg * LROWS + g * 16, 16), 16)
            upart[rsl, :] = upart[rsl, :] + parts[0]
        cs[par] = cs[par] + acc

        @pl.when(n + NLOAD < n_load)
        def _():
            load(n + NLOAD).start()

    def xcopy(m):
        i = lax.div(m, n_group)
        rg = lax.rem(m, n_group)
        slot = lax.rem(m, NSTAGE)
        return rcopy(stage.at[slot],
                     a.at[pl.ds(al(c * ROWS + rg * LROWS, LROWS), LROWS), pl.ds(al(i * STRIPE, STRIPE), STRIPE)],
                     xs.at[slot], xr.at[i], sib)

    def dgsend(p, i):
        return rcopy(dcs.at[(1, 1, 1, 0, 0, 0, 0)[i], p], dcr.at[i, p], dgs, dgr.at[p // (CHIPS - 1) if isinstance(p, int) else lax.div(p, CHIPS - 1)],
                     (xn, yn, dg, sib, xnc, ync, dgc)[i])

    def dusend(i):
        return rcopy(dus, dur.at[i], dvs, dvr, (zn, sib, zsib)[i])

    def stripe_degrees(p, par):
        v = jnp.sum(cs[par], axis=0, keepdims=True)
        for g in range(8):
            dcs[par, p, g:g + 1, :] = v[:, g * 256:(g + 1) * 256]
        cs[par] = jnp.zeros((8, STRIPE), F32)
        for k in ((6, 5, 4, 3), (2, 1, 0))[par]:
            dgsend(p, k).start()

    def own_first(rg, _):
        count(0, rg, 1, rg, 0)
        return 0

    for cp in inputs:
        cp.wait()
    usum[...] = ue_ref[...].astype(F32)
    eut[0, :, pl.ds(ucol, UROWS)] = ue_ref[...].astype(F32).T.astype(BF)
    own_rows = pl.ds(al(me * STRIPE, STRIPE), STRIPE)
    panel[0, own_rows, :] = ie_ref[...]
    pl.semaphore_wait(barrier, len(peers))

    def half_rows(q, h):
        return pl.ds(al(q * STRIPE + h * HALF, HALF), HALF)

    def ei0(i):
        q, h, to = ((me, 0, xn), (me, 1, yn), (me, 1, xn), (me, 0, yn), (y * 2 + ox, 0, yn), (oy * 2 + x, 1, xn))[i]
        blk = panel.at[0, half_rows(q, h)]
        src = ie_ref.at[pl.ds(h * HALF, HALF)] if i < 4 else blk
        return rcopy(src, blk, eis, eir.at[min(i, 2)], to)

    def ua(j, i):
        blk = eut.at[j, :, pl.ds(ucol, UROWS)]
        return rcopy(blk, blk, uas, uar.at[j], (zn, sib, zsib)[i])

    for i in range(4):
        ei0(i).start()
    for i in range(3):
        ua(0, i).start()

    lax.fori_loop(0, n_group, own_first, 0)

    def sib_first(rg, _):
        count(0, rg, 0, n_group + rg, rg)
        xcopy(rg).start()
        return 0

    lax.fori_loop(0, n_group, sib_first, 0)
    for par in range(2):
        stripe_degrees(0, par)

    def mask_step(m, _):
        i = lax.div(m, n_group)
        rg = lax.rem(m, n_group)
        w = m - n_group

        @pl.when(m >= NSTAGE)
        def _():
            xcopy(m - NSTAGE).wait_send()
        count(i, rg, 0, 2 * m, lax.rem(m, NSTAGE))

        @pl.when(lax.rem(w, 3) != 0)
        def _():
            xcopy(n_group + lax.div(2 * w, 3)).start()

        @pl.when(m == 2 * n_group)
        def _():
            ei0(0).wait_recv()
            ei0(4).start()
            ei0(1).wait_recv()
            ei0(5).start()
        @pl.when(rg == n_group - 1)
        def _():
            stripe_degrees(i, 0)
        count(i, rg, 1, 2 * m + 1, 0)

        @pl.when(i == CHIPS - 1)
        def _():
            rsl = pl.ds(al(rg * LROWS, LROWS), LROWS)
            dus[pl.ds(rg, 1), :] = jnp.sum(upart[rsl, :].T, axis=0, keepdims=True)

        @pl.when(m == CHIPS * n_group - 1)
        def _():
            for k in range(3):
                dusend(k).start()

        @pl.when(rg == n_group - 1)
        def _():
            stripe_degrees(i, 1)
        return 0

    lax.fori_loop(n_group, CHIPS * n_group, mask_step, 0)

    for k in range(N_HELD):
        xcopy(jnp.int32(CHIPS * n_group - N_HELD + k)).start()

    def all_of(ref, ss, rs):
        return rcopy(ref, ref, ss, rs, sib)

    def swapped(i):
        region = a.at[pl.ds(al(oc * ROWS, ROWS), ROWS), pl.ds(al(i * STRIPE, STRIPE), STRIPE)]
        rcopy(region, region, xs.at[0], xr.at[i], sib).wait_recv()

    def item_inverse(lo, hi, sem):
        all_of(dcr.at[:, pl.ds(lo, hi - lo)], dgs, dgr.at[sem]).wait_recv()
        for p in range(lo, hi):
            v = dcs[1, p]
            for k in range(7):
                v = v + dcr[k, p]
            v = lax.rsqrt(jnp.maximum(v, 1.0))
            for g in range(8):
                invi[0:1, p * STRIPE + g * 256:p * STRIPE + (g + 1) * 256] = v[g:g + 1, :]

    item_inverse(0, CHIPS - 1, 0)
    all_of(dur, dvs, dvr).wait_recv()
    for blk, v in ((c, dus[...] + dur[0]), (oc, dur[1] + dur[2])):
        v = lax.rsqrt(jnp.maximum(v, 1.0))
        for b in range(ROWS // 128):
            w = jnp.broadcast_to(v[b:b + 1, :], (128, 128))
            upart[pl.ds(al(blk * ROWS + b * 128, 128), 128), :] = w.T
    for i in range(3):
        swapped(i)

    def tile_q(t):
        h = lax.rem(t, 2)
        u = lax.div(t, 2)
        f1, f2 = 1 - lax.div(u, 2), lax.rem(lax.div(u + 1, 2), 2)
        fx = (1 - h) * f1 + h * f2
        fy = (1 - h) * f2 + h * f1
        return (y + fy - 2 * y * fy) * 2 + (x + fx - 2 * x * fx)

    def in_order(o):
        h = lax.rem(o, 2)
        u = lax.div(o, 2)
        swap = (1 - h) * y * ox + h * oy * x
        return h + 2 * (u + swap - 2 * u * swap)

    def s1(st, t, k, cols=pl.ds(0, CH)):
        h = lax.rem(t, 2)
        to = dev(x + (1 - h) * (1 - 2 * x), y + h * (1 - 2 * y), c, z)
        return rcopy(part.at[t, k, :, cols], r1.at[t, k, :, cols], s1s, s1r.at[k], to)

    def s2(st, h, k):
        return rcopy(part.at[4 + h, k], r2.at[h, k], s2s, s2r.at[k], (yn, xn)[h])

    def chunk_rows(q, h, k):
        return pl.ds(al(q * STRIPE + h * HALF + k * CH, CH), CH)

    def ag(st, d, h, k):
        blk = panel.at[1 - st, chunk_rows(me, h, k)]
        rs = agr.at[k] if d == h else agr.at[NCH]
        return rcopy(blk, blk, ags.at[st], rs, (xn, yn)[d])

    def fw(st, h, k):
        q = (y * 2 + ox, oy * 2 + x)[h]
        blk = panel.at[1 - st, chunk_rows(q, h, k)]
        return rcopy(blk, blk, fws.at[st], fwr, (yn, xn)[h])

    def usib(j):
        return rcopy(upart.at[pl.ds(al(oc * ROWS, ROWS), ROWS)], ursib, usibs, usibr, sib)

    def uz(j):
        return rcopy(upart.at[pl.ds(al(c * ROWS + oz * UROWS, UROWS), UROWS)], urz,
                     uzs, uzr, zn)

    qh, qq = QUERIES // 2, QUERIES // 4
    quarter = pl.ds(al(c * qh + z * qq, qq), qq)

    def pq_sib():
        return rcopy(pkc.at[pl.ds(al(oc * qh, qh), qh)], pks, pqs, pqr.at[0], sib)

    def pq_z():
        return rcopy(pkc.at[pl.ds(al(c * qh + oz * qq, qq), qq)], pkz, pqs, pqr.at[1], zn)

    def pq_x(i):
        h, to = ((0, xn), (1, yn), (0, yn), (1, xn))[i]
        src = (pkc if i < 2 else pka).at[pl.ds(al(c * qh + z * qq + h * (qq // 2), qq // 2), qq // 2)]
        return rcopy(src, pkx.at[i], pqs, pqr.at[2 + i // 2], to)

    def pq_a(i):
        return rcopy(pkf.at[quarter], pkf.at[quarter], pqs, pqr.at[4], (zn, sib, zsib)[i])

    def badd(u, v):
        return (u.astype(F32) + v.astype(F32)).astype(BF)

    def normalise(base, width):
        def norm(g, _):
            rsl = pl.ds(al(g * 128, 128), 128)
            iu = upart[rsl, :]
            for b in range(width // 128):
                cc = pl.ds(al(base + b * 128, 128), 128)
                a[rsl, cc] = a[rsl, cc] * (iu * invi[0:1, cc]).astype(BF)
            return 0
        lax.fori_loop(0, 2 * ROWS // 128, norm, 0)

    def fu_out():
        return pltpu.make_async_copy(fu_ref, fu_hbm, outs.at[0])

    def pk_out():
        return pltpu.make_async_copy(pkf, pk_hbm, outs.at[1])

    def fi_out(h, k):
        loc = pl.ds(al(h * HALF + k * CH, CH), CH)
        return pltpu.make_async_copy(fi_ref.at[loc], fi_hbm.at[loc], fis)

    for j in range(LAYERS):
        st = j % 2
        last = j == LAYERS - 1
        all_of(eut.at[j, :, pl.ds(0, 3 * UROWS)], uas, uar.at[j]).wait_recv()

        def item_tile(t, _):
            base = al(tile_q(t) * STRIPE + lax.rem(t, 2) * HALF, HALF)
            if j == 0:
                normalise(base, HALF)
            res = dot(eut[j], a[:, pl.ds(base, HALF)], 1, 0)
            for k in range(NCH):
                part[t, k] = res[:, k * CH:(k + 1) * CH]
            return 0

        def send_tile(o, _):
            t = in_order(o)
            item_tile(t, 0)
            for k in range(NCH):
                s1(st, t, k).start()
            return 0

        def first_chunk(n, _):
            h = lax.rem(n, 2)
            t = in_order(h)
            k = lax.div(n, 2)
            base = al(tile_q(t) * STRIPE + h * HALF + k * CH, CH)
            normalise(base, CH)
            part[t, k] = dot(eut[j], a[:, pl.ds(base, CH)], 1, 0)
            s1(st, t, k).start()
            return 0

        def first_half(n, _):
            h = lax.rem(n, 2)
            t = in_order(h)
            cols = pl.ds(al(lax.div(n, 2) * 128, 128), 128)
            base = al(tile_q(t) * STRIPE + h * HALF + lax.div(n, 2) * 128, 128)
            normalise(base, 128)
            part[t, 0, :, cols] = dot(eut[j], a[:, pl.ds(base, 128)], 1, 0)
            s1(st, t, 0, cols).start()
            return 0

        def stage1(k, _):
            all_of(r1.at[:, k], s1s, s1r.at[k]).wait_recv()
            for h in range(2):
                part[4 + h, k] = part[4 + h, k] + r1[2 + h, k]
                part[6 + h, k] = part[6 + h, k] + r1[h, k]
                s2(st, h, k).start()
            return 0

        def stage2(k, _):
            all_of(r2.at[:, k], s2s, s2r.at[k]).wait_recv()
            for h in range(2):
                e = (part[6 + h, k] + r2[h, k]).T.astype(BF)
                rsl = chunk_rows(me, h, k)
                if last:
                    loc = pl.ds(al(h * HALF + k * CH, CH), CH)
                    tot = ie_ref[loc, :].astype(F32) + panel[1, rsl, :].astype(F32)
                    tot = tot + panel[0, rsl, :].astype(F32) + e.astype(F32)
                    fi_ref[loc, :] = (tot * (1.0 / (LAYERS + 1))).astype(BF)
                    fi_out(h, k).start()
                else:
                    panel[1 - st, rsl, :] = e
                    ag(st, 0, h, k).start()
                    ag(st, 1, h, k).start()
            return 0

        def forward(k, _):
            all_of(panel.at[1 - st, pl.ds(0, 2 * CH)], ags.at[st], agr.at[k]).wait_recv()
            fw(st, 0, k).start()
            fw(st, 1, k).start()
            return 0

        def user_near(i, _):
            rsl = pl.ds(al(i * UROWS, UROWS), UROWS)
            tot = None
            for q in (me, y * 2 + ox, oy * 2 + x):
                ks = pl.ds(al(q * STRIPE, STRIPE), STRIPE)
                d = dot(a[rsl, ks], panel[st, ks, :], 1, 0)
                tot = d if tot is None else tot + d
            upart[rsl, :] = tot
            if j == 0:
                @pl.when(i == 2)
                def _():
                    stage1(2, 0)
            return 0

        def user_far(i, _):
            b = lax.div(i, 2)
            rsl = pl.ds(al((b * c + (1 - b) * oc) * ROWS + lax.rem(i, 2) * UROWS, UROWS), UROWS)
            ks = pl.ds(al((oy * 2 + ox) * STRIPE, STRIPE), STRIPE)
            upart[rsl, :] = upart[rsl, :] + dot(a[rsl, ks], panel[st, ks, :], 1, 0)

            @pl.when(i == 1)
            def _():
                usib(j).start()
            return 0

        def users():
            if j == 0:
                all_of(panel.at[0, pl.ds(0, 4 * HALF)], eis, eir.at[2]).wait_recv()
            else:
                all_of(panel.at[st, pl.ds(0, STRIPE)], ags.at[1 - st], agr.at[NCH]).wait_recv()
            lax.fori_loop(0, 4, user_near, 0)
            if j == 0:
                stage1(3, 0)
                stage2(0, 0)
            if j > 0:
                all_of(panel.at[st, pl.ds(0, STRIPE)], fws.at[1 - st], fwr).wait_recv()
            lax.fori_loop(0, 4, user_far, 0)

        def users_out():
            usib(j).wait_recv()
            mine = pl.ds(al(c * ROWS, ROWS), ROWS)
            upart[mine, :] = upart[mine, :] + ursib[...]
            uz(j).start()

        def user_final():
            uz(j).wait_recv()
            e = (upart[pl.ds(ucol, UROWS), :] + urz[...]).astype(BF).astype(F32)
            usum[...] = usum[...] + e
            if not last:
                eut[j + 1, :, pl.ds(ucol, UROWS)] = e.T.astype(BF)
                for i in range(3):
                    ua(j + 1, i).start()
                return
            fu = (usum[...] * (1.0 / (LAYERS + 1))).astype(BF)
            fu_ref[...] = fu
            fu_out().start()
            ids = lax.broadcasted_iota(jnp.int32, (UROWS, QUERIES), 0) + (row * 2 + z) * UROWS
            hot = jnp.where(ids == q_ref[...], 1.0, 0.0).astype(BF)
            pkc[...] = dot(hot, fu, 0, 0).astype(BF)
            pq_sib().start()

        if j == 0:
            lax.fori_loop(0, 4, first_half, 0)
            lax.fori_loop(2, 2 * NCH, first_chunk, 0)
            item_inverse(CHIPS - 1, CHIPS, 1)
            swapped(CHIPS - 1)
            lax.fori_loop(2, 4, send_tile, 0)
            lax.fori_loop(4, 8, item_tile, 0)
            lax.fori_loop(0, 2, stage1, 0)
            users()
            users_out()
            lax.fori_loop(1, NCH, stage2, 0)
            user_final()
        else:
            lax.fori_loop(0, 2, send_tile, 0)
            users()
            users_out()
            lax.fori_loop(2, 4, send_tile, 0)
            lax.fori_loop(4, 8, item_tile, 0)
            if not last:
                lax.fori_loop(0, 2, stage1, 0)
            user_final()
            if last:
                pq_sib().wait_recv()
                hrows = pl.ds(al(c * qh, qh), qh)
                pkc[hrows, :] = badd(pkc[hrows, :], pks[...])
                pq_z().start()
                stage1(0, 0)
                pq_z().wait_recv()
                pkc[quarter, :] = badd(pkc[quarter, :], pkz[...])
                for i in range(2):
                    pq_x(i).start()
                stage1(1, 0)
                all_of(pkx.at[pl.ds(0, 2)], pqs, pqr.at[2]).wait_recv()
                for i in range(2):
                    rsl = pl.ds(al(c * qh + z * qq + i * (qq // 2), qq // 2), qq // 2)
                    pka[rsl, :] = badd(pkc[rsl, :], pkx[i])
                for i in range(2, 4):
                    pq_x(i).start()
            lax.fori_loop(2, NCH, stage1, 0)
            lax.fori_loop(0, 2, stage2, 0)
            if last:
                all_of(pkx.at[pl.ds(2, 2)], pqs, pqr.at[3]).wait_recv()
                for i in range(2, 4):
                    rsl = pl.ds(al(c * qh + z * qq + (i - 2) * (qq // 2), qq // 2), qq // 2)
                    pkf[rsl, :] = badd(pka[rsl, :], pkx[i])
                for i in range(3):
                    pq_a(i).start()
            lax.fori_loop(2, NCH, stage2, 0)
        if not last:
            lax.fori_loop(0, NCH, forward, 0)

        usib(j).wait_send()
        uz(j).wait_send()
        all_of(eut.at[j, :, pl.ds(0, 3 * UROWS)], uas, uar.at[j]).wait_send()
        all_of(part.at[pl.ds(0, 4)], s1s, s1r.at[0]).wait_send()
        all_of(part.at[pl.ds(4, 2)], s2s, s2r.at[0]).wait_send()
        if j == 0:
            all_of(dcr, dgs, dgr.at[0]).wait_send()
            all_of(dur, dvs, dvr).wait_send()
            def drain_swap(m, _):
                xcopy(m).wait_send()
                return 0
            lax.fori_loop(CHIPS * n_group - NSTAGE, CHIPS * n_group, drain_swap, 0)
            all_of(panel.at[0, pl.ds(0, 6 * HALF)], eis, eir.at[2]).wait_send()
        else:
            all_of(panel.at[st, pl.ds(0, 2 * STRIPE)], ags.at[1 - st], agr.at[NCH]).wait_send()
            all_of(panel.at[st, pl.ds(0, STRIPE)], fws.at[1 - st], fwr).wait_send()

    all_of(pkf.at[pl.ds(0, 3 * qq)], pqs, pqr.at[4]).wait_recv()
    pk_out().start()
    all_of(fi_ref, pqs, pqr.at[4]).wait_send()
    pltpu.make_async_copy(fi_ref, fi_hbm, fis).wait()
    fu_out().wait()
    pk_out().wait()


def score_kernel(fu_ref, fi_ref, pk_ref, fu_out, fi_out, s_out, buf, sem, out_sem):
    copies = [pltpu.make_async_copy(fu_ref, fu_out, out_sem.at[0]),
              pltpu.make_async_copy(fi_ref, fi_out, out_sem.at[1])]
    for i in range(QUERIES // SROWS):
        rsl = pl.ds(i * SROWS, SROWS)
        buf[i] = dot(pk_ref[rsl, :], fi_ref[...], 1, 1)
        copies.append(pltpu.make_async_copy(buf.at[i], s_out.at[rsl, :], sem.at[i]))
        if i == 0:
            for cp in copies:
                cp.start()
        else:
            copies[-1].start()
    for cp in copies:
        cp.wait()


def scores_of(fu, fi, picked):
    vm = pl.BlockSpec(memory_space=pltpu.VMEM)
    hbm = pl.BlockSpec(memory_space=pl.ANY)
    return pl.pallas_call(
        score_kernel,
        out_shape=(jax.ShapeDtypeStruct(fu.shape, BF), jax.ShapeDtypeStruct(fi.shape, BF),
                   jax.ShapeDtypeStruct((QUERIES, STRIPE), F32)),
        in_specs=[vm, vm, vm],
        out_specs=(hbm, hbm, hbm),
        scratch_shapes=[pltpu.VMEM((QUERIES // SROWS, SROWS, STRIPE), F32),
                        pltpu.SemaphoreType.DMA((QUERIES // SROWS,)), pltpu.SemaphoreType.DMA((2,))],
        name='scores',
    )(fu, fi, picked)


def propagate(mask_blk, user_shard, item_shard, queries):
    hbm = pl.BlockSpec(memory_space=pl.ANY)
    dma = pltpu.SemaphoreType.DMA
    qh, qq = QUERIES // 2, QUERIES // 4
    scratch = [
        pltpu.VMEM((UROWS, EMB), BF),
        pltpu.VMEM((STRIPE, EMB), BF),
        pltpu.VMEM((1, QUERIES), jnp.int32),
        pltpu.VMEM((UROWS, EMB), BF),
        pltpu.VMEM((STRIPE, EMB), BF),
        pltpu.VMEM((QUERIES, EMB), BF),
        pltpu.VMEM((2 * ROWS, COLS), BF),
        pltpu.VMEM((8, NCH, EMB, CH), F32),
        pltpu.VMEM((4, NCH, EMB, CH), F32),
        pltpu.VMEM((2, NCH, EMB, CH), F32),
        pltpu.VMEM((2, COLS, EMB), BF),
        pltpu.VMEM((LAYERS, EMB, 2 * ROWS), BF),
        pltpu.VMEM((2 * ROWS, EMB), F32),
        pltpu.VMEM((ROWS, EMB), F32),
        pltpu.VMEM((UROWS, EMB), F32),
        pltpu.VMEM((1, COLS), F32),
        pltpu.VMEM((NLOAD, LROWS, STRIPE), jnp.int32),
        pltpu.VMEM((NSTAGE, LROWS, STRIPE), BF),
        pltpu.VMEM((2, 8, STRIPE), F32),
        pltpu.VMEM((2, CHIPS, 8, STRIPE // 8), F32),
        pltpu.VMEM((7, CHIPS, 8, STRIPE // 8), F32),
        pltpu.VMEM((8, ROWS // 8), F32),
        pltpu.VMEM((3, 8, ROWS // 8), F32),
        pltpu.VMEM((UROWS, EMB), F32),
        pltpu.VMEM((QUERIES, EMB), BF),
        pltpu.VMEM((qh, EMB), BF),
        pltpu.VMEM((qq, EMB), BF),
        pltpu.VMEM((4, qq // 2, EMB), BF),
        pltpu.VMEM((QUERIES, EMB), BF),
        dma((NLOAD,)), dma((NSTAGE,)), dma((CHIPS,)),
        dma, dma((NCH,)),
        dma, dma((NCH,)),
        dma((2,)), dma((NCH + 1,)),
        dma((2,)), dma,
        dma, dma, dma, dma,
        dma, dma((LAYERS,)),
        dma, dma((3,)), dma, dma((2,)), dma, dma,
        dma, dma((5,)),
        dma((3,)), dma((2,)), dma,
    ]
    return pl.pallas_call(
        kernel,
        out_shape=(jax.ShapeDtypeStruct((UROWS, EMB), BF),
                   jax.ShapeDtypeStruct((STRIPE, EMB), BF),
                   jax.ShapeDtypeStruct((QUERIES, EMB), BF)),
        in_specs=[hbm] * 4,
        out_specs=(hbm, hbm, hbm),
        scratch_shapes=scratch,
        compiler_params=pltpu.CompilerParams(collective_id=0, has_side_effects=True,
                                             vmem_limit_bytes=67043328),
        name='propagate',
    )(mask_blk, user_shard, item_shard, queries)


def solution(mesh):
    def device_step(mask_blk, user_shard, item_shard, queries):
        fu, fi, picked = propagate(mask_blk, user_shard, item_shard, queries.reshape(1, QUERIES))
        return scores_of(fu, fi, picked)

    return jax.shard_map(
        device_step, mesh=mesh,
        in_specs=(P('row', 'col'), P(('row', 'col'), None), P(('col', 'row'), None), P()),
        out_specs=(P(('row', 'col'), None), P(('col', 'row'), None), P(None, ('col', 'row'))),
        check_vma=False)
```

```python
import functools

import jax
import jax.numpy as jnp
from jax import lax
from jax.experimental import pallas as pl
from jax.experimental.pallas import tpu as pltpu
from jax.sharding import PartitionSpec as P

LAYERS = 3
BF = jnp.bfloat16
F32 = jnp.float32
EMB = 128
ROWS = 1024
STRIPE = 2048
CHIPS = 4
COLS = STRIPE * CHIPS
UROWS = 512
HALF = STRIPE // 2
NCH = 4
CH = HALF // NCH
LROWS = 128
NLOAD = 6
NSTAGE = 11
N_HELD = 8
QUERIES = 1024
SROWS = 128


def al(v, m):
    return pl.multiple_of(v, m)


def dot(a, b, ca, cb):
    return lax.dot_general(a, b, (((ca,), (cb,)), ((), ())), preferred_element_type=F32)


def kernel(mask_ref, ue_hbm, ie_hbm, q_hbm, fu_ref, fi_ref, pk_ref, ue_ref, ie_ref, q_ref, pkf,
           a, part, r1, r2, panel, eut, upart, ursib, urz, invi, mbuf, stage,
           cs, dcs, dcr, dus, dur, usum, pkc, pks, pkz, pkx, pka,
           lsem, xs, xr, s1s, s1r, s2s, s2r, ags, agr, fws, fwr,
           usibs, usibr, uzs, uzr, uas, uar, eis, eir, dgs, dgr, dvs, dvr, pqs, pqr, ins):
    row = lax.axis_index('row')
    z = lax.axis_index('col')
    c = lax.rem(row, 2)
    x = lax.rem(lax.div(row, 2), 2)
    y = lax.div(row, 4)
    me = y * 2 + x

    def dev(xx, yy, cc, zz):
        return {'row': (yy * 2 + xx) * 2 + cc, 'col': zz}

    ox, oy, oc, oz = 1 - x, 1 - y, 1 - c, 1 - z
    xn, yn, dg = dev(ox, y, c, z), dev(x, oy, c, z), dev(ox, oy, c, z)
    zn, sib, zsib = dev(x, y, c, oz), dev(x, y, oc, z), dev(x, y, oc, oz)
    xnc, ync, dgc = dev(ox, y, oc, z), dev(x, oy, oc, z), dev(ox, oy, oc, z)

    def rcopy(src, dst, ss, rs, to):
        return pltpu.make_async_remote_copy(src_ref=src, dst_ref=dst, send_sem=ss, recv_sem=rs,
                                            device_id=to, device_id_type=pl.DeviceIdType.MESH)

    barrier = pltpu.get_barrier_semaphore()
    peers = (xn, yn, dg, zn, sib, zsib, xnc, ync, dgc)
    for peer in peers:
        pl.semaphore_signal(barrier, inc=1, device_id=peer, device_id_type=pl.DeviceIdType.MESH)

    n_group = ROWS // LROWS
    n_load = n_group * 2 * CHIPS

    def load_at(i, rg, par, n):
        s = 2 * i + par * c + (1 - par) * oc
        slot = lax.rem(n, NLOAD)
        return pltpu.make_async_copy(
            mask_ref.at[pl.ds(al(rg * LROWS, LROWS), LROWS), pl.ds(al(s * STRIPE, STRIPE), STRIPE)],
            mbuf.at[slot], lsem.at[slot])

    def load(n):
        first = 1 - lax.min(lax.div(n, 2 * n_group), 1)
        i = lax.div(n, 2 * n_group)
        w = lax.rem(n, 2 * n_group)
        rg = first * lax.rem(w, n_group) + (1 - first) * lax.div(w, 2)
        par = first * (1 - lax.div(w, n_group)) + (1 - first) * lax.rem(w, 2)
        return load_at(i, rg, par, n)

    inputs = [pltpu.make_async_copy(src, dst, ins.at[i])
              for i, (src, dst) in enumerate(((ie_hbm, ie_ref), (ue_hbm, ue_ref), (q_hbm, q_ref)))]
    for cp in inputs:
        cp.start()
    for n in range(NLOAD):
        load(jnp.int32(n)).start()
    cs[...] = jnp.zeros_like(cs)
    upart[pl.ds(0, ROWS), :] = jnp.zeros((ROWS, EMB), F32)
    ucol = al(c * ROWS + z * UROWS, UROWS)

    def count(i, rg, par, n, sslot):
        slot = lax.rem(n, NLOAD)
        load_at(i, rg, par, n).wait()
        cols = pl.ds(al(i * STRIPE, STRIPE), STRIPE)
        acc = jnp.zeros((8, STRIPE), F32)
        for g in range(LROWS // 16):
            v = mbuf[slot, g * 16:(g + 1) * 16, :].astype(F32)
            b = v.astype(BF)
            if par == 0:
                stage[sslot, g * 16:(g + 1) * 16, :] = b
            else:
                a[pl.ds(al(c * ROWS + rg * LROWS + g * 16, 16), 16), cols] = b
            acc = acc + v[0:8] + v[8:16]
            parts = [v[:, q * 128:(q + 1) * 128] for q in range(STRIPE // 128)]
            while len(parts) > 1:
                parts = [parts[q] + parts[q + 1] for q in range(0, len(parts), 2)]
            rsl = pl.ds(al(rg * LROWS + g * 16, 16), 16)
            upart[rsl, :] = upart[rsl, :] + parts[0]
        cs[par] = cs[par] + acc

        @pl.when(n + NLOAD < n_load)
        def _():
            load(n + NLOAD).start()

    def xcopy(m):
        i = lax.div(m, n_group)
        rg = lax.rem(m, n_group)
        slot = lax.rem(m, NSTAGE)
        return rcopy(stage.at[slot],
                     a.at[pl.ds(al(c * ROWS + rg * LROWS, LROWS), LROWS), pl.ds(al(i * STRIPE, STRIPE), STRIPE)],
                     xs.at[slot], xr.at[i], sib)

    def dgsend(p, i):
        return rcopy(dcs.at[(1, 1, 1, 0, 0, 0, 0)[i], p], dcr.at[i, p], dgs, dgr.at[p // (CHIPS - 1) if isinstance(p, int) else lax.div(p, CHIPS - 1)],
                     (xn, yn, dg, sib, xnc, ync, dgc)[i])

    def dusend(i):
        return rcopy(dus, dur.at[i], dvs, dvr, (zn, sib, zsib)[i])

    def stripe_degrees(p, par):
        v = jnp.sum(cs[par], axis=0, keepdims=True)
        for g in range(8):
            dcs[par, p, g:g + 1, :] = v[:, g * 256:(g + 1) * 256]
        cs[par] = jnp.zeros((8, STRIPE), F32)
        for k in ((6, 5, 4, 3), (2, 1, 0))[par]:
            dgsend(p, k).start()

    def own_first(rg, _):
        count(0, rg, 1, rg, 0)
        return 0

    for cp in inputs:
        cp.wait()
    usum[...] = ue_ref[...].astype(F32)
    eut[0, :, pl.ds(ucol, UROWS)] = ue_ref[...].astype(F32).T.astype(BF)
    own_rows = pl.ds(al(me * STRIPE, STRIPE), STRIPE)
    panel[0, own_rows, :] = ie_ref[...]
    pl.semaphore_wait(barrier, len(peers))

    def half_rows(q, h):
        return pl.ds(al(q * STRIPE + h * HALF, HALF), HALF)

    def ei0(i):
        q, h, to = ((me, 0, xn), (me, 1, yn), (me, 1, xn), (me, 0, yn), (y * 2 + ox, 0, yn), (oy * 2 + x, 1, xn))[i]
        blk = panel.at[0, half_rows(q, h)]
        src = ie_ref.at[pl.ds(h * HALF, HALF)] if i < 4 else blk
        return rcopy(src, blk, eis, eir.at[min(i, 2)], to)

    def ua(j, i):
        blk = eut.at[j, :, pl.ds(ucol, UROWS)]
        return rcopy(blk, blk, uas, uar.at[j], (zn, sib, zsib)[i])

    for i in range(4):
        ei0(i).start()
    for i in range(3):
        ua(0, i).start()

    lax.fori_loop(0, n_group, own_first, 0)

    def sib_first(rg, _):
        count(0, rg, 0, n_group + rg, rg)
        xcopy(rg).start()
        return 0

    lax.fori_loop(0, n_group, sib_first, 0)
    for par in range(2):
        stripe_degrees(0, par)

    def mask_step(m, _):
        i = lax.div(m, n_group)
        rg = lax.rem(m, n_group)
        w = m - n_group

        @pl.when(m >= NSTAGE)
        def _():
            xcopy(m - NSTAGE).wait_send()
        count(i, rg, 0, 2 * m, lax.rem(m, NSTAGE))

        @pl.when(lax.rem(w, 3) != 0)
        def _():
            xcopy(n_group + lax.div(2 * w, 3)).start()

        @pl.when(m == 2 * n_group)
        def _():
            ei0(0).wait_recv()
            ei0(4).start()
            ei0(1).wait_recv()
            ei0(5).start()
        @pl.when(rg == n_group - 1)
        def _():
            stripe_degrees(i, 0)
        count(i, rg, 1, 2 * m + 1, 0)

        @pl.when(i == CHIPS - 1)
        def _():
            rsl = pl.ds(al(rg * LROWS, LROWS), LROWS)
            dus[pl.ds(rg, 1), :] = jnp.sum(upart[rsl, :].T, axis=0, keepdims=True)

        @pl.when(m == CHIPS * n_group - 1)
        def _():
            for k in range(3):
                dusend(k).start()

        @pl.when(rg == n_group - 1)
        def _():
            stripe_degrees(i, 1)
        return 0

    lax.fori_loop(n_group, CHIPS * n_group, mask_step, 0)

    for k in range(N_HELD):
        xcopy(jnp.int32(CHIPS * n_group - N_HELD + k)).start()

    def all_of(ref, ss, rs):
        return rcopy(ref, ref, ss, rs, sib)

    def swapped(i):
        region = a.at[pl.ds(al(oc * ROWS, ROWS), ROWS), pl.ds(al(i * STRIPE, STRIPE), STRIPE)]
        rcopy(region, region, xs.at[0], xr.at[i], sib).wait_recv()

    def item_inverse(lo, hi, sem):
        all_of(dcr.at[:, pl.ds(lo, hi - lo)], dgs, dgr.at[sem]).wait_recv()
        for p in range(lo, hi):
            v = dcs[1, p]
            for k in range(7):
                v = v + dcr[k, p]
            v = lax.rsqrt(jnp.maximum(v, 1.0))
            for g in range(8):
                invi[0:1, p * STRIPE + g * 256:p * STRIPE + (g + 1) * 256] = v[g:g + 1, :]

    item_inverse(0, CHIPS - 1, 0)
    all_of(dur, dvs, dvr).wait_recv()
    for blk, v in ((c, dus[...] + dur[0]), (oc, dur[1] + dur[2])):
        v = lax.rsqrt(jnp.maximum(v, 1.0))
        for b in range(ROWS // 128):
            w = jnp.broadcast_to(v[b:b + 1, :], (128, 128))
            upart[pl.ds(al(blk * ROWS + b * 128, 128), 128), :] = w.T
    for i in range(3):
        swapped(i)

    def tile_q(t):
        h = lax.rem(t, 2)
        u = lax.div(t, 2)
        f1, f2 = 1 - lax.div(u, 2), lax.rem(lax.div(u + 1, 2), 2)
        fx = (1 - h) * f1 + h * f2
        fy = (1 - h) * f2 + h * f1
        return (y + fy - 2 * y * fy) * 2 + (x + fx - 2 * x * fx)

    def in_order(o):
        h = lax.rem(o, 2)
        u = lax.div(o, 2)
        swap = (1 - h) * y * ox + h * oy * x
        return h + 2 * (u + swap - 2 * u * swap)

    def s1(st, t, k, cols=pl.ds(0, CH)):
        h = lax.rem(t, 2)
        to = dev(x + (1 - h) * (1 - 2 * x), y + h * (1 - 2 * y), c, z)
        return rcopy(part.at[t, k, :, cols], r1.at[t, k, :, cols], s1s, s1r.at[k], to)

    def s2(st, h, k):
        return rcopy(part.at[4 + h, k], r2.at[h, k], s2s, s2r.at[k], (yn, xn)[h])

    def chunk_rows(q, h, k):
        return pl.ds(al(q * STRIPE + h * HALF + k * CH, CH), CH)

    def ag(st, d, h, k):
        blk = panel.at[1 - st, chunk_rows(me, h, k)]
        rs = agr.at[k] if d == h else agr.at[NCH]
        return rcopy(blk, blk, ags.at[st], rs, (xn, yn)[d])

    def fw(st, h, k):
        q = (y * 2 + ox, oy * 2 + x)[h]
        blk = panel.at[1 - st, chunk_rows(q, h, k)]
        return rcopy(blk, blk, fws.at[st], fwr, (yn, xn)[h])

    def usib(j):
        return rcopy(upart.at[pl.ds(al(oc * ROWS, ROWS), ROWS)], ursib, usibs, usibr, sib)

    def uz(j):
        return rcopy(upart.at[pl.ds(al(c * ROWS + oz * UROWS, UROWS), UROWS)], urz,
                     uzs, uzr, zn)

    qh, qq = QUERIES // 2, QUERIES // 4
    quarter = pl.ds(al(c * qh + z * qq, qq), qq)

    def pq_sib():
        return rcopy(pkc.at[pl.ds(al(oc * qh, qh), qh)], pks, pqs, pqr.at[0], sib)

    def pq_z():
        return rcopy(pkc.at[pl.ds(al(c * qh + oz * qq, qq), qq)], pkz, pqs, pqr.at[1], zn)

    def pq_x(i):
        h, to = ((0, xn), (1, yn), (0, yn), (1, xn))[i]
        src = (pkc if i < 2 else pka).at[pl.ds(al(c * qh + z * qq + h * (qq // 2), qq // 2), qq // 2)]
        return rcopy(src, pkx.at[i], pqs, pqr.at[2 + i // 2], to)

    def pq_a(i):
        return rcopy(pkf.at[quarter], pkf.at[quarter], pqs, pqr.at[4], (zn, sib, zsib)[i])

    def badd(u, v):
        return (u.astype(F32) + v.astype(F32)).astype(BF)

    def normalise(base, width):
        def norm(g, _):
            rsl = pl.ds(al(g * 128, 128), 128)
            iu = upart[rsl, :]
            for b in range(width // 128):
                cc = pl.ds(al(base + b * 128, 128), 128)
                a[rsl, cc] = a[rsl, cc] * (iu * invi[0:1, cc]).astype(BF)
            return 0
        lax.fori_loop(0, 2 * ROWS // 128, norm, 0)

    for j in range(LAYERS):
        st = j % 2
        last = j == LAYERS - 1
        all_of(eut.at[j, :, pl.ds(0, 3 * UROWS)], uas, uar.at[j]).wait_recv()

        def item_tile(t, _):
            base = al(tile_q(t) * STRIPE + lax.rem(t, 2) * HALF, HALF)
            if j == 0:
                normalise(base, HALF)
            res = dot(eut[j], a[:, pl.ds(base, HALF)], 1, 0)
            for k in range(NCH):
                part[t, k] = res[:, k * CH:(k + 1) * CH]
            return 0

        def send_tile(o, _):
            t = in_order(o)
            item_tile(t, 0)
            for k in range(NCH):
                s1(st, t, k).start()
            return 0

        def first_chunk(n, _):
            h = lax.rem(n, 2)
            t = in_order(h)
            k = lax.div(n, 2)
            base = al(tile_q(t) * STRIPE + h * HALF + k * CH, CH)
            normalise(base, CH)
            part[t, k] = dot(eut[j], a[:, pl.ds(base, CH)], 1, 0)
            s1(st, t, k).start()
            return 0

        def first_half(n, _):
            h = lax.rem(n, 2)
            t = in_order(h)
            cols = pl.ds(al(lax.div(n, 2) * 128, 128), 128)
            base = al(tile_q(t) * STRIPE + h * HALF + lax.div(n, 2) * 128, 128)
            normalise(base, 128)
            part[t, 0, :, cols] = dot(eut[j], a[:, pl.ds(base, 128)], 1, 0)
            s1(st, t, 0, cols).start()
            return 0

        def stage1(k, _):
            all_of(r1.at[:, k], s1s, s1r.at[k]).wait_recv()
            for h in range(2):
                part[4 + h, k] = part[4 + h, k] + r1[2 + h, k]
                part[6 + h, k] = part[6 + h, k] + r1[h, k]
                s2(st, h, k).start()
            return 0

        def stage2(k, _):
            all_of(r2.at[:, k], s2s, s2r.at[k]).wait_recv()
            for h in range(2):
                e = (part[6 + h, k] + r2[h, k]).T.astype(BF)
                rsl = chunk_rows(me, h, k)
                if last:
                    loc = pl.ds(al(h * HALF + k * CH, CH), CH)
                    tot = ie_ref[loc, :].astype(F32) + panel[1, rsl, :].astype(F32)
                    tot = tot + panel[0, rsl, :].astype(F32) + e.astype(F32)
                    fi_ref[loc, :] = (tot * (1.0 / (LAYERS + 1))).astype(BF)
                else:
                    panel[1 - st, rsl, :] = e
                    ag(st, 0, h, k).start()
                    ag(st, 1, h, k).start()
            return 0

        def forward(k, _):
            all_of(panel.at[1 - st, pl.ds(0, 2 * CH)], ags.at[st], agr.at[k]).wait_recv()
            fw(st, 0, k).start()
            fw(st, 1, k).start()
            return 0

        def user_near(i, _):
            rsl = pl.ds(al(i * UROWS, UROWS), UROWS)
            tot = None
            for q in (me, y * 2 + ox, oy * 2 + x):
                ks = pl.ds(al(q * STRIPE, STRIPE), STRIPE)
                d = dot(a[rsl, ks], panel[st, ks, :], 1, 0)
                tot = d if tot is None else tot + d
            upart[rsl, :] = tot
            if j == 0:
                @pl.when(i == 2)
                def _():
                    stage1(2, 0)
            return 0

        def user_far(i, _):
            b = lax.div(i, 2)
            rsl = pl.ds(al((b * c + (1 - b) * oc) * ROWS + lax.rem(i, 2) * UROWS, UROWS), UROWS)
            ks = pl.ds(al((oy * 2 + ox) * STRIPE, STRIPE), STRIPE)
            upart[rsl, :] = upart[rsl, :] + dot(a[rsl, ks], panel[st, ks, :], 1, 0)

            @pl.when(i == 1)
            def _():
                usib(j).start()
            return 0

        def users():
            if j == 0:
                all_of(panel.at[0, pl.ds(0, 4 * HALF)], eis, eir.at[2]).wait_recv()
            else:
                all_of(panel.at[st, pl.ds(0, STRIPE)], ags.at[1 - st], agr.at[NCH]).wait_recv()
            lax.fori_loop(0, 4, user_near, 0)
            if j == 0:
                stage1(3, 0)
                stage2(0, 0)
            if j > 0:
                all_of(panel.at[st, pl.ds(0, STRIPE)], fws.at[1 - st], fwr).wait_recv()
            lax.fori_loop(0, 4, user_far, 0)

        def users_out():
            usib(j).wait_recv()
            mine = pl.ds(al(c * ROWS, ROWS), ROWS)
            upart[mine, :] = upart[mine, :] + ursib[...]
            uz(j).start()

        def user_final():
            uz(j).wait_recv()
            e = (upart[pl.ds(ucol, UROWS), :] + urz[...]).astype(BF).astype(F32)
            usum[...] = usum[...] + e
            if not last:
                eut[j + 1, :, pl.ds(ucol, UROWS)] = e.T.astype(BF)
                for i in range(3):
                    ua(j + 1, i).start()
                return
            fu = (usum[...] * (1.0 / (LAYERS + 1))).astype(BF)
            fu_ref[...] = fu
            ids = lax.broadcasted_iota(jnp.int32, (UROWS, QUERIES), 0) + (row * 2 + z) * UROWS
            hot = jnp.where(ids == q_ref[...], 1.0, 0.0).astype(BF)
            pkc[...] = dot(hot, fu, 0, 0).astype(BF)
            pq_sib().start()

        if j == 0:
            lax.fori_loop(0, 4, first_half, 0)
            lax.fori_loop(2, 2 * NCH, first_chunk, 0)
            item_inverse(CHIPS - 1, CHIPS, 1)
            swapped(CHIPS - 1)
            lax.fori_loop(2, 4, send_tile, 0)
            lax.fori_loop(4, 8, item_tile, 0)
            lax.fori_loop(0, 2, stage1, 0)
            users()
            users_out()
            lax.fori_loop(1, NCH, stage2, 0)
            user_final()
        else:
            lax.fori_loop(0, 2, send_tile, 0)
            users()
            users_out()
            lax.fori_loop(2, 4, send_tile, 0)
            lax.fori_loop(4, 8, item_tile, 0)
            if not last:
                lax.fori_loop(0, 2, stage1, 0)
            user_final()
            if last:
                pq_sib().wait_recv()
                hrows = pl.ds(al(c * qh, qh), qh)
                pkc[hrows, :] = badd(pkc[hrows, :], pks[...])
                pq_z().start()
                stage1(0, 0)
                pq_z().wait_recv()
                pkc[quarter, :] = badd(pkc[quarter, :], pkz[...])
                for i in range(2):
                    pq_x(i).start()
                stage1(1, 0)
                all_of(pkx.at[pl.ds(0, 2)], pqs, pqr.at[2]).wait_recv()
                for i in range(2):
                    rsl = pl.ds(al(c * qh + z * qq + i * (qq // 2), qq // 2), qq // 2)
                    pka[rsl, :] = badd(pkc[rsl, :], pkx[i])
                for i in range(2, 4):
                    pq_x(i).start()
            lax.fori_loop(2, NCH, stage1, 0)
            lax.fori_loop(0, 2, stage2, 0)
            if last:
                all_of(pkx.at[pl.ds(2, 2)], pqs, pqr.at[3]).wait_recv()
                for i in range(2, 4):
                    rsl = pl.ds(al(c * qh + z * qq + (i - 2) * (qq // 2), qq // 2), qq // 2)
                    pkf[rsl, :] = badd(pka[rsl, :], pkx[i])
                for i in range(3):
                    pq_a(i).start()
            lax.fori_loop(2, NCH, stage2, 0)
        if not last:
            lax.fori_loop(0, NCH, forward, 0)

        usib(j).wait_send()
        uz(j).wait_send()
        all_of(eut.at[j, :, pl.ds(0, 3 * UROWS)], uas, uar.at[j]).wait_send()
        all_of(part.at[pl.ds(0, 4)], s1s, s1r.at[0]).wait_send()
        all_of(part.at[pl.ds(4, 2)], s2s, s2r.at[0]).wait_send()
        if j == 0:
            all_of(dcr, dgs, dgr.at[0]).wait_send()
            all_of(dur, dvs, dvr).wait_send()
            def drain_swap(m, _):
                xcopy(m).wait_send()
                return 0
            lax.fori_loop(CHIPS * n_group - NSTAGE, CHIPS * n_group, drain_swap, 0)
            all_of(panel.at[0, pl.ds(0, 6 * HALF)], eis, eir.at[2]).wait_send()
        else:
            all_of(panel.at[st, pl.ds(0, 2 * STRIPE)], ags.at[1 - st], agr.at[NCH]).wait_send()
            all_of(panel.at[st, pl.ds(0, STRIPE)], fws.at[1 - st], fwr).wait_send()

    all_of(pkf.at[pl.ds(0, 3 * qq)], pqs, pqr.at[4]).wait_recv()
    pk_ref[...] = pkf[...]
    all_of(ie_ref, pqs, pqr.at[4]).wait_send()


def score_kernel(fu_ref, fi_ref, pk_ref, fu_out, fi_out, s_out, buf, sem, out_sem):
    copies = [pltpu.make_async_copy(fu_ref, fu_out, out_sem.at[0]),
              pltpu.make_async_copy(fi_ref, fi_out, out_sem.at[1])]
    for i in range(QUERIES // SROWS):
        rsl = pl.ds(i * SROWS, SROWS)
        buf[i] = dot(pk_ref[rsl, :], fi_ref[...], 1, 1)
        copies.append(pltpu.make_async_copy(buf.at[i], s_out.at[rsl, :], sem.at[i]))
        if i == 0:
            for cp in copies:
                cp.start()
        else:
            copies[-1].start()
    for cp in copies:
        cp.wait()


def scores_of(fu, fi, picked):
    vm = pl.BlockSpec(memory_space=pltpu.VMEM)
    hbm = pl.BlockSpec(memory_space=pl.ANY)
    return pl.pallas_call(
        score_kernel,
        out_shape=(jax.ShapeDtypeStruct(fu.shape, BF), jax.ShapeDtypeStruct(fi.shape, BF),
                   jax.ShapeDtypeStruct((QUERIES, STRIPE), F32)),
        in_specs=[vm, vm, vm],
        out_specs=(hbm, hbm, hbm),
        scratch_shapes=[pltpu.VMEM((QUERIES // SROWS, SROWS, STRIPE), F32),
                        pltpu.SemaphoreType.DMA((QUERIES // SROWS,)), pltpu.SemaphoreType.DMA((2,))],
        compiler_params=pltpu.CompilerParams(vmem_limit_bytes=16 * 1024 * 1024),
        name='scores',
    )(fu, fi, picked)


def propagate(mask_blk, user_shard, item_shard, queries):
    hbm = pl.BlockSpec(memory_space=pl.ANY)
    vm = pl.BlockSpec(memory_space=pltpu.VMEM)
    dma = pltpu.SemaphoreType.DMA
    qh, qq = QUERIES // 2, QUERIES // 4
    scratch = [
        pltpu.VMEM((UROWS, EMB), BF),
        pltpu.VMEM((STRIPE, EMB), BF),
        pltpu.VMEM((1, QUERIES), jnp.int32),
        pltpu.VMEM((QUERIES, EMB), BF),
        pltpu.VMEM((2 * ROWS, COLS), BF),
        pltpu.VMEM((8, NCH, EMB, CH), F32),
        pltpu.VMEM((4, NCH, EMB, CH), F32),
        pltpu.VMEM((2, NCH, EMB, CH), F32),
        pltpu.VMEM((2, COLS, EMB), BF),
        pltpu.VMEM((LAYERS, EMB, 2 * ROWS), BF),
        pltpu.VMEM((2 * ROWS, EMB), F32),
        pltpu.VMEM((ROWS, EMB), F32),
        pltpu.VMEM((UROWS, EMB), F32),
        pltpu.VMEM((1, COLS), F32),
        pltpu.VMEM((NLOAD, LROWS, STRIPE), jnp.int32),
        pltpu.VMEM((NSTAGE, LROWS, STRIPE), BF),
        pltpu.VMEM((2, 8, STRIPE), F32),
        pltpu.VMEM((2, CHIPS, 8, STRIPE // 8), F32),
        pltpu.VMEM((7, CHIPS, 8, STRIPE // 8), F32),
        pltpu.VMEM((8, ROWS // 8), F32),
        pltpu.VMEM((3, 8, ROWS // 8), F32),
        pltpu.VMEM((UROWS, EMB), F32),
        pltpu.VMEM((QUERIES, EMB), BF),
        pltpu.VMEM((qh, EMB), BF),
        pltpu.VMEM((qq, EMB), BF),
        pltpu.VMEM((4, qq // 2, EMB), BF),
        pltpu.VMEM((QUERIES, EMB), BF),
        dma((NLOAD,)), dma((NSTAGE,)), dma((CHIPS,)),
        dma, dma((NCH,)),
        dma, dma((NCH,)),
        dma((2,)), dma((NCH + 1,)),
        dma((2,)), dma,
        dma, dma, dma, dma,
        dma, dma((LAYERS,)),
        dma, dma((3,)), dma, dma((2,)), dma, dma,
        dma, dma((5,)),
        dma((3,)),
    ]
    return pl.pallas_call(
        kernel,
        out_shape=(pltpu.VMEM((UROWS, EMB), BF), pltpu.VMEM((STRIPE, EMB), BF), pltpu.VMEM((QUERIES, EMB), BF)),
        in_specs=[hbm] * 4,
        out_specs=(vm, vm, vm),
        scratch_shapes=scratch,
        compiler_params=pltpu.CompilerParams(collective_id=0, has_side_effects=True,
                                             vmem_limit_bytes=64487424),
        name='propagate',
    )(mask_blk, user_shard, item_shard, queries)


def solution(mesh):
    def device_step(mask_blk, user_shard, item_shard, queries):
        fu, fi, picked = propagate(mask_blk, user_shard, item_shard, queries.reshape(1, QUERIES))
        return scores_of(fu, fi, picked)

    return jax.shard_map(
        device_step, mesh=mesh,
        in_specs=(P('row', 'col'), P(('row', 'col'), None), P(('col', 'row'), None), P()),
        out_specs=(P(('row', 'col'), None), P(('col', 'row'), None), P(None, ('col', 'row'))),
        check_vma=False)
```

```python
import functools

import jax
import jax.numpy as jnp
from jax import lax
from jax.experimental import pallas as pl
from jax.experimental.pallas import tpu as pltpu
from jax.sharding import PartitionSpec as P

LAYERS = 3
BF = jnp.bfloat16
F32 = jnp.float32
EMB = 128
ROWS = 1024
STRIPE = 2048
CHIPS = 4
COLS = STRIPE * CHIPS
UROWS = 512
HALF = STRIPE // 2
NCH = 4
CH = HALF // NCH
LROWS = 128
NLOAD = 6
NSTAGE = 11
N_HELD = 8
QUERIES = 1024
SROWS = 128


def al(v, m):
    return pl.multiple_of(v, m)


def dot(a, b, ca, cb):
    return lax.dot_general(a, b, (((ca,), (cb,)), ((), ())), preferred_element_type=F32)


def kernel(mask_ref, ue_hbm, ie_hbm, q_hbm, fu_ref, fi_ref, pk_ref, ue_ref, ie_ref, q_ref, pkf,
           a, part, r1, r2, panel, eut, upart, ursib, urz, invi, mbuf, stage,
           cs, dcs, dcr, dus, dur, usum, pkc, pks, pkz, pkx, pka,
           lsem, xs, xr, s1s, s1r, s2s, ags, agr, fws, fwr,
           usibs, usibr, uzs, uzr, uas, uar, eis, eir, dgs, dgr, dvs, dvr, pqs, ins):
    row = lax.axis_index('row')
    z = lax.axis_index('col')
    c = lax.rem(row, 2)
    x = lax.rem(lax.div(row, 2), 2)
    y = lax.div(row, 4)
    me = y * 2 + x

    def dev(xx, yy, cc, zz):
        return {'row': (yy * 2 + xx) * 2 + cc, 'col': zz}

    ox, oy, oc, oz = 1 - x, 1 - y, 1 - c, 1 - z
    xn, yn, dg = dev(ox, y, c, z), dev(x, oy, c, z), dev(ox, oy, c, z)
    zn, sib, zsib = dev(x, y, c, oz), dev(x, y, oc, z), dev(x, y, oc, oz)
    xnc, ync, dgc = dev(ox, y, oc, z), dev(x, oy, oc, z), dev(ox, oy, oc, z)

    def rcopy(src, dst, ss, rs, to):
        return pltpu.make_async_remote_copy(src_ref=src, dst_ref=dst, send_sem=ss, recv_sem=rs,
                                            device_id=to, device_id_type=pl.DeviceIdType.MESH)

    barrier = pltpu.get_barrier_semaphore()
    peers = (xn, yn, dg, zn, sib, zsib, xnc, ync, dgc)
    for peer in peers:
        pl.semaphore_signal(barrier, inc=1, device_id=peer, device_id_type=pl.DeviceIdType.MESH)

    n_group = ROWS // LROWS
    n_load = n_group * 2 * CHIPS

    def load_at(i, rg, par, n):
        s = 2 * i + par * c + (1 - par) * oc
        slot = lax.rem(n, NLOAD)
        return pltpu.make_async_copy(
            mask_ref.at[pl.ds(al(rg * LROWS, LROWS), LROWS), pl.ds(al(s * STRIPE, STRIPE), STRIPE)],
            mbuf.at[slot], lsem.at[slot])

    def load(n):
        first = 1 - lax.min(lax.div(n, 2 * n_group), 1)
        i = lax.div(n, 2 * n_group)
        w = lax.rem(n, 2 * n_group)
        rg = first * lax.rem(w, n_group) + (1 - first) * lax.div(w, 2)
        par = first * (1 - lax.div(w, n_group)) + (1 - first) * lax.rem(w, 2)
        return load_at(i, rg, par, n)

    inputs = [pltpu.make_async_copy(src, dst, ins.at[i])
              for i, (src, dst) in enumerate(((ie_hbm, ie_ref), (ue_hbm, ue_ref), (q_hbm, q_ref)))]
    for cp in inputs:
        cp.start()
    for n in range(NLOAD):
        load(jnp.int32(n)).start()
    cs[...] = jnp.zeros_like(cs)
    upart[pl.ds(0, ROWS), :] = jnp.zeros((ROWS, EMB), F32)
    ucol = al(c * ROWS + z * UROWS, UROWS)

    def count(i, rg, par, n, sslot):
        slot = lax.rem(n, NLOAD)
        load_at(i, rg, par, n).wait()
        cols = pl.ds(al(i * STRIPE, STRIPE), STRIPE)
        acc = jnp.zeros((8, STRIPE), F32)
        for g in range(LROWS // 16):
            v = mbuf[slot, g * 16:(g + 1) * 16, :].astype(F32)
            b = v.astype(BF)
            if par == 0:
                stage[sslot, g * 16:(g + 1) * 16, :] = b
            else:
                a[pl.ds(al(c * ROWS + rg * LROWS + g * 16, 16), 16), cols] = b
            acc = acc + v[0:8] + v[8:16]
            parts = [v[:, q * 128:(q + 1) * 128] for q in range(STRIPE // 128)]
            while len(parts) > 1:
                parts = [parts[q] + parts[q + 1] for q in range(0, len(parts), 2)]
            rsl = pl.ds(al(rg * LROWS + g * 16, 16), 16)
            upart[rsl, :] = upart[rsl, :] + parts[0]
        cs[par] = cs[par] + acc

        @pl.when(n + NLOAD < n_load)
        def _():
            load(n + NLOAD).start()

    def xcopy(m):
        i = lax.div(m, n_group)
        rg = lax.rem(m, n_group)
        slot = lax.rem(m, NSTAGE)
        return rcopy(stage.at[slot],
                     a.at[pl.ds(al(c * ROWS + rg * LROWS, LROWS), LROWS), pl.ds(al(i * STRIPE, STRIPE), STRIPE)],
                     xs.at[slot], xr.at[i], sib)

    def dgsend(p, i):
        return rcopy(dcs.at[(1, 1, 1, 0, 0, 0, 0)[i], p], dcr.at[i, p], dgs, dgr.at[p // (CHIPS - 1) if isinstance(p, int) else lax.div(p, CHIPS - 1)],
                     (xn, yn, dg, sib, xnc, ync, dgc)[i])

    def dusend(i):
        return rcopy(dus, dur.at[i], dvs, dvr.at[min(i, 1)], (zn, sib, zsib)[i])

    def stripe_degrees(p, par):
        v = jnp.sum(cs[par], axis=0, keepdims=True)
        for g in range(8):
            dcs[par, p, g:g + 1, :] = v[:, g * 256:(g + 1) * 256]
        cs[par] = jnp.zeros((8, STRIPE), F32)
        for k in ((6, 5, 4, 3), (2, 1, 0))[par]:
            dgsend(p, k).start()

    def own_first(rg, _):
        count(0, rg, 1, rg, 0)
        return 0

    for cp in inputs:
        cp.wait()
    usum[...] = ue_ref[...].astype(F32)
    eut[0, :, pl.ds(ucol, UROWS)] = ue_ref[...].astype(F32).T.astype(BF)
    own_rows = pl.ds(al(me * STRIPE, STRIPE), STRIPE)
    panel[0, own_rows, :] = ie_ref[...]
    pl.semaphore_wait(barrier, len(peers))

    def half_rows(q, h):
        return pl.ds(al(q * STRIPE + h * HALF, HALF), HALF)

    def ei0(i):
        q, h, to = ((me, 0, xn), (me, 1, yn), (me, 1, xn), (me, 0, yn), (y * 2 + ox, 0, yn), (oy * 2 + x, 1, xn))[i]
        blk = panel.at[0, half_rows(q, h)]
        src = ie_ref.at[pl.ds(h * HALF, HALF)] if i < 4 else blk
        return rcopy(src, blk, eis, eir.at[min(i, 2)], to)

    def ua(j, i):
        blk = eut.at[j, :, pl.ds(ucol, UROWS)]
        return rcopy(blk, blk, uas, uar.at[j], (zn, sib, zsib)[i])

    for i in range(4):
        ei0(i).start()
    for i in range(3):
        ua(0, i).start()

    lax.fori_loop(0, n_group, own_first, 0)

    def sib_first(rg, _):
        count(0, rg, 0, n_group + rg, rg)
        xcopy(rg).start()
        return 0

    lax.fori_loop(0, n_group, sib_first, 0)
    for par in range(2):
        stripe_degrees(0, par)

    def mask_step(m, _):
        i = lax.div(m, n_group)
        rg = lax.rem(m, n_group)
        w = m - n_group

        @pl.when(m >= NSTAGE)
        def _():
            xcopy(m - NSTAGE).wait_send()
        count(i, rg, 0, 2 * m, lax.rem(m, NSTAGE))

        @pl.when(lax.rem(w, 3) != 0)
        def _():
            xcopy(n_group + lax.div(2 * w, 3)).start()

        @pl.when(m == 2 * n_group)
        def _():
            ei0(0).wait_recv()
            ei0(4).start()
            ei0(1).wait_recv()
            ei0(5).start()
        @pl.when(rg == n_group - 1)
        def _():
            stripe_degrees(i, 0)
        count(i, rg, 1, 2 * m + 1, 0)

        @pl.when(i == CHIPS - 1)
        def _():
            rsl = pl.ds(al(rg * LROWS, LROWS), LROWS)
            dus[pl.ds(rg, 1), :] = jnp.sum(upart[rsl, :].T, axis=0, keepdims=True)

        @pl.when(m == CHIPS * n_group - 1)
        def _():
            for k in range(3):
                dusend(k).start()

        @pl.when(rg == n_group - 1)
        def _():
            stripe_degrees(i, 1)
        return 0

    lax.fori_loop(n_group, CHIPS * n_group, mask_step, 0)

    for k in range(N_HELD):
        xcopy(jnp.int32(CHIPS * n_group - N_HELD + k)).start()

    def all_of(ref, ss, rs):
        return rcopy(ref, ref, ss, rs, sib)

    def swapped(i):
        region = a.at[pl.ds(al(oc * ROWS, ROWS), ROWS), pl.ds(al(i * STRIPE, STRIPE), STRIPE)]
        rcopy(region, region, xs.at[0], xr.at[i], sib).wait_recv()

    def item_inverse(lo, hi, sem):
        all_of(dcr.at[:, pl.ds(lo, hi - lo)], dgs, dgr.at[sem]).wait_recv()
        for p in range(lo, hi):
            v = dcs[1, p]
            for k in range(7):
                v = v + dcr[k, p]
            v = lax.rsqrt(jnp.maximum(v, 1.0))
            for g in range(8):
                invi[0:1, p * STRIPE + g * 256:p * STRIPE + (g + 1) * 256] = v[g:g + 1, :]

    item_inverse(0, CHIPS - 1, 0)
    def user_inverse(blk, v):
        v = lax.rsqrt(jnp.maximum(v, 1.0))
        for b in range(ROWS // 128):
            w = jnp.broadcast_to(v[b:b + 1, :], (128, 128))
            upart[pl.ds(al(blk * ROWS + b * 128, 128), 128), :] = w.T

    dusend(0).wait_recv()
    user_inverse(c, dus[...] + dur[0])
    all_of(dur.at[pl.ds(1, 2)], dvs, dvr.at[1]).wait_recv()
    user_inverse(oc, dur[1] + dur[2])
    for i in range(3):
        swapped(i)

    def tile_q(t):
        h = lax.rem(t, 2)
        u = lax.div(t, 2)
        f1, f2 = 1 - lax.div(u, 2), lax.rem(lax.div(u + 1, 2), 2)
        fx = (1 - h) * f1 + h * f2
        fy = (1 - h) * f2 + h * f1
        return (y + fy - 2 * y * fy) * 2 + (x + fx - 2 * x * fx)

    def in_order(o):
        h = lax.rem(o, 2)
        u = lax.div(o, 2)
        swap = (1 - h) * y * ox + h * oy * x
        return h + 2 * (u + swap - 2 * u * swap)

    def s1(st, t, k, cols=pl.ds(0, CH)):
        h = lax.rem(t, 2)
        to = dev(x + (1 - h) * (1 - 2 * x), y + h * (1 - 2 * y), c, z)
        return rcopy(part.at[t, k, :, cols], r1.at[t, k, :, cols], s1s, s1r.at[k], to)

    def s2(st, h, k):
        return rcopy(part.at[4 + h, k], r2.at[h, k], s2s, xr.at[k], (yn, xn)[h])

    def chunk_rows(q, h, k):
        return pl.ds(al(q * STRIPE + h * HALF + k * CH, CH), CH)

    def ag(st, d, h, k):
        blk = panel.at[1 - st, chunk_rows(me, h, k)]
        rs = agr.at[k] if d == h else agr.at[NCH]
        return rcopy(blk, blk, ags.at[st], rs, (xn, yn)[d])

    def fw(st, h, k):
        q = (y * 2 + ox, oy * 2 + x)[h]
        blk = panel.at[1 - st, chunk_rows(q, h, k)]
        return rcopy(blk, blk, fws.at[st], fwr, (yn, xn)[h])

    def usib(j):
        return rcopy(upart.at[pl.ds(al(oc * ROWS, ROWS), ROWS)], ursib, usibs, usibr, sib)

    def uz(j):
        return rcopy(upart.at[pl.ds(al(c * ROWS + oz * UROWS, UROWS), UROWS)], urz,
                     uzs, uzr, zn)

    qh, qq = QUERIES // 2, QUERIES // 4
    quarter = pl.ds(al(c * qh + z * qq, qq), qq)

    def pq_sib():
        return rcopy(pkc.at[pl.ds(al(oc * qh, qh), qh)], pks, pqs, xs.at[0], sib)

    def pq_z():
        return rcopy(pkc.at[pl.ds(al(c * qh + oz * qq, qq), qq)], pkz, pqs, xs.at[1], zn)

    def pq_x(i):
        h, to = ((0, xn), (1, yn), (0, yn), (1, xn))[i]
        src = (pkc if i < 2 else pka).at[pl.ds(al(c * qh + z * qq + h * (qq // 2), qq // 2), qq // 2)]
        return rcopy(src, pkx.at[i], pqs, xs.at[2 + i // 2], to)

    def pq_a(i):
        return rcopy(pkf.at[quarter], pkf.at[quarter], pqs, xs.at[4], (zn, sib, zsib)[i])

    def badd(u, v):
        return (u.astype(F32) + v.astype(F32)).astype(BF)

    def normalise(base, width):
        def norm(g, _):
            rsl = pl.ds(al(g * 128, 128), 128)
            iu = upart[rsl, :]
            for b in range(width // 128):
                cc = pl.ds(al(base + b * 128, 128), 128)
                a[rsl, cc] = a[rsl, cc] * (iu * invi[0:1, cc]).astype(BF)
            return 0
        lax.fori_loop(0, 2 * ROWS // 128, norm, 0)

    for j in range(LAYERS):
        st = j % 2
        last = j == LAYERS - 1
        all_of(eut.at[j, :, pl.ds(0, 3 * UROWS)], uas, uar.at[j]).wait_recv()

        def item_tile(t, _):
            base = al(tile_q(t) * STRIPE + lax.rem(t, 2) * HALF, HALF)
            if j == 0:
                normalise(base, HALF)
            res = dot(eut[j], a[:, pl.ds(base, HALF)], 1, 0)
            for k in range(NCH):
                part[t, k] = res[:, k * CH:(k + 1) * CH]
            return 0

        def send_tile(o, _):
            t = in_order(o)
            item_tile(t, 0)
            for k in range(NCH):
                s1(st, t, k).start()
            return 0

        def first_chunk(n, _):
            h = lax.rem(n, 2)
            t = in_order(h)
            k = lax.div(n, 2)
            base = al(tile_q(t) * STRIPE + h * HALF + k * CH, CH)
            normalise(base, CH)
            part[t, k] = dot(eut[j], a[:, pl.ds(base, CH)], 1, 0)
            s1(st, t, k).start()
            return 0

        def first_half(n, _):
            h = lax.rem(n, 2)
            t = in_order(h)
            cols = pl.ds(al(lax.div(n, 2) * 128, 128), 128)
            base = al(tile_q(t) * STRIPE + h * HALF + lax.div(n, 2) * 128, 128)
            normalise(base, 128)
            part[t, 0, :, cols] = dot(eut[j], a[:, pl.ds(base, 128)], 1, 0)
            s1(st, t, 0, cols).start()
            return 0

        def stage1(k, _):
            all_of(r1.at[:, k], s1s, s1r.at[k]).wait_recv()
            for h in range(2):
                part[4 + h, k] = part[4 + h, k] + r1[2 + h, k]
                part[6 + h, k] = part[6 + h, k] + r1[h, k]
                s2(st, h, k).start()
            return 0

        def stage2(k, _):
            all_of(r2.at[:, k], s2s, xr.at[k]).wait_recv()
            for h in range(2):
                e = (part[6 + h, k] + r2[h, k]).T.astype(BF)
                rsl = chunk_rows(me, h, k)
                if last:
                    loc = pl.ds(al(h * HALF + k * CH, CH), CH)
                    tot = ie_ref[loc, :].astype(F32) + panel[1, rsl, :].astype(F32)
                    tot = tot + panel[0, rsl, :].astype(F32) + e.astype(F32)
                    fi_ref[loc, :] = (tot * (1.0 / (LAYERS + 1))).astype(BF)
                else:
                    panel[1 - st, rsl, :] = e
                    ag(st, 0, h, k).start()
                    ag(st, 1, h, k).start()
            return 0

        def forward(k, _):
            all_of(panel.at[1 - st, pl.ds(0, 2 * CH)], ags.at[st], agr.at[k]).wait_recv()
            fw(st, 0, k).start()
            fw(st, 1, k).start()
            return 0

        def user_near(i, _):
            rsl = pl.ds(al(i * UROWS, UROWS), UROWS)
            tot = None
            for q in (me, y * 2 + ox, oy * 2 + x):
                ks = pl.ds(al(q * STRIPE, STRIPE), STRIPE)
                d = dot(a[rsl, ks], panel[st, ks, :], 1, 0)
                tot = d if tot is None else tot + d
            upart[rsl, :] = tot
            if j == 0:
                @pl.when(i == 2)
                def _():
                    stage1(2, 0)
            return 0

        def user_far(i, _):
            b = lax.div(i, 2)
            rsl = pl.ds(al((b * c + (1 - b) * oc) * ROWS + lax.rem(i, 2) * UROWS, UROWS), UROWS)
            ks = pl.ds(al((oy * 2 + ox) * STRIPE, STRIPE), STRIPE)
            upart[rsl, :] = upart[rsl, :] + dot(a[rsl, ks], panel[st, ks, :], 1, 0)

            @pl.when(i == 1)
            def _():
                usib(j).start()
            return 0

        def users():
            if j == 0:
                all_of(panel.at[0, pl.ds(0, 4 * HALF)], eis, eir.at[2]).wait_recv()
            else:
                all_of(panel.at[st, pl.ds(0, STRIPE)], ags.at[1 - st], agr.at[NCH]).wait_recv()
            lax.fori_loop(0, 4, user_near, 0)
            if j == 0:
                stage1(3, 0)
                stage2(0, 0)
            if j > 0:
                all_of(panel.at[st, pl.ds(0, STRIPE)], fws.at[1 - st], fwr).wait_recv()
            lax.fori_loop(0, 4, user_far, 0)

        def users_out():
            usib(j).wait_recv()
            mine = pl.ds(al(c * ROWS, ROWS), ROWS)
            upart[mine, :] = upart[mine, :] + ursib[...]
            uz(j).start()

        def user_final():
            uz(j).wait_recv()
            e = (upart[pl.ds(ucol, UROWS), :] + urz[...]).astype(BF).astype(F32)
            usum[...] = usum[...] + e
            if not last:
                eut[j + 1, :, pl.ds(ucol, UROWS)] = e.T.astype(BF)
                for i in range(3):
                    ua(j + 1, i).start()
                return
            fu = (usum[...] * (1.0 / (LAYERS + 1))).astype(BF)
            fu_ref[...] = fu
            ids = lax.broadcasted_iota(jnp.int32, (UROWS, QUERIES), 0) + (row * 2 + z) * UROWS
            hot = jnp.where(ids == q_ref[...], 1.0, 0.0).astype(BF)
            pkc[...] = dot(hot, fu, 0, 0).astype(BF)
            pq_sib().start()

        if j == 0:
            lax.fori_loop(0, 4, first_half, 0)
            lax.fori_loop(2, 2 * NCH, first_chunk, 0)
            item_inverse(CHIPS - 1, CHIPS, 1)
            swapped(CHIPS - 1)
            lax.fori_loop(2, 4, send_tile, 0)
            lax.fori_loop(4, 8, item_tile, 0)
            lax.fori_loop(0, 2, stage1, 0)
            users()
            users_out()
            lax.fori_loop(1, NCH, stage2, 0)
            user_final()
        else:
            lax.fori_loop(0, 2, send_tile, 0)
            users()
            users_out()
            lax.fori_loop(2, 4, send_tile, 0)
            lax.fori_loop(4, 8, item_tile, 0)
            if not last:
                lax.fori_loop(0, 2, stage1, 0)
            user_final()
            if last:
                pq_sib().wait_recv()
                hrows = pl.ds(al(c * qh, qh), qh)
                pkc[hrows, :] = badd(pkc[hrows, :], pks[...])
                pq_z().start()
                stage1(0, 0)
                pq_z().wait_recv()
                pkc[quarter, :] = badd(pkc[quarter, :], pkz[...])
                for i in range(2):
                    pq_x(i).start()
                stage1(1, 0)
                all_of(pkx.at[pl.ds(0, 2)], pqs, xs.at[2]).wait_recv()
                for i in range(2):
                    rsl = pl.ds(al(c * qh + z * qq + i * (qq // 2), qq // 2), qq // 2)
                    pka[rsl, :] = badd(pkc[rsl, :], pkx[i])
                for i in range(2, 4):
                    pq_x(i).start()
            lax.fori_loop(2, NCH, stage1, 0)
            lax.fori_loop(0, 2, stage2, 0)
            if last:
                all_of(pkx.at[pl.ds(2, 2)], pqs, xs.at[3]).wait_recv()
                for i in range(2, 4):
                    rsl = pl.ds(al(c * qh + z * qq + (i - 2) * (qq // 2), qq // 2), qq // 2)
                    pkf[rsl, :] = badd(pka[rsl, :], pkx[i])
                for i in range(3):
                    pq_a(i).start()
            lax.fori_loop(2, NCH, stage2, 0)
        if not last:
            lax.fori_loop(0, NCH, forward, 0)

        usib(j).wait_send()
        uz(j).wait_send()
        all_of(eut.at[j, :, pl.ds(0, 3 * UROWS)], uas, uar.at[j]).wait_send()
        all_of(part.at[pl.ds(0, 4)], s1s, s1r.at[0]).wait_send()
        all_of(part.at[pl.ds(4, 2)], s2s, xr.at[0]).wait_send()
        if j == 0:
            all_of(dcr, dgs, dgr.at[0]).wait_send()
            all_of(dur, dvs, dvr.at[0]).wait_send()
            def drain_swap(m, _):
                xcopy(m).wait_send()
                return 0
            lax.fori_loop(CHIPS * n_group - NSTAGE, CHIPS * n_group, drain_swap, 0)
            all_of(panel.at[0, pl.ds(0, 6 * HALF)], eis, eir.at[2]).wait_send()
        else:
            all_of(panel.at[st, pl.ds(0, 2 * STRIPE)], ags.at[1 - st], agr.at[NCH]).wait_send()
            all_of(panel.at[st, pl.ds(0, STRIPE)], fws.at[1 - st], fwr).wait_send()

    all_of(pkf.at[pl.ds(0, 3 * qq)], pqs, xs.at[4]).wait_recv()
    pk_ref[...] = pkf[...]
    all_of(ie_ref, pqs, xs.at[4]).wait_send()


def score_kernel(fu_ref, fi_ref, pk_ref, fu_out, fi_out, s_out, buf, sem, out_sem):
    small = [pltpu.make_async_copy(fu_ref, fu_out, out_sem.at[0]),
             pltpu.make_async_copy(fi_ref, fi_out, out_sem.at[1])]
    for i in range(QUERIES // SROWS):
        rsl = pl.ds(i * SROWS, SROWS)
        buf[rsl, :] = dot(pk_ref[rsl, :], fi_ref[...], 1, 1)
        pltpu.make_async_copy(buf.at[rsl], s_out.at[rsl, :], sem).start()
        if i == 0:
            for cp in small:
                cp.start()
    for cp in small:
        cp.wait()
    pltpu.make_async_copy(buf, s_out, sem).wait()


def scores_of(fu, fi, picked):
    vm = pl.BlockSpec(memory_space=pltpu.VMEM)
    hbm = pl.BlockSpec(memory_space=pl.ANY)
    return pl.pallas_call(
        score_kernel,
        out_shape=(jax.ShapeDtypeStruct(fu.shape, BF), jax.ShapeDtypeStruct(fi.shape, BF),
                   jax.ShapeDtypeStruct((QUERIES, STRIPE), F32)),
        in_specs=[vm, vm, vm],
        out_specs=(hbm, hbm, hbm),
        scratch_shapes=[pltpu.VMEM((QUERIES, STRIPE), F32),
                        pltpu.SemaphoreType.DMA, pltpu.SemaphoreType.DMA((2,))],
        compiler_params=pltpu.CompilerParams(vmem_limit_bytes=16 * 1024 * 1024),
        name='scores',
    )(fu, fi, picked)


def propagate(mask_blk, user_shard, item_shard, queries):
    hbm = pl.BlockSpec(memory_space=pl.ANY)
    vm = pl.BlockSpec(memory_space=pltpu.VMEM)
    dma = pltpu.SemaphoreType.DMA
    qh, qq = QUERIES // 2, QUERIES // 4
    scratch = [
        pltpu.VMEM((UROWS, EMB), BF),
        pltpu.VMEM((STRIPE, EMB), BF),
        pltpu.VMEM((1, QUERIES), jnp.int32),
        pltpu.VMEM((QUERIES, EMB), BF),
        pltpu.VMEM((2 * ROWS, COLS), BF),
        pltpu.VMEM((8, NCH, EMB, CH), F32),
        pltpu.VMEM((4, NCH, EMB, CH), F32),
        pltpu.VMEM((2, NCH, EMB, CH), F32),
        pltpu.VMEM((2, COLS, EMB), BF),
        pltpu.VMEM((LAYERS, EMB, 2 * ROWS), BF),
        pltpu.VMEM((2 * ROWS, EMB), F32),
        pltpu.VMEM((ROWS, EMB), F32),
        pltpu.VMEM((UROWS, EMB), F32),
        pltpu.VMEM((1, COLS), F32),
        pltpu.VMEM((NLOAD, LROWS, STRIPE), jnp.int32),
        pltpu.VMEM((NSTAGE, LROWS, STRIPE), BF),
        pltpu.VMEM((2, 8, STRIPE), F32),
        pltpu.VMEM((2, CHIPS, 8, STRIPE // 8), F32),
        pltpu.VMEM((7, CHIPS, 8, STRIPE // 8), F32),
        pltpu.VMEM((8, ROWS // 8), F32),
        pltpu.VMEM((3, 8, ROWS // 8), F32),
        pltpu.VMEM((UROWS, EMB), F32),
        pltpu.VMEM((QUERIES, EMB), BF),
        pltpu.VMEM((qh, EMB), BF),
        pltpu.VMEM((qq, EMB), BF),
        pltpu.VMEM((4, qq // 2, EMB), BF),
        pltpu.VMEM((QUERIES, EMB), BF),
        dma((NLOAD,)), dma((NSTAGE,)), dma((CHIPS,)),
        dma, dma((NCH,)), dma,
        dma((2,)), dma((NCH + 1,)),
        dma((2,)), dma,
        dma, dma, dma, dma,
        dma, dma((LAYERS,)),
        dma, dma((3,)), dma, dma((2,)), dma, dma((2,)),
        dma,
        dma((3,)),
    ]
    return pl.pallas_call(
        kernel,
        out_shape=(pltpu.VMEM((UROWS, EMB), BF), pltpu.VMEM((STRIPE, EMB), BF), pltpu.VMEM((QUERIES, EMB), BF)),
        in_specs=[hbm] * 4,
        out_specs=(vm, vm, vm),
        scratch_shapes=scratch,
        compiler_params=pltpu.CompilerParams(collective_id=0, has_side_effects=True,
                                             vmem_limit_bytes=64487424),
        name='propagate',
    )(mask_blk, user_shard, item_shard, queries)


def solution(mesh):
    def device_step(mask_blk, user_shard, item_shard, queries):
        fu, fi, picked = propagate(mask_blk, user_shard, item_shard, queries.reshape(1, QUERIES))
        return scores_of(fu, fi, picked)

    return jax.shard_map(
        device_step, mesh=mesh,
        in_specs=(P('row', 'col'), P(('row', 'col'), None), P(('col', 'row'), None), P()),
        out_specs=(P(('row', 'col'), None), P(('col', 'row'), None), P(None, ('col', 'row'))),
        check_vma=False)
```

```python
import functools

import jax
import jax.numpy as jnp
from jax import lax
from jax.experimental import pallas as pl
from jax.experimental.pallas import tpu as pltpu
from jax.sharding import PartitionSpec as P

LAYERS = 3
BF = jnp.bfloat16
F32 = jnp.float32
EMB = 128
ROWS = 1024
STRIPE = 2048
CHIPS = 4
COLS = STRIPE * CHIPS
UROWS = 512
HALF = STRIPE // 2
NCH = 4
CH = HALF // NCH
LROWS = 128
NLOAD = 7
NSTAGE = 11
N_HELD = 8
QUERIES = 1024
SROWS = 128


def al(v, m):
    return pl.multiple_of(v, m)


def dot(a, b, ca, cb):
    return lax.dot_general(a, b, (((ca,), (cb,)), ((), ())), preferred_element_type=F32)


def kernel(mask_ref, ue_hbm, ie_hbm, q_hbm, fu_ref, fi_ref, pk_ref, ue_ref, ie_ref, q_ref, pkf,
           a, part, r1, r2, panel, eut, upart, ursib, urz, invi, mbuf, stage,
           cs, dcs, dcr, dus, dur, usum, pkc, pks, pkz, pkx, pka,
           lsem, xs, xr, s1s, s1r, s2s, ags, agr, fws, fwr,
           usibs, usibr, uzs, uzr, uas, uar, eis, eir, dgs, dgr, dvs, dvr, pqs, ins):
    row = lax.axis_index('row')
    z = lax.axis_index('col')
    c = lax.rem(row, 2)
    x = lax.rem(lax.div(row, 2), 2)
    y = lax.div(row, 4)
    me = y * 2 + x

    def dev(xx, yy, cc, zz):
        return {'row': (yy * 2 + xx) * 2 + cc, 'col': zz}

    ox, oy, oc, oz = 1 - x, 1 - y, 1 - c, 1 - z
    xn, yn, dg = dev(ox, y, c, z), dev(x, oy, c, z), dev(ox, oy, c, z)
    zn, sib, zsib = dev(x, y, c, oz), dev(x, y, oc, z), dev(x, y, oc, oz)
    xnc, ync, dgc = dev(ox, y, oc, z), dev(x, oy, oc, z), dev(ox, oy, oc, z)

    def rcopy(src, dst, ss, rs, to):
        return pltpu.make_async_remote_copy(src_ref=src, dst_ref=dst, send_sem=ss, recv_sem=rs,
                                            device_id=to, device_id_type=pl.DeviceIdType.MESH)

    barrier = pltpu.get_barrier_semaphore()
    peers = (xn, yn, dg, zn, sib, zsib, xnc, ync, dgc)
    for peer in peers:
        pl.semaphore_signal(barrier, inc=1, device_id=peer, device_id_type=pl.DeviceIdType.MESH)

    n_group = ROWS // LROWS
    n_load = n_group * 2 * CHIPS

    def load_at(i, rg, par, n):
        s = 2 * i + par * c + (1 - par) * oc
        slot = lax.rem(n, NLOAD)
        return pltpu.make_async_copy(
            mask_ref.at[pl.ds(al(rg * LROWS, LROWS), LROWS), pl.ds(al(s * STRIPE, STRIPE), STRIPE)],
            mbuf.at[slot], lsem.at[slot])

    def load(n):
        first = 1 - lax.min(lax.div(n, 2 * n_group), 1)
        i = lax.div(n, 2 * n_group)
        w = lax.rem(n, 2 * n_group)
        rg = first * lax.rem(w, n_group) + (1 - first) * lax.div(w, 2)
        par = first * (1 - lax.div(w, n_group)) + (1 - first) * lax.rem(w, 2)
        return load_at(i, rg, par, n)

    inputs = [pltpu.make_async_copy(src, dst, ins.at[i])
              for i, (src, dst) in enumerate(((ie_hbm, ie_ref), (ue_hbm, ue_ref), (q_hbm, q_ref)))]
    for cp in inputs:
        cp.start()
    for n in range(NLOAD):
        load(jnp.int32(n)).start()
    cs[...] = jnp.zeros_like(cs)
    upart[pl.ds(0, ROWS), :] = jnp.zeros((ROWS, EMB), F32)
    ucol = al(c * ROWS + z * UROWS, UROWS)

    def count(i, rg, par, n, sslot):
        slot = lax.rem(n, NLOAD)
        load_at(i, rg, par, n).wait()
        cols = pl.ds(al(i * STRIPE, STRIPE), STRIPE)
        acc = jnp.zeros((8, STRIPE), F32)
        for g in range(LROWS // 16):
            v = mbuf[slot, g * 16:(g + 1) * 16, :].astype(F32)
            b = v.astype(BF)
            if par == 0:
                stage[sslot, g * 16:(g + 1) * 16, :] = b
            else:
                a[pl.ds(al(c * ROWS + rg * LROWS + g * 16, 16), 16), cols] = b
            acc = acc + v[0:8] + v[8:16]
            parts = [v[:, q * 128:(q + 1) * 128] for q in range(STRIPE // 128)]
            while len(parts) > 1:
                parts = [parts[q] + parts[q + 1] for q in range(0, len(parts), 2)]
            rsl = pl.ds(al(rg * LROWS + g * 16, 16), 16)
            upart[rsl, :] = upart[rsl, :] + parts[0]
        cs[par] = cs[par] + acc

        @pl.when(n + NLOAD < n_load)
        def _():
            load(n + NLOAD).start()

    def xcopy(m):
        i = lax.div(m, n_group)
        rg = lax.rem(m, n_group)
        slot = lax.rem(m, NSTAGE)
        return rcopy(stage.at[slot],
                     a.at[pl.ds(al(c * ROWS + rg * LROWS, LROWS), LROWS), pl.ds(al(i * STRIPE, STRIPE), STRIPE)],
                     xs.at[slot], xr.at[i], sib)

    def dgsend(p, i):
        return rcopy(dcs.at[(1, 1, 1, 0, 0, 0, 0)[i], p], dcr.at[i, p], dgs, dgr.at[p // (CHIPS - 1) if isinstance(p, int) else lax.div(p, CHIPS - 1)],
                     (xn, yn, dg, sib, xnc, ync, dgc)[i])

    def dusend(i):
        return rcopy(dus, dur.at[i], dvs, dvr.at[min(i, 1)], (zn, sib, zsib)[i])

    def stripe_degrees(p, par):
        v = jnp.sum(cs[par], axis=0, keepdims=True)
        for g in range(8):
            dcs[par, p, g:g + 1, :] = v[:, g * 256:(g + 1) * 256]
        cs[par] = jnp.zeros((8, STRIPE), F32)
        for k in ((6, 5, 4, 3), (2, 1, 0))[par]:
            dgsend(p, k).start()

    def own_first(rg, _):
        count(0, rg, 1, rg, 0)
        return 0

    for cp in inputs:
        cp.wait()
    usum[...] = ue_ref[...].astype(F32)
    eut[0, :, pl.ds(ucol, UROWS)] = ue_ref[...].astype(F32).T.astype(BF)
    own_rows = pl.ds(al(me * STRIPE, STRIPE), STRIPE)
    panel[0, own_rows, :] = ie_ref[...]
    pl.semaphore_wait(barrier, len(peers))

    def half_rows(q, h):
        return pl.ds(al(q * STRIPE + h * HALF, HALF), HALF)

    def ei0(i):
        q, h, to = ((me, 0, xn), (me, 1, yn), (me, 1, xn), (me, 0, yn), (y * 2 + ox, 0, yn), (oy * 2 + x, 1, xn))[i]
        blk = panel.at[0, half_rows(q, h)]
        src = ie_ref.at[pl.ds(h * HALF, HALF)] if i < 4 else blk
        return rcopy(src, blk, eis, eir.at[min(i, 2)], to)

    def ua(j, i):
        blk = eut.at[j, :, pl.ds(ucol, UROWS)]
        return rcopy(blk, blk, uas, uar.at[j], (zn, sib, zsib)[i])

    for i in range(4):
        ei0(i).start()
    for i in range(3):
        ua(0, i).start()

    lax.fori_loop(0, n_group, own_first, 0)

    def sib_first(rg, _):
        count(0, rg, 0, n_group + rg, rg)
        xcopy(rg).start()
        return 0

    lax.fori_loop(0, n_group, sib_first, 0)
    for par in range(2):
        stripe_degrees(0, par)

    def mask_step(m, _):
        i = lax.div(m, n_group)
        rg = lax.rem(m, n_group)
        w = m - n_group

        @pl.when(m >= NSTAGE)
        def _():
            xcopy(m - NSTAGE).wait_send()
        count(i, rg, 0, 2 * m, lax.rem(m, NSTAGE))

        @pl.when(lax.rem(w, 3) != 0)
        def _():
            xcopy(n_group + lax.div(2 * w, 3)).start()

        @pl.when(m == 2 * n_group)
        def _():
            ei0(0).wait_recv()
            ei0(4).start()
            ei0(1).wait_recv()
            ei0(5).start()
        @pl.when(rg == n_group - 1)
        def _():
            stripe_degrees(i, 0)
        count(i, rg, 1, 2 * m + 1, 0)

        @pl.when(i == CHIPS - 1)
        def _():
            rsl = pl.ds(al(rg * LROWS, LROWS), LROWS)
            dus[pl.ds(rg, 1), :] = jnp.sum(upart[rsl, :].T, axis=0, keepdims=True)

        @pl.when(m == CHIPS * n_group - 1)
        def _():
            for k in range(3):
                dusend(k).start()

        @pl.when(rg == n_group - 1)
        def _():
            stripe_degrees(i, 1)
        return 0

    lax.fori_loop(n_group, CHIPS * n_group, mask_step, 0)

    for k in range(N_HELD):
        xcopy(jnp.int32(CHIPS * n_group - N_HELD + k)).start()

    def all_of(ref, ss, rs):
        return rcopy(ref, ref, ss, rs, sib)

    def swapped(i):
        region = a.at[pl.ds(al(oc * ROWS, ROWS), ROWS), pl.ds(al(i * STRIPE, STRIPE), STRIPE)]
        rcopy(region, region, xs.at[0], xr.at[i], sib).wait_recv()

    def item_inverse(lo, hi, sem):
        all_of(dcr.at[:, pl.ds(lo, hi - lo)], dgs, dgr.at[sem]).wait_recv()
        for p in range(lo, hi):
            v = dcs[1, p]
            for k in range(7):
                v = v + dcr[k, p]
            v = lax.rsqrt(jnp.maximum(v, 1.0))
            for g in range(8):
                invi[0:1, p * STRIPE + g * 256:p * STRIPE + (g + 1) * 256] = v[g:g + 1, :]

    item_inverse(0, CHIPS - 1, 0)
    def user_inverse(blk, v):
        v = lax.rsqrt(jnp.maximum(v, 1.0))
        for b in range(ROWS // 128):
            w = jnp.broadcast_to(v[b:b + 1, :], (128, 128))
            upart[pl.ds(al(blk * ROWS + b * 128, 128), 128), :] = w.T

    dusend(0).wait_recv()
    user_inverse(c, dus[...] + dur[0])
    all_of(dur.at[pl.ds(1, 2)], dvs, dvr.at[1]).wait_recv()
    user_inverse(oc, dur[1] + dur[2])
    for i in range(3):
        swapped(i)

    def tile_q(t):
        h = lax.rem(t, 2)
        u = lax.div(t, 2)
        f1, f2 = 1 - lax.div(u, 2), lax.rem(lax.div(u + 1, 2), 2)
        fx = (1 - h) * f1 + h * f2
        fy = (1 - h) * f2 + h * f1
        return (y + fy - 2 * y * fy) * 2 + (x + fx - 2 * x * fx)

    def in_order(o):
        h = lax.rem(o, 2)
        u = lax.div(o, 2)
        swap = (1 - h) * y * ox + h * oy * x
        return h + 2 * (u + swap - 2 * u * swap)

    def s1(st, t, k, cols=pl.ds(0, CH)):
        h = lax.rem(t, 2)
        to = dev(x + (1 - h) * (1 - 2 * x), y + h * (1 - 2 * y), c, z)
        return rcopy(part.at[t, k, :, cols], r1.at[t, k, :, cols], s1s, s1r.at[k], to)

    def s2(st, h, k):
        return rcopy(part.at[4 + h, k], r2.at[h, k], s2s, xr.at[k], (yn, xn)[h])

    def chunk_rows(q, h, k):
        return pl.ds(al(q * STRIPE + h * HALF + k * CH, CH), CH)

    def ag(st, d, h, k):
        blk = panel.at[1 - st, chunk_rows(me, h, k)]
        rs = agr.at[k] if d == h else agr.at[NCH]
        return rcopy(blk, blk, ags.at[st], rs, (xn, yn)[d])

    def fw(st, h, k):
        q = (y * 2 + ox, oy * 2 + x)[h]
        blk = panel.at[1 - st, chunk_rows(q, h, k)]
        return rcopy(blk, blk, fws.at[st], fwr, (yn, xn)[h])

    def usib(j):
        return rcopy(upart.at[pl.ds(al(oc * ROWS, ROWS), ROWS)], ursib, usibs, usibr, sib)

    def uz(j):
        return rcopy(upart.at[pl.ds(al(c * ROWS + oz * UROWS, UROWS), UROWS)], urz,
                     uzs, uzr, zn)

    qh, qq = QUERIES // 2, QUERIES // 4
    quarter = pl.ds(al(c * qh + z * qq, qq), qq)

    def pq_sib():
        return rcopy(pkc.at[pl.ds(al(oc * qh, qh), qh)], pks, pqs, xs.at[0], sib)

    def pq_z():
        return rcopy(pkc.at[pl.ds(al(c * qh + oz * qq, qq), qq)], pkz, pqs, xs.at[1], zn)

    def pq_x(i):
        h, to = ((0, xn), (1, yn), (0, yn), (1, xn))[i]
        src = (pkc if i < 2 else pka).at[pl.ds(al(c * qh + z * qq + h * (qq // 2), qq // 2), qq // 2)]
        return rcopy(src, pkx.at[i], pqs, xs.at[2 + i // 2], to)

    def pq_a(i):
        return rcopy(pkf.at[quarter], pkf.at[quarter], pqs, xs.at[4], (zn, sib, zsib)[i])

    def badd(u, v):
        return (u.astype(F32) + v.astype(F32)).astype(BF)

    def normalise(base, width):
        def norm(g, _):
            rsl = pl.ds(al(g * 128, 128), 128)
            iu = upart[rsl, :]
            for b in range(width // 128):
                cc = pl.ds(al(base + b * 128, 128), 128)
                a[rsl, cc] = a[rsl, cc] * (iu * invi[0:1, cc]).astype(BF)
            return 0
        lax.fori_loop(0, 2 * ROWS // 128, norm, 0)

    for j in range(LAYERS):
        st = j % 2
        last = j == LAYERS - 1
        all_of(eut.at[j, :, pl.ds(0, 3 * UROWS)], uas, uar.at[j]).wait_recv()

        def item_tile(t, _):
            base = al(tile_q(t) * STRIPE + lax.rem(t, 2) * HALF, HALF)
            if j == 0:
                normalise(base, HALF)
            res = dot(eut[j], a[:, pl.ds(base, HALF)], 1, 0)
            for k in range(NCH):
                part[t, k] = res[:, k * CH:(k + 1) * CH]
            return 0

        def send_tile(o, _):
            t = in_order(o)
            item_tile(t, 0)
            for k in range(NCH):
                s1(st, t, k).start()
            return 0

        def first_chunk(n, _):
            h = lax.rem(n, 2)
            t = in_order(h)
            k = lax.div(n, 2)
            base = al(tile_q(t) * STRIPE + h * HALF + k * CH, CH)
            normalise(base, CH)
            part[t, k] = dot(eut[j], a[:, pl.ds(base, CH)], 1, 0)
            s1(st, t, k).start()
            return 0

        def first_half(n, _):
            h = lax.rem(n, 2)
            t = in_order(h)
            cols = pl.ds(al(lax.div(n, 2) * 128, 128), 128)
            base = al(tile_q(t) * STRIPE + h * HALF + lax.div(n, 2) * 128, 128)
            normalise(base, 128)
            part[t, 0, :, cols] = dot(eut[j], a[:, pl.ds(base, 128)], 1, 0)
            s1(st, t, 0, cols).start()
            return 0

        def stage1(k, _):
            all_of(r1.at[:, k], s1s, s1r.at[k]).wait_recv()
            for h in range(2):
                part[4 + h, k] = part[4 + h, k] + r1[2 + h, k]
                part[6 + h, k] = part[6 + h, k] + r1[h, k]
                s2(st, h, k).start()
            return 0

        def stage2(k, _):
            all_of(r2.at[:, k], s2s, xr.at[k]).wait_recv()
            for h in range(2):
                e = (part[6 + h, k] + r2[h, k]).T.astype(BF)
                rsl = chunk_rows(me, h, k)
                if last:
                    loc = pl.ds(al(h * HALF + k * CH, CH), CH)
                    tot = ie_ref[loc, :].astype(F32) + panel[1, rsl, :].astype(F32)
                    tot = tot + panel[0, rsl, :].astype(F32) + e.astype(F32)
                    fi_ref[loc, :] = (tot * (1.0 / (LAYERS + 1))).astype(BF)
                else:
                    panel[1 - st, rsl, :] = e
                    ag(st, 0, h, k).start()
                    ag(st, 1, h, k).start()
            return 0

        def forward(k, _):
            all_of(panel.at[1 - st, pl.ds(0, 2 * CH)], ags.at[st], agr.at[k]).wait_recv()
            fw(st, 0, k).start()
            fw(st, 1, k).start()
            return 0

        def user_near(i, _):
            rsl = pl.ds(al(i * UROWS, UROWS), UROWS)
            tot = None
            for q in (me, y * 2 + ox, oy * 2 + x):
                ks = pl.ds(al(q * STRIPE, STRIPE), STRIPE)
                d = dot(a[rsl, ks], panel[st, ks, :], 1, 0)
                tot = d if tot is None else tot + d
            upart[rsl, :] = tot
            if j == 0:
                @pl.when(i == 2)
                def _():
                    stage1(2, 0)
            return 0

        def user_far(i, _):
            b = lax.div(i, 2)
            rsl = pl.ds(al((b * c + (1 - b) * oc) * ROWS + lax.rem(i, 2) * UROWS, UROWS), UROWS)
            ks = pl.ds(al((oy * 2 + ox) * STRIPE, STRIPE), STRIPE)
            upart[rsl, :] = upart[rsl, :] + dot(a[rsl, ks], panel[st, ks, :], 1, 0)

            @pl.when(i == 1)
            def _():
                usib(j).start()
            return 0

        def users():
            if j == 0:
                all_of(panel.at[0, pl.ds(0, 4 * HALF)], eis, eir.at[2]).wait_recv()
            else:
                all_of(panel.at[st, pl.ds(0, STRIPE)], ags.at[1 - st], agr.at[NCH]).wait_recv()
            lax.fori_loop(0, 4, user_near, 0)
            if j == 0:
                stage1(3, 0)
                stage2(0, 0)
            if j > 0:
                all_of(panel.at[st, pl.ds(0, STRIPE)], fws.at[1 - st], fwr).wait_recv()
            lax.fori_loop(0, 4, user_far, 0)

        def users_out():
            usib(j).wait_recv()
            mine = pl.ds(al(c * ROWS, ROWS), ROWS)
            upart[mine, :] = upart[mine, :] + ursib[...]
            uz(j).start()

        def user_final():
            uz(j).wait_recv()
            e = (upart[pl.ds(ucol, UROWS), :] + urz[...]).astype(BF).astype(F32)
            usum[...] = usum[...] + e
            if not last:
                eut[j + 1, :, pl.ds(ucol, UROWS)] = e.T.astype(BF)
                for i in range(3):
                    ua(j + 1, i).start()
                return
            fu = (usum[...] * (1.0 / (LAYERS + 1))).astype(BF)
            fu_ref[...] = fu
            ids = lax.broadcasted_iota(jnp.int32, (UROWS, QUERIES), 0) + (row * 2 + z) * UROWS
            hot = jnp.where(ids == q_ref[...], 1.0, 0.0).astype(BF)
            pkc[...] = dot(hot, fu, 0, 0).astype(BF)
            pq_sib().start()

        if j == 0:
            lax.fori_loop(0, 4, first_half, 0)
            lax.fori_loop(2, 2 * NCH, first_chunk, 0)
            item_inverse(CHIPS - 1, CHIPS, 1)
            swapped(CHIPS - 1)
            lax.fori_loop(2, 4, send_tile, 0)
            lax.fori_loop(4, 8, item_tile, 0)
            lax.fori_loop(0, 2, stage1, 0)
            users()
            users_out()
            lax.fori_loop(1, NCH, stage2, 0)
            user_final()
        else:
            lax.fori_loop(0, 2, send_tile, 0)
            users()
            users_out()
            lax.fori_loop(2, 4, send_tile, 0)
            lax.fori_loop(4, 8, item_tile, 0)
            if not last:
                lax.fori_loop(0, 2, stage1, 0)
            user_final()
            if last:
                pq_sib().wait_recv()
                hrows = pl.ds(al(c * qh, qh), qh)
                pkc[hrows, :] = badd(pkc[hrows, :], pks[...])
                pq_z().start()
                stage1(0, 0)
                pq_z().wait_recv()
                pkc[quarter, :] = badd(pkc[quarter, :], pkz[...])
                for i in range(2):
                    pq_x(i).start()
                stage1(1, 0)
                all_of(pkx.at[pl.ds(0, 2)], pqs, xs.at[2]).wait_recv()
                for i in range(2):
                    rsl = pl.ds(al(c * qh + z * qq + i * (qq // 2), qq // 2), qq // 2)
                    pka[rsl, :] = badd(pkc[rsl, :], pkx[i])
                for i in range(2, 4):
                    pq_x(i).start()
            lax.fori_loop(2, NCH, stage1, 0)
            lax.fori_loop(0, 2, stage2, 0)
            if last:
                all_of(pkx.at[pl.ds(2, 2)], pqs, xs.at[3]).wait_recv()
                for i in range(2, 4):
                    rsl = pl.ds(al(c * qh + z * qq + (i - 2) * (qq // 2), qq // 2), qq // 2)
                    pkf[rsl, :] = badd(pka[rsl, :], pkx[i])
                for i in range(3):
                    pq_a(i).start()
            lax.fori_loop(2, NCH, stage2, 0)
        if not last:
            lax.fori_loop(0, NCH, forward, 0)

        usib(j).wait_send()
        uz(j).wait_send()
        all_of(eut.at[j, :, pl.ds(0, 3 * UROWS)], uas, uar.at[j]).wait_send()
        all_of(part.at[pl.ds(0, 4)], s1s, s1r.at[0]).wait_send()
        all_of(part.at[pl.ds(4, 2)], s2s, xr.at[0]).wait_send()
        if j == 0:
            all_of(dcr, dgs, dgr.at[0]).wait_send()
            all_of(dur, dvs, dvr.at[0]).wait_send()
            def drain_swap(m, _):
                xcopy(m).wait_send()
                return 0
            lax.fori_loop(CHIPS * n_group - NSTAGE, CHIPS * n_group, drain_swap, 0)
            all_of(panel.at[0, pl.ds(0, 6 * HALF)], eis, eir.at[2]).wait_send()
        else:
            all_of(panel.at[st, pl.ds(0, 2 * STRIPE)], ags.at[1 - st], agr.at[NCH]).wait_send()
            all_of(panel.at[st, pl.ds(0, STRIPE)], fws.at[1 - st], fwr).wait_send()

    all_of(pkf.at[pl.ds(0, 3 * qq)], pqs, xs.at[4]).wait_recv()
    pk_ref[...] = pkf[...]
    all_of(ie_ref, pqs, xs.at[4]).wait_send()


def score_kernel(fu_ref, fi_ref, pk_ref, fu_out, fi_out, s_out, buf, sem, out_sem):
    small = [pltpu.make_async_copy(fu_ref, fu_out, out_sem.at[0]),
             pltpu.make_async_copy(fi_ref, fi_out, out_sem.at[1])]
    for i in range(QUERIES // SROWS):
        rsl = pl.ds(i * SROWS, SROWS)
        buf[rsl, :] = dot(pk_ref[rsl, :], fi_ref[...], 1, 1)
        pltpu.make_async_copy(buf.at[rsl], s_out.at[rsl, :], sem).start()
        if i == 0:
            for cp in small:
                cp.start()
    for cp in small:
        cp.wait()
    pltpu.make_async_copy(buf, s_out, sem).wait()


def scores_of(fu, fi, picked):
    vm = pl.BlockSpec(memory_space=pltpu.VMEM)
    hbm = pl.BlockSpec(memory_space=pl.ANY)
    return pl.pallas_call(
        score_kernel,
        out_shape=(jax.ShapeDtypeStruct(fu.shape, BF), jax.ShapeDtypeStruct(fi.shape, BF),
                   jax.ShapeDtypeStruct((QUERIES, STRIPE), F32)),
        in_specs=[vm, vm, vm],
        out_specs=(hbm, hbm, hbm),
        scratch_shapes=[pltpu.VMEM((QUERIES, STRIPE), F32),
                        pltpu.SemaphoreType.DMA, pltpu.SemaphoreType.DMA((2,))],
        compiler_params=pltpu.CompilerParams(vmem_limit_bytes=16 * 1024 * 1024),
        name='scores',
    )(fu, fi, picked)


def propagate(mask_blk, user_shard, item_shard, queries):
    hbm = pl.BlockSpec(memory_space=pl.ANY)
    vm = pl.BlockSpec(memory_space=pltpu.VMEM)
    dma = pltpu.SemaphoreType.DMA
    qh, qq = QUERIES // 2, QUERIES // 4
    scratch = [
        pltpu.VMEM((UROWS, EMB), BF),
        pltpu.VMEM((STRIPE, EMB), BF),
        pltpu.VMEM((1, QUERIES), jnp.int32),
        pltpu.VMEM((QUERIES, EMB), BF),
        pltpu.VMEM((2 * ROWS, COLS), BF),
        pltpu.VMEM((8, NCH, EMB, CH), F32),
        pltpu.VMEM((4, NCH, EMB, CH), F32),
        pltpu.VMEM((2, NCH, EMB, CH), F32),
        pltpu.VMEM((2, COLS, EMB), BF),
        pltpu.VMEM((LAYERS, EMB, 2 * ROWS), BF),
        pltpu.VMEM((2 * ROWS, EMB), F32),
        pltpu.VMEM((ROWS, EMB), F32),
        pltpu.VMEM((UROWS, EMB), F32),
        pltpu.VMEM((1, COLS), F32),
        pltpu.VMEM((NLOAD, LROWS, STRIPE), jnp.int32),
        pltpu.VMEM((NSTAGE, LROWS, STRIPE), BF),
        pltpu.VMEM((2, 8, STRIPE), F32),
        pltpu.VMEM((2, CHIPS, 8, STRIPE // 8), F32),
        pltpu.VMEM((7, CHIPS, 8, STRIPE // 8), F32),
        pltpu.VMEM((8, ROWS // 8), F32),
        pltpu.VMEM((3, 8, ROWS // 8), F32),
        pltpu.VMEM((UROWS, EMB), F32),
        pltpu.VMEM((QUERIES, EMB), BF),
        pltpu.VMEM((qh, EMB), BF),
        pltpu.VMEM((qq, EMB), BF),
        pltpu.VMEM((4, qq // 2, EMB), BF),
        pltpu.VMEM((QUERIES, EMB), BF),
        dma((NLOAD,)), dma((NSTAGE,)), dma((CHIPS,)),
        dma, dma((NCH,)), dma,
        dma((2,)), dma((NCH + 1,)),
        dma((2,)), dma,
        dma, dma, dma, dma,
        dma, dma((LAYERS,)),
        dma, dma((3,)), dma, dma((2,)), dma, dma((2,)),
        dma,
        dma((3,)),
    ]
    return pl.pallas_call(
        kernel,
        out_shape=(pltpu.VMEM((UROWS, EMB), BF), pltpu.VMEM((STRIPE, EMB), BF), pltpu.VMEM((QUERIES, EMB), BF)),
        in_specs=[hbm] * 4,
        out_specs=(vm, vm, vm),
        scratch_shapes=scratch,
        compiler_params=pltpu.CompilerParams(collective_id=0, has_side_effects=True,
                                             vmem_limit_bytes=65929216),
        name='propagate',
    )(mask_blk, user_shard, item_shard, queries)


def solution(mesh):
    def device_step(mask_blk, user_shard, item_shard, queries):
        fu, fi, picked = propagate(mask_blk, user_shard, item_shard, queries.reshape(1, QUERIES))
        return scores_of(fu, fi, picked)

    return jax.shard_map(
        device_step, mesh=mesh,
        in_specs=(P('row', 'col'), P(('row', 'col'), None), P(('col', 'row'), None), P()),
        out_specs=(P(('row', 'col'), None), P(('col', 'row'), None), P(None, ('col', 'row'))),
        check_vma=False)
```
